256 devices in a mesh: curve: 64 (over y, z, core), sub: 4 (over x).
Axes of the slice: x: 4, y: 4, z: 8, core: 2. Of those that a mesh axis runs over, the one named last changes fastest.
Arguments:
- forcing: float32 [12, 6144, 1024], P(None, 'curve', 'sub'), may hold values from -10 to 10
- metric: float32 [6144, 1024], P('curve', 'sub'), may hold values from 0.25 to 4
- jacobian: float32 [6144, 1024], P('curve', 'sub'), may hold values from 0.5 to 2
- mode_scale: float32 [12], replicated, may hold values from 0.1 to 10
Outputs:
- solution: float32 [12, 6144, 1024], P(None, 'curve', 'sub')
- residual: float32 [12, 6144, 1024], P(None, 'curve', 'sub')
The draws below stay inside these ranges and needn't reach their ends.
All inputs are finite; a program needn't handle non-finite values.
Results may differ from the reference program's by a relative error of at most 0.0003.
Values sent between devices are 32-bit elements; how exact they have to be, the bound alone decides.
No kernel may reach another device: no remote copies, remote signals or barrier semaphores. Data moves between devices by JAX's collectives and lax.ppermute only.
A program may use at most 64 MiB of HBM per device.

```python
import math
import jax
import jax.numpy as jnp
import numpy as np
from jax import lax

NP = 4
MODES = 12
ITERS = 3
EBX = 24
NX = 6144
NY = 1024


def draw_forcing(key, part):
    noise_key, scale_key = jax.random.split(jax.random.fold_in(key, 7))
    regions = NX // (NP * EBX)
    region_scale = jnp.exp(jax.random.uniform(scale_key, (regions,), jnp.float32, math.log(0.3), math.log(3.0)))
    per_row = jnp.repeat(region_scale, NP * EBX)
    base = jax.random.normal(noise_key, (MODES, NX, NY), jnp.float32)
    return jnp.clip(base * per_row[None, :, None], -10.0, 10.0)


def block_scale(key, extent, cuts, low, high):
    level, own = 1.0, jax.random.fold_in(key, 6)
    for axis_at, blocks in cuts:
        steps = jnp.exp(jax.random.uniform(jax.random.fold_in(own, axis_at), (blocks,), jnp.float32, low / len(cuts), high / len(cuts)))
        level = level * jnp.repeat(steps, extent[axis_at] // blocks).reshape([-1 if axis == axis_at else 1 for axis in range(len(extent))])
    return level


def setup_inputs(seed: int = 0) -> dict:
    key_list = jax.random.split(jax.random.key(seed), 5)
    forcing = draw_forcing(jax.random.fold_in(key_list[4], 71), 0)
    metric = jnp.clip(jnp.exp(math.log(4.0) - 2.7725887 * jax.random.uniform(key_list[1], (NX, NY), jnp.float32) ** block_scale(key_list[1], (NX, NY), ((0, 64), (1, 4)), -0.2, 0.2)), 0.25, 4.0)
    jacobian = jnp.clip(jnp.exp(math.log(2.0) - 1.3862944 * jax.random.uniform(key_list[2], (NX, NY), jnp.float32) ** block_scale(key_list[2], (NX, NY), ((0, 64), (1, 4)), -0.2, 0.2)), 0.5, 2.0)
    mode_scale = jnp.clip(jnp.exp(jax.random.uniform(key_list[3], (MODES,), jnp.float32, math.log(0.1), math.log(10.0))), 0.1, 10.0)
    return {"forcing": forcing, "metric": metric, "jacobian": jacobian, "mode_scale": mode_scale}


def gll_tables():
    points = np.array([-1.0, -1.0 / math.sqrt(5.0), 1.0 / math.sqrt(5.0), 1.0])
    weights = np.array([1.0 / 6.0, 5.0 / 6.0, 5.0 / 6.0, 1.0 / 6.0])
    factor = np.array([np.prod([points[j] - points[m] for m in range(4) if m != j]) for j in range(4)])
    slopes = np.zeros((4, 4))
    for i in range(4):
        for j in range(4):
            if i != j:
                slopes[i, j] = factor[i] / (factor[j] * (points[i] - points[j]))
        slopes[i, i] = sum((1.0 / (points[i] - points[m]) for m in range(4) if m != i))
    return (slopes, weights)

def line_tables(count):
    phase = jnp.arange(count, dtype=jnp.int32) % 4
    on_edge = (phase == 0) | (phase == 3)
    line_w = jnp.where(on_edge, jnp.float32(1.0 / 6.0), jnp.float32(5.0 / 6.0))
    line_mult = jnp.where(on_edge, jnp.float32(2.0), jnp.float32(1.0))
    return (line_w, line_mult)

def assemble(values):
    for axis_dim in (0, 1):
        phase = lax.broadcasted_iota(jnp.int32, values.shape, axis_dim) % 4
        values = values + jnp.where(phase == 3, jnp.roll(values, -1, axis_dim), 0.0) + jnp.where(phase == 0, jnp.roll(values, 1, axis_dim), 0.0)
    return values

def apply_local(values, scale, slopes, mass_w, flux_w):
    row_count, col_count = values.shape
    shape4 = (row_count // 4, 4, col_count // 4, 4)
    blocks = values.reshape(shape4)
    hp = lax.Precision.HIGHEST
    grad_x = jnp.einsum('ak,xkyb->xayb', slopes, blocks, precision=hp)
    grad_y = jnp.einsum('bk,xayk->xayb', slopes, blocks, precision=hp)
    weight4 = flux_w.reshape(shape4)
    lap = jnp.einsum('ka,xkyb->xayb', slopes, weight4 * grad_x, precision=hp) + jnp.einsum('kb,xayk->xayb', slopes, weight4 * grad_y, precision=hp)
    return mass_w * values + scale * lap.reshape(row_count, col_count)

def diag_terms(flux_w, slopes):
    row_count, col_count = flux_w.shape
    shape4 = (row_count // 4, 4, col_count // 4, 4)
    weight4 = flux_w.reshape(shape4)
    hp = lax.Precision.HIGHEST
    squared = slopes * slopes
    terms = jnp.einsum('ka,xkyb->xayb', squared, weight4, precision=hp) + jnp.einsum('kb,xayk->xayb', squared, weight4, precision=hp)
    return terms.reshape(row_count, col_count)

def reference(forcing, metric, jacobian, mode_scale):
    slopes = jnp.asarray(gll_tables()[0], jnp.float32)
    row_w, row_mult = line_tables(metric.shape[0])
    col_w, col_mult = line_tables(metric.shape[1])
    grid_w = row_w[:, None] * col_w[None, :]
    inv_count = 1.0 / (row_mult[:, None] * col_mult[None, :])
    mass_w = jacobian * grid_w
    flux_w = metric * grid_w
    mass_diag = assemble(mass_w)
    lap_diag = assemble(diag_terms(flux_w, slopes))

    def solve_mode(member):
        source, scale = member
        rhs = assemble(source * mass_w)
        precond = mass_diag + scale * lap_diag
        solution = jnp.zeros_like(rhs)
        residual = rhs
        zvec = residual / precond
        direction = zvec
        rho_now = jnp.sum(residual * zvec * inv_count)
        for iteration in range(ITERS):
            image = assemble(apply_local(direction, scale, slopes, mass_w, flux_w))
            step_len = rho_now / jnp.sum(direction * image * inv_count)
            solution = solution + step_len * direction
            residual = residual - step_len * image
            zvec = residual / precond
            rho_next = jnp.sum(residual * zvec * inv_count)
            direction = zvec + rho_next / rho_now * direction
            rho_now = rho_next
        return (solution, residual)
    solution, residual = lax.map(solve_mode, (forcing, mode_scale))
    return (solution, residual)
```

```python
import functools
import math

import jax
import jax.numpy as jnp
import numpy as np
from jax import lax
from jax.experimental import pallas as pl
from jax.experimental.pallas import tpu as pltpu
from jax.sharding import PartitionSpec as P

GHOST = 4
PACK = 4
LANES = 128
AXES = ("curve", "sub")


def gll_tables():
    points = np.array([-1.0, -1.0 / math.sqrt(5.0), 1.0 / math.sqrt(5.0), 1.0])
    weights = np.array([1.0 / 6.0, 5.0 / 6.0, 5.0 / 6.0, 1.0 / 6.0])
    factor = np.array(
        [np.prod([points[j] - points[m] for m in range(4) if m != j]) for j in range(4)]
    )
    slopes = np.zeros((4, 4))
    for i in range(4):
        for j in range(4):
            if i != j:
                slopes[i, j] = factor[i] / (factor[j] * (points[i] - points[j]))
        slopes[i, i] = sum((1.0 / (points[i] - points[m]) for m in range(4) if m != i))
    return (slopes, weights)


SLOPES, WEIGHTS = gll_tables()
PAIRS = [(a, k) for a in range(4) for k in range(a + 1, 4)]


def plane(group, a, b):
    return (group * 4 + a) * 4 + b


def spread_kernel(rows, f_ref, metric_ref, jacobian_ref, up_ref, down_ref, t_ref, low_ref, high_ref, xs, xt):
    half = pl.program_id(0)
    own = rows // 4
    groups = f_ref.shape[0] // PACK
    per_half = LANES // 4
    for group in range(groups + 1):
        for a in range(4):
            at = group * 4 + a
            for m in range(PACK):
                if group < groups:
                    index = group * PACK + m
                    mine = f_ref[index, pl.ds(a, own, stride=4), :]
                else:
                    index = groups * PACK + m % 2
                    mine = (metric_ref, jacobian_ref)[m % 2][pl.ds(a, own, stride=4), :]
                xs[at, pl.ds(m, own, stride=PACK), :] = mine
                xs[at, pl.ds(own * PACK + m, GHOST, stride=PACK), :] = down_ref[
                    index, pl.ds(a, GHOST, stride=4), :
                ]
                xs[at, pl.ds((own + GHOST) * PACK + m, GHOST, stride=PACK), :] = up_ref[
                    index, pl.ds(a, GHOST, stride=4), :
                ]
            xt[at] = xs[at].T
            for b in range(4):
                t_ref[at * 4 + b] = xt[at, pl.ds(b, per_half, stride=4), :]

    @pl.when(half == 0)
    def _():
        for p in range(t_ref.shape[0]):
            low_ref[p] = t_ref[p, :GHOST, :]

    @pl.when(half == pl.num_programs(0) - 1)
    def _():
        for p in range(t_ref.shape[0]):
            high_ref[p] = t_ref[p, per_half - GHOST :, :]


def line_operator(coefs, values):
    out = [None] * 4
    for (a, k), coef in zip(PAIRS, coefs):
        flow = coef * (values[k] - values[a])
        out[a] = flow if out[a] is None else out[a] + flow
        out[k] = -flow if out[k] is None else out[k] - flow
    return out


def krylov_kernel(
    own_rows,
    t_ref,
    right_ref,
    left_ref,
    scale_ref,
    u0_ref,
    u1_ref,
    u2_ref,
    w_ref,
    mass_sum_ref,
    lap_sum_ref,
    part_ref,
    mass_ref,
    krow,
    kcol,
    minv,
    edge,
):
    groups = u0_ref.shape[0] // 16
    cols = t_ref.shape[1]
    total = u0_ref.shape[1]
    tiles = total // 8
    lane = lax.broadcasted_iota(jnp.int32, (8, LANES), 1)

    def next_row(x):
        return pltpu.roll(x, LANES - PACK, 1)

    def prev_row(x):
        return pltpu.roll(x, PACK, 1)

    def join_rows(first, last):
        shared = last + next_row(first)
        return prev_row(shared), shared

    def tile(t):
        return pl.ds(pl.multiple_of(t * 8, 8), 8)

    def set_edge(t, i, first, last):
        edge[2 * i, pl.ds(pl.multiple_of(t * 8 + 8, 8), 8), :] = first
        edge[2 * i + 1, pl.ds(pl.multiple_of(t * 8 + 8, 8), 8), :] = last

    def join_cols(i):
        edge[2 * i, total + 8 : total + 16, :] = edge[2 * i, 8:16, :]
        edge[2 * i + 1, 0:8, :] = edge[2 * i + 1, total : total + 8, :]
        first = edge[2 * i, 8 : total + 8, :] + edge[2 * i + 1, 7 : total + 7, :]
        last = edge[2 * i + 1, 8 : total + 8, :] + edge[2 * i, 9 : total + 9, :]
        return first, last

    def coefficients(t, fetch):
        even = lane % 2 == 0
        flux = [[None] * 4 for _ in range(4)]
        mass = [[None] * 4 for _ in range(4)]
        for a in range(4):
            for b in range(4):
                x = fetch(plane(groups, a, b))
                w = np.float32(WEIGHTS[a] * WEIGHTS[b])
                flux[a][b] = jnp.where(even, x, pltpu.roll(x, 1, 1)) * w
                mass[a][b] = jnp.where(even, pltpu.roll(x, LANES - 1, 1), x) * w
                mass_ref[a * 4 + b, tile(t), :] = mass[a][b]
        lap = [[None] * 4 for _ in range(4)]

        def add(a, b, value):
            lap[a][b] = value if lap[a][b] is None else lap[a][b] + value

        for line in range(4):
            for i, (p, q) in enumerate(PAIRS):
                c = [np.float32(SLOPES[j, p] * SLOPES[j, q]) for j in range(4)]
                kr = sum(flux[j][line] * c[j] for j in range(4))
                kc = sum(flux[line][j] * c[j] for j in range(4))
                krow[line * 6 + i, tile(t), :] = kr
                kcol[line * 6 + i, tile(t), :] = kc
                add(p, line, -kr)
                add(q, line, -kr)
                add(line, p, -kc)
                add(line, q, -kc)
        for values, out, base in ((mass, mass_sum_ref, 0), (lap, lap_sum_ref, 4)):
            for b in range(4):
                first, last = join_rows(values[0][b], values[3][b])
                column = [first, values[1][b], values[2][b], last]
                for a in range(4):
                    if b in (1, 2):
                        out[a * 4 + b, tile(t), :] = column[a]
                    else:
                        edge[2 * (base + a) + b // 3, pl.ds(pl.multiple_of(t * 8 + 8, 8), 8), :] = column[a]

    def own_tile(t):
        return lambda p: t_ref[p, tile(t), :]

    def ghost_tile(p):
        return jnp.concatenate([right_ref[p], left_ref[p]], axis=0)

    pl.loop(0, cols // 8)(lambda t: coefficients(t, own_tile(t)))
    coefficients(cols // 8, ghost_tile)
    for i in range(8):
        first, last = join_cols(i)
        out = (mass_sum_ref, lap_sum_ref)[i // 4]
        a = i % 4
        out[a * 4] = first
        out[a * 4 + 3] = last

    @pl.loop(0, 16)
    def _(p):
        mass_sum = mass_sum_ref[p]
        lap_sum = lap_sum_ref[p]
        for group in range(groups):
            minv[group * 16 + p] = 1.0 / (mass_sum + scale_ref[group : group + 1, :] * lap_sum)

    def source(t, fetch):
        for group in range(groups):
            for b in range(4):
                column = [
                    fetch(plane(group, a, b)) * mass_ref[a * 4 + b, tile(t), :] for a in range(4)
                ]
                for a in range(4):
                    w_ref[plane(group, a, b), tile(t), :] = column[a]
                column[0], column[3] = join_rows(column[0], column[3])
                for a in range(4):
                    p = plane(group, a, b)
                    if b in (1, 2):
                        u0_ref[p, tile(t), :] = column[a] * minv[p, tile(t), :]
                    else:
                        edge[2 * (group * 4 + a) + b // 3, pl.ds(pl.multiple_of(t * 8 + 8, 8), 8), :] = column[a]

    pl.loop(0, cols // 8)(lambda t: source(t, own_tile(t)))
    source(cols // 8, ghost_tile)

    @pl.loop(0, groups * 4)
    def _(i):
        first, last = join_cols(i)
        u0_ref[i * 4] = first * minv[i * 4]
        u0_ref[i * 4 + 3] = last * minv[i * 4 + 3]

    zero = jnp.zeros((8, LANES), jnp.float32)

    def first_moment(t, sums):
        sums = list(sums)
        for group in range(groups):
            for p in range(group * 16, group * 16 + 16):
                sums[group] += w_ref[p, tile(t), :] * u0_ref[p, tile(t), :]
        return tuple(sums)

    moments = [lax.fori_loop(0, cols // 8, first_moment, (zero,) * groups)]

    def apply(now_ref, old_ref, new_ref):
        def body(t, sums):
            sums = list(sums)
            own = (t < cols // 8).astype(jnp.float32)
            for group in range(groups):
                u = [[now_ref[plane(group, a, b), tile(t), :] for b in range(4)] for a in range(4)]
                lap = [[None] * 4 for _ in range(4)]
                for line in range(4):
                    out = line_operator(
                        [krow[line * 6 + i, tile(t), :] for i in range(6)],
                        [u[a][line] for a in range(4)],
                    )
                    for a in range(4):
                        lap[a][line] = out[a]
                for line in range(4):
                    out = line_operator(
                        [kcol[line * 6 + i, tile(t), :] for i in range(6)], u[line]
                    )
                    for b in range(4):
                        lap[line][b] = lap[line][b] + out[b]
                scale = scale_ref[group : group + 1, :]
                with_now, with_old = zero, zero
                y = [[None] * 4 for _ in range(4)]
                for a in range(4):
                    for b in range(4):
                        y[a][b] = mass_ref[a * 4 + b, tile(t), :] * u[a][b] + scale * lap[a][b]
                        with_now += u[a][b] * y[a][b]
                        if old_ref is not None:
                            with_old += old_ref[plane(group, a, b), tile(t), :] * y[a][b]
                sums[group] += own * with_now
                if old_ref is not None:
                    sums[groups + group] += own * with_old
                for b in range(4):
                    column = [y[a][b] for a in range(4)]
                    column[0], column[3] = join_rows(column[0], column[3])
                    for a in range(4):
                        p = plane(group, a, b)
                        if b in (1, 2):
                            if new_ref is None:
                                w_ref[p, tile(t), :] = column[a]
                            else:
                                new_ref[p, tile(t), :] = column[a] * minv[p, tile(t), :] - u[a][b]
                        else:
                            edge[2 * (group * 4 + a) + b // 3, pl.ds(pl.multiple_of(t * 8 + 8, 8), 8), :] = column[a]
            return tuple(sums)

        count = groups * (1 if old_ref is None else 2)
        sums = lax.fori_loop(0, tiles, body, (zero,) * count)

        @pl.loop(0, groups * 4)
        def _(i):
            for b, value in zip((0, 3), join_cols(i)):
                p = i * 4 + b
                if new_ref is None:
                    w_ref[p] = value
                else:
                    new_ref[p] = value * minv[p] - now_ref[p]

        return [sums[i * groups : (i + 1) * groups] for i in range(count // groups)]

    (g00,) = apply(u0_ref, None, u1_ref)
    g11, g01 = apply(u1_ref, u0_ref, u2_ref)
    g22, g12 = apply(u2_ref, u1_ref, None)
    rows = [jnp.sum(x, axis=0, keepdims=True) for q in (moments[0], g00, g01, g11, g12, g22) for x in q]
    rows += [jnp.zeros((1, LANES), jnp.float32)] * (-len(rows) % 8)
    table = jnp.concatenate(rows, axis=0)
    lanes = lax.broadcasted_iota(jnp.int32, table.shape, 1)
    lines = lax.broadcasted_iota(jnp.int32, table.shape, 0)
    table = jnp.where(lanes < own_rows // 4 * PACK, table, 0.0)
    shift = PACK
    while shift < LANES:
        table = table + pltpu.roll(table, shift, 1)
        shift *= 2
    table = jnp.where(lanes // PACK == lines, table, 0.0)
    part_ref[...] = jnp.broadcast_to(jnp.sum(table, axis=0, keepdims=True), part_ref.shape)


def combine_kernel(
    parts_ref, scale_ref, u0_ref, u1_ref, u2_ref, w_ref, mass_sum_ref, lap_sum_ref, sol_hbm, res_hbm, sol, res, xs, xt, sems
):
    halves, modes, rows, _ = sol.shape
    groups = modes // PACK
    own = rows // 4
    per_half = LANES // 4
    total = jnp.sum(parts_ref[...], axis=0, keepdims=True)
    table = jnp.broadcast_to(total, (24, LANES))
    lanes = lax.broadcasted_iota(jnp.int32, table.shape, 1)
    lines = lax.broadcasted_iota(jnp.int32, table.shape, 0)
    table = jnp.where(lanes // PACK == lines, table, 0.0)
    shift = PACK
    while shift < LANES:
        table = table + pltpu.roll(table, shift, 1)
        shift *= 2
    b0, g00, g01, g11, g12, g22 = [table[q * groups : (q + 1) * groups] for q in range(6)]
    g02 = g11
    b1 = g00 - b0
    b2 = g01 - b1
    l10 = g01 / g00
    l20 = g02 / g00
    d1 = g11 - l10 * g01
    t12 = g12 - l20 * g01
    l21 = t12 / d1
    d2 = g22 - l20 * g02 - l21 * t12
    y1 = b1 - l10 * b0
    y2 = b2 - l20 * b0 - l21 * y1
    c2 = y2 / d2
    c1 = y1 / d1 - l21 * c2
    c0 = b0 / g00 - l10 * c1 - l20 * c2
    copies = []
    for half in range(halves):
        span = slice(half * per_half, (half + 1) * per_half)
        for group in range(groups):
            k0, k1, k2 = [c[group : group + 1, :] for c in (c0, c1, c2)]
            scale = scale_ref[group : group + 1, :]
            for a in range(4):
                slot = group * 4 + a
                for b in range(4):
                    p = plane(group, a, b)
                    u0, u1, u2 = u0_ref[p, span, :], u1_ref[p, span, :], u2_ref[p, span, :]
                    diag = mass_sum_ref[a * 4 + b, span, :] + scale * lap_sum_ref[a * 4 + b, span, :]
                    xs[0, slot, pl.ds(b, per_half, stride=4), :] = k0 * u0 + k1 * u1 + k2 * u2
                    xs[1, slot, pl.ds(b, per_half, stride=4), :] = (
                        diag * (u0 - k0 * (u1 + u0) - k1 * (u2 + u1)) - k2 * w_ref[p, span, :]
                    )
                for i, out in enumerate((sol, res)):
                    xt[i, slot] = xs[i, slot].T
                    for m in range(PACK):
                        out[half, group * PACK + m, pl.ds(a, own, stride=4), :] = xt[
                            i, slot, pl.ds(m, own, stride=PACK), :
                        ]
        for i, (out, hbm) in enumerate(((sol, sol_hbm), (res, res_hbm))):
            copy = pltpu.make_async_copy(
                out.at[half], hbm.at[:, :, pl.ds(half * LANES, LANES)], sems.at[half, i]
            )
            copy.start()
            copies.append(copy)
    for copy in copies:
        copy.wait()


def shards(forcing, metric, jacobian, mode_scale):
    modes, rows, cols = forcing.shape
    groups = modes // PACK
    halo = 4 * GHOST
    f32 = jnp.float32

    def shift(x, axis, step):
        count = lax.axis_size(axis)
        return lax.ppermute(x, axis, [(i, (i + step) % count) for i in range(count)])

    def stack(span):
        return jnp.concatenate([forcing[:, span], metric[None, span], jacobian[None, span]], axis=0)

    up = shift(stack(slice(rows - halo, rows)), "curve", 1)
    down = shift(stack(slice(0, halo)), "curve", -1)

    planes = 16 * (groups + 1)
    ecols = cols // 4
    halves = cols // LANES
    per_half = LANES // 4
    whole = lambda *shape: pl.BlockSpec(shape, lambda h: (0,) * len(shape))
    spread, low, high = pl.pallas_call(
        functools.partial(spread_kernel, rows),
        grid=(halves,),
        in_specs=[
            pl.BlockSpec((modes, rows, LANES), lambda h: (0, 0, h)),
            pl.BlockSpec((rows, LANES), lambda h: (0, h)),
            pl.BlockSpec((rows, LANES), lambda h: (0, h)),
            pl.BlockSpec((modes + 2, halo, LANES), lambda h: (0, 0, h)),
            pl.BlockSpec((modes + 2, halo, LANES), lambda h: (0, 0, h)),
        ],
        out_specs=[
            pl.BlockSpec((planes, per_half, LANES), lambda h: (0, h, 0)),
            whole(planes, GHOST, LANES),
            whole(planes, GHOST, LANES),
        ],
        out_shape=[
            jax.ShapeDtypeStruct((planes, ecols, LANES), f32),
            jax.ShapeDtypeStruct((planes, GHOST, LANES), f32),
            jax.ShapeDtypeStruct((planes, GHOST, LANES), f32),
        ],
        scratch_shapes=[pltpu.VMEM((planes // 4, LANES, LANES), f32)] * 2,
        name="spread",
    )(forcing, metric, jacobian, up, down)

    left = shift(high, "sub", 1)
    right = shift(low, "sub", -1)
    scale = jnp.tile(mode_scale.reshape(groups, PACK), (1, LANES // PACK))

    total = ecols + 2 * GHOST
    state = jax.ShapeDtypeStruct((16 * groups, total, LANES), f32)
    shared = jax.ShapeDtypeStruct((16, total, LANES), f32)
    devices = lax.axis_size(AXES[0]) * lax.axis_size(AXES[1])
    vmem = pl.BlockSpec(memory_space=pltpu.VMEM)
    u0, u1, u2, w3, mass_sum, lap_sum, part = pl.pallas_call(
        functools.partial(krylov_kernel, rows),
        in_specs=[vmem] * 4,
        out_specs=[vmem] * 7,
        out_shape=[state] * 4 + [shared] * 2 + [jax.ShapeDtypeStruct((devices, LANES), f32)],
        scratch_shapes=[
            pltpu.VMEM((16, total, LANES), f32),
            pltpu.VMEM((24, total, LANES), f32),
            pltpu.VMEM((24, total, LANES), f32),
            pltpu.VMEM((16 * groups, total, LANES), f32),
            pltpu.VMEM((8 * groups, total + 16, LANES), f32),
        ],
        name="krylov",
    )(spread, right, left, scale)

    parts = lax.all_to_all(part, AXES, 0, 0, tiled=True)

    out = jax.ShapeDtypeStruct((modes, rows, cols), f32)
    anywhere = pl.BlockSpec(memory_space=pl.ANY)
    return tuple(
        pl.pallas_call(
            combine_kernel,
            in_specs=[vmem] * 8,
            out_specs=[anywhere] * 2,
            out_shape=[out] * 2,
            scratch_shapes=[
                pltpu.VMEM((halves, modes, rows, LANES), f32),
                pltpu.VMEM((halves, modes, rows, LANES), f32),
                pltpu.VMEM((2, 4 * groups, LANES, LANES), f32),
                pltpu.VMEM((2, 4 * groups, LANES, LANES), f32),
                pltpu.SemaphoreType.DMA((halves, 2)),
            ],
            name="combine",
        )(parts, scale, u0, u1, u2, w3, mass_sum, lap_sum)
    )


def solution(mesh):
    in_specs = (P(None, "curve", "sub"), P("curve", "sub"), P("curve", "sub"), P())
    out_specs = (P(None, "curve", "sub"), P(None, "curve", "sub"))
    return jax.shard_map(
        shards, mesh=mesh, in_specs=in_specs, out_specs=out_specs, check_vma=False
    )
```

```python
import functools
import math

import jax
import jax.numpy as jnp
import numpy as np
from jax import lax
from jax.experimental import pallas as pl
from jax.experimental.pallas import tpu as pltpu
from jax.sharding import PartitionSpec as P

GHOST = 4
PACK = 4
LANES = 128
AXES = ("curve", "sub")


def gll_tables():
    points = np.array([-1.0, -1.0 / math.sqrt(5.0), 1.0 / math.sqrt(5.0), 1.0])
    weights = np.array([1.0 / 6.0, 5.0 / 6.0, 5.0 / 6.0, 1.0 / 6.0])
    factor = np.array(
        [np.prod([points[j] - points[m] for m in range(4) if m != j]) for j in range(4)]
    )
    slopes = np.zeros((4, 4))
    for i in range(4):
        for j in range(4):
            if i != j:
                slopes[i, j] = factor[i] / (factor[j] * (points[i] - points[j]))
        slopes[i, i] = sum((1.0 / (points[i] - points[m]) for m in range(4) if m != i))
    return (slopes, weights)


SLOPES, WEIGHTS = gll_tables()
PAIRS = [(a, k) for a in range(4) for k in range(a + 1, 4)]


def plane(group, a, b):
    return (group * 4 + a) * 4 + b


def strips_kernel(f_hbm, metric_hbm, jacobian_hbm, top, bottom, sems):
    modes, rows, _ = f_hbm.shape
    halo = top.shape[1]
    copies = []
    for side, (out, at) in enumerate(((top, 0), (bottom, rows - halo))):
        span = pl.ds(at, halo)
        copies += [
            pltpu.make_async_copy(f_hbm.at[:, span, :], out.at[pl.ds(0, modes)], sems.at[side, 0]),
            pltpu.make_async_copy(metric_hbm.at[span, :], out.at[modes], sems.at[side, 1]),
            pltpu.make_async_copy(jacobian_hbm.at[span, :], out.at[modes + 1], sems.at[side, 2]),
        ]
    for copy in copies:
        copy.start()
    for copy in copies:
        copy.wait()


def spread_kernel(rows, f_ref, metric_ref, jacobian_ref, up_ref, down_ref, t_ref, low_ref, high_ref, xs, xt):
    half = pl.program_id(0)
    own = rows // 4
    groups = f_ref.shape[0] // PACK
    per_half = LANES // 4
    for group in range(groups + 1):
        for a in range(4):
            at = group * 4 + a
            for m in range(PACK):
                if group < groups:
                    index = group * PACK + m
                    mine = f_ref[index, pl.ds(a, own, stride=4), :]
                else:
                    index = groups * PACK + m % 2
                    mine = (metric_ref, jacobian_ref)[m % 2][pl.ds(a, own, stride=4), :]
                xs[at, pl.ds(m, own, stride=PACK), :] = mine
                xs[at, pl.ds(own * PACK + m, GHOST, stride=PACK), :] = down_ref[
                    index, pl.ds(a, GHOST, stride=4), :
                ]
                xs[at, pl.ds((own + GHOST) * PACK + m, GHOST, stride=PACK), :] = up_ref[
                    index, pl.ds(a, GHOST, stride=4), :
                ]
            xt[at] = xs[at].T
            for b in range(4):
                t_ref[at * 4 + b] = xt[at, pl.ds(b, per_half, stride=4), :]

    @pl.when(half == 0)
    def _():
        for p in range(t_ref.shape[0]):
            low_ref[p] = t_ref[p, :GHOST, :]

    @pl.when(half == pl.num_programs(0) - 1)
    def _():
        for p in range(t_ref.shape[0]):
            high_ref[p] = t_ref[p, per_half - GHOST :, :]


def line_operator(coefs, values):
    out = [None] * 4
    for (a, k), coef in zip(PAIRS, coefs):
        flow = coef * (values[k] - values[a])
        out[a] = flow if out[a] is None else out[a] + flow
        out[k] = -flow if out[k] is None else out[k] - flow
    return out


def krylov_kernel(
    own_rows,
    t_ref,
    right_ref,
    left_ref,
    scale_ref,
    u0_ref,
    u1_ref,
    u2_ref,
    w_ref,
    mass_sum_ref,
    lap_sum_ref,
    part_ref,
    mass_ref,
    krow,
    kcol,
    minv,
    edge,
):
    groups = u0_ref.shape[0] // 16
    cols = t_ref.shape[1]
    total = u0_ref.shape[1]
    tiles = total // 8
    lane = lax.broadcasted_iota(jnp.int32, (8, LANES), 1)

    def next_row(x):
        return pltpu.roll(x, LANES - PACK, 1)

    def prev_row(x):
        return pltpu.roll(x, PACK, 1)

    def join_rows(first, last):
        shared = last + next_row(first)
        return prev_row(shared), shared

    def tile(t):
        return pl.ds(pl.multiple_of(t * 8, 8), 8)

    def set_edge(t, i, first, last):
        edge[2 * i, pl.ds(pl.multiple_of(t * 8 + 8, 8), 8), :] = first
        edge[2 * i + 1, pl.ds(pl.multiple_of(t * 8 + 8, 8), 8), :] = last

    def join_cols(i):
        edge[2 * i, total + 8 : total + 16, :] = edge[2 * i, 8:16, :]
        edge[2 * i + 1, 0:8, :] = edge[2 * i + 1, total : total + 8, :]
        first = edge[2 * i, 8 : total + 8, :] + edge[2 * i + 1, 7 : total + 7, :]
        last = edge[2 * i + 1, 8 : total + 8, :] + edge[2 * i, 9 : total + 9, :]
        return first, last

    def coefficients(t, fetch):
        even = lane % 2 == 0
        flux = [[None] * 4 for _ in range(4)]
        mass = [[None] * 4 for _ in range(4)]
        for a in range(4):
            for b in range(4):
                x = fetch(plane(groups, a, b))
                w = np.float32(WEIGHTS[a] * WEIGHTS[b])
                flux[a][b] = jnp.where(even, x, pltpu.roll(x, 1, 1)) * w
                mass[a][b] = jnp.where(even, pltpu.roll(x, LANES - 1, 1), x) * w
                mass_ref[a * 4 + b, tile(t), :] = mass[a][b]
        lap = [[None] * 4 for _ in range(4)]

        def add(a, b, value):
            lap[a][b] = value if lap[a][b] is None else lap[a][b] + value

        for line in range(4):
            for i, (p, q) in enumerate(PAIRS):
                c = [np.float32(SLOPES[j, p] * SLOPES[j, q]) for j in range(4)]
                kr = sum(flux[j][line] * c[j] for j in range(4))
                kc = sum(flux[line][j] * c[j] for j in range(4))
                krow[line * 6 + i, tile(t), :] = kr
                kcol[line * 6 + i, tile(t), :] = kc
                add(p, line, -kr)
                add(q, line, -kr)
                add(line, p, -kc)
                add(line, q, -kc)
        for values, out, base in ((mass, mass_sum_ref, 0), (lap, lap_sum_ref, 4)):
            for b in range(4):
                first, last = join_rows(values[0][b], values[3][b])
                column = [first, values[1][b], values[2][b], last]
                for a in range(4):
                    if b in (1, 2):
                        out[a * 4 + b, tile(t), :] = column[a]
                    else:
                        edge[2 * (base + a) + b // 3, pl.ds(pl.multiple_of(t * 8 + 8, 8), 8), :] = column[a]

    def own_tile(t):
        return lambda p: t_ref[p, tile(t), :]

    def ghost_tile(p):
        return jnp.concatenate([right_ref[p], left_ref[p]], axis=0)

    pl.loop(0, cols // 8)(lambda t: coefficients(t, own_tile(t)))
    coefficients(cols // 8, ghost_tile)
    for i in range(8):
        first, last = join_cols(i)
        out = (mass_sum_ref, lap_sum_ref)[i // 4]
        a = i % 4
        out[a * 4] = first
        out[a * 4 + 3] = last

    @pl.loop(0, 16)
    def _(p):
        mass_sum = mass_sum_ref[p]
        lap_sum = lap_sum_ref[p]
        for group in range(groups):
            minv[group * 16 + p] = 1.0 / (mass_sum + scale_ref[group : group + 1, :] * lap_sum)

    def source(t, fetch):
        for group in range(groups):
            for b in range(4):
                column = [
                    fetch(plane(group, a, b)) * mass_ref[a * 4 + b, tile(t), :] for a in range(4)
                ]
                for a in range(4):
                    w_ref[plane(group, a, b), tile(t), :] = column[a]
                column[0], column[3] = join_rows(column[0], column[3])
                for a in range(4):
                    p = plane(group, a, b)
                    if b in (1, 2):
                        u0_ref[p, tile(t), :] = column[a] * minv[p, tile(t), :]
                    else:
                        edge[2 * (group * 4 + a) + b // 3, pl.ds(pl.multiple_of(t * 8 + 8, 8), 8), :] = column[a]

    pl.loop(0, cols // 8)(lambda t: source(t, own_tile(t)))
    source(cols // 8, ghost_tile)

    @pl.loop(0, groups * 4)
    def _(i):
        first, last = join_cols(i)
        u0_ref[i * 4] = first * minv[i * 4]
        u0_ref[i * 4 + 3] = last * minv[i * 4 + 3]

    zero = jnp.zeros((8, LANES), jnp.float32)

    def first_moment(t, sums):
        sums = list(sums)
        for group in range(groups):
            for p in range(group * 16, group * 16 + 16):
                sums[group] += w_ref[p, tile(t), :] * u0_ref[p, tile(t), :]
        return tuple(sums)

    moments = [lax.fori_loop(0, cols // 8, first_moment, (zero,) * groups)]

    def apply(now_ref, old_ref, new_ref):
        def body(t, sums):
            sums = list(sums)
            own = (t < cols // 8).astype(jnp.float32)
            for group in range(groups):
                u = [[now_ref[plane(group, a, b), tile(t), :] for b in range(4)] for a in range(4)]
                lap = [[None] * 4 for _ in range(4)]
                for line in range(4):
                    out = line_operator(
                        [krow[line * 6 + i, tile(t), :] for i in range(6)],
                        [u[a][line] for a in range(4)],
                    )
                    for a in range(4):
                        lap[a][line] = out[a]
                for line in range(4):
                    out = line_operator(
                        [kcol[line * 6 + i, tile(t), :] for i in range(6)], u[line]
                    )
                    for b in range(4):
                        lap[line][b] = lap[line][b] + out[b]
                scale = scale_ref[group : group + 1, :]
                with_now, with_old = zero, zero
                y = [[None] * 4 for _ in range(4)]
                for a in range(4):
                    for b in range(4):
                        y[a][b] = mass_ref[a * 4 + b, tile(t), :] * u[a][b] + scale * lap[a][b]
                        with_now += u[a][b] * y[a][b]
                        if old_ref is not None:
                            with_old += old_ref[plane(group, a, b), tile(t), :] * y[a][b]
                sums[group] += own * with_now
                if old_ref is not None:
                    sums[groups + group] += own * with_old
                for b in range(4):
                    column = [y[a][b] for a in range(4)]
                    column[0], column[3] = join_rows(column[0], column[3])
                    for a in range(4):
                        p = plane(group, a, b)
                        if b in (1, 2):
                            if new_ref is None:
                                w_ref[p, tile(t), :] = column[a]
                            else:
                                new_ref[p, tile(t), :] = column[a] * minv[p, tile(t), :] - u[a][b]
                        else:
                            edge[2 * (group * 4 + a) + b // 3, pl.ds(pl.multiple_of(t * 8 + 8, 8), 8), :] = column[a]
            return tuple(sums)

        count = groups * (1 if old_ref is None else 2)
        sums = lax.fori_loop(0, tiles, body, (zero,) * count)

        @pl.loop(0, groups * 4)
        def _(i):
            for b, value in zip((0, 3), join_cols(i)):
                p = i * 4 + b
                if new_ref is None:
                    w_ref[p] = value
                else:
                    new_ref[p] = value * minv[p] - now_ref[p]

        return [sums[i * groups : (i + 1) * groups] for i in range(count // groups)]

    (g00,) = apply(u0_ref, None, u1_ref)
    g11, g01 = apply(u1_ref, u0_ref, u2_ref)
    g22, g12 = apply(u2_ref, u1_ref, None)
    rows = [jnp.sum(x, axis=0, keepdims=True) for q in (moments[0], g00, g01, g11, g12, g22) for x in q]
    rows += [jnp.zeros((1, LANES), jnp.float32)] * (-len(rows) % 8)
    table = jnp.concatenate(rows, axis=0)
    lanes = lax.broadcasted_iota(jnp.int32, table.shape, 1)
    lines = lax.broadcasted_iota(jnp.int32, table.shape, 0)
    table = jnp.where(lanes < own_rows // 4 * PACK, table, 0.0)
    shift = PACK
    while shift < LANES:
        table = table + pltpu.roll(table, shift, 1)
        shift *= 2
    table = jnp.where(lanes // PACK == lines, table, 0.0)
    part_ref[...] = jnp.broadcast_to(jnp.sum(table, axis=0, keepdims=True), part_ref.shape)


def combine_kernel(
    parts_ref, scale_ref, u0_ref, u1_ref, u2_ref, w_ref, mass_sum_ref, lap_sum_ref, sol_hbm, res_hbm, sol, res, xs, xt, sems
):
    halves, modes, rows, _ = sol.shape
    groups = modes // PACK
    own = rows // 4
    per_half = LANES // 4
    total = jnp.sum(parts_ref[...], axis=0, keepdims=True)
    table = jnp.broadcast_to(total, (24, LANES))
    lanes = lax.broadcasted_iota(jnp.int32, table.shape, 1)
    lines = lax.broadcasted_iota(jnp.int32, table.shape, 0)
    table = jnp.where(lanes // PACK == lines, table, 0.0)
    shift = PACK
    while shift < LANES:
        table = table + pltpu.roll(table, shift, 1)
        shift *= 2
    b0, g00, g01, g11, g12, g22 = [table[q * groups : (q + 1) * groups] for q in range(6)]
    g02 = g11
    b1 = g00 - b0
    b2 = g01 - b1
    l10 = g01 / g00
    l20 = g02 / g00
    d1 = g11 - l10 * g01
    t12 = g12 - l20 * g01
    l21 = t12 / d1
    d2 = g22 - l20 * g02 - l21 * t12
    y1 = b1 - l10 * b0
    y2 = b2 - l20 * b0 - l21 * y1
    c2 = y2 / d2
    c1 = y1 / d1 - l21 * c2
    c0 = b0 / g00 - l10 * c1 - l20 * c2
    copies = []
    for half in range(halves):
        span = slice(half * per_half, (half + 1) * per_half)
        for group in range(groups):
            k0, k1, k2 = [c[group : group + 1, :] for c in (c0, c1, c2)]
            scale = scale_ref[group : group + 1, :]
            for a in range(4):
                slot = group * 4 + a
                for b in range(4):
                    p = plane(group, a, b)
                    u0, u1, u2 = u0_ref[p, span, :], u1_ref[p, span, :], u2_ref[p, span, :]
                    diag = mass_sum_ref[a * 4 + b, span, :] + scale * lap_sum_ref[a * 4 + b, span, :]
                    xs[0, slot, pl.ds(b, per_half, stride=4), :] = k0 * u0 + k1 * u1 + k2 * u2
                    xs[1, slot, pl.ds(b, per_half, stride=4), :] = (
                        diag * (u0 - k0 * (u1 + u0) - k1 * (u2 + u1)) - k2 * w_ref[p, span, :]
                    )
                for i, out in enumerate((sol, res)):
                    xt[i, slot] = xs[i, slot].T
                    for m in range(PACK):
                        out[half, group * PACK + m, pl.ds(a, own, stride=4), :] = xt[
                            i, slot, pl.ds(m, own, stride=PACK), :
                        ]
        for i, (out, hbm) in enumerate(((sol, sol_hbm), (res, res_hbm))):
            copy = pltpu.make_async_copy(
                out.at[half], hbm.at[:, :, pl.ds(half * LANES, LANES)], sems.at[half, i]
            )
            copy.start()
            copies.append(copy)
    for copy in copies:
        copy.wait()


def shards(forcing, metric, jacobian, mode_scale):
    modes, rows, cols = forcing.shape
    groups = modes // PACK
    halo = 4 * GHOST
    f32 = jnp.float32

    def shift(x, axis, step):
        count = lax.axis_size(axis)
        return lax.ppermute(x, axis, [(i, (i + step) % count) for i in range(count)])

    vmem = pl.BlockSpec(memory_space=pltpu.VMEM)
    anywhere = pl.BlockSpec(memory_space=pl.ANY)
    top, bottom = pl.pallas_call(
        strips_kernel,
        in_specs=[anywhere] * 3,
        out_specs=[vmem] * 2,
        out_shape=[jax.ShapeDtypeStruct((modes + 2, halo, cols), f32)] * 2,
        scratch_shapes=[pltpu.SemaphoreType.DMA((2, 3))],
        name="strips",
    )(forcing, metric, jacobian)
    up = shift(bottom, "curve", 1)
    down = shift(top, "curve", -1)

    planes = 16 * (groups + 1)
    ecols = cols // 4
    halves = cols // LANES
    per_half = LANES // 4
    whole = lambda *shape: pl.BlockSpec(shape, lambda h: (0,) * len(shape))
    spread, low, high = pl.pallas_call(
        functools.partial(spread_kernel, rows),
        grid=(halves,),
        in_specs=[
            pl.BlockSpec((modes, rows, LANES), lambda h: (0, 0, h)),
            pl.BlockSpec((rows, LANES), lambda h: (0, h)),
            pl.BlockSpec((rows, LANES), lambda h: (0, h)),
            pl.BlockSpec((modes + 2, halo, LANES), lambda h: (0, 0, h)),
            pl.BlockSpec((modes + 2, halo, LANES), lambda h: (0, 0, h)),
        ],
        out_specs=[
            pl.BlockSpec((planes, per_half, LANES), lambda h: (0, h, 0)),
            whole(planes, GHOST, LANES),
            whole(planes, GHOST, LANES),
        ],
        out_shape=[
            jax.ShapeDtypeStruct((planes, ecols, LANES), f32),
            jax.ShapeDtypeStruct((planes, GHOST, LANES), f32),
            jax.ShapeDtypeStruct((planes, GHOST, LANES), f32),
        ],
        scratch_shapes=[pltpu.VMEM((planes // 4, LANES, LANES), f32)] * 2,
        compiler_params=pltpu.CompilerParams(vmem_limit_bytes=12 << 20),
        name="spread",
    )(forcing, metric, jacobian, up, down)

    left = shift(high, "sub", 1)
    right = shift(low, "sub", -1)
    scale = jnp.tile(mode_scale.reshape(groups, PACK), (1, LANES // PACK))

    total = ecols + 2 * GHOST
    state = jax.ShapeDtypeStruct((16 * groups, total, LANES), f32)
    shared = jax.ShapeDtypeStruct((16, total, LANES), f32)
    devices = lax.axis_size(AXES[0]) * lax.axis_size(AXES[1])
    u0, u1, u2, w3, mass_sum, lap_sum, part = pl.pallas_call(
        functools.partial(krylov_kernel, rows),
        in_specs=[vmem] * 4,
        out_specs=[vmem] * 7,
        out_shape=[state] * 4 + [shared] * 2 + [jax.ShapeDtypeStruct((devices, LANES), f32)],
        scratch_shapes=[
            pltpu.VMEM((16, total, LANES), f32),
            pltpu.VMEM((24, total, LANES), f32),
            pltpu.VMEM((24, total, LANES), f32),
            pltpu.VMEM((16 * groups, total, LANES), f32),
            pltpu.VMEM((8 * groups, total + 16, LANES), f32),
        ],
        compiler_params=pltpu.CompilerParams(vmem_limit_bytes=24 << 20),
        name="krylov",
    )(spread, right, left, scale)

    parts = lax.all_to_all(part, AXES, 0, 0, tiled=True)

    out = jax.ShapeDtypeStruct((modes, rows, cols), f32)
    return tuple(
        pl.pallas_call(
            combine_kernel,
            in_specs=[vmem] * 8,
            out_specs=[anywhere] * 2,
            out_shape=[out] * 2,
            scratch_shapes=[
                pltpu.VMEM((halves, modes, rows, LANES), f32),
                pltpu.VMEM((halves, modes, rows, LANES), f32),
                pltpu.VMEM((2, 4 * groups, LANES, LANES), f32),
                pltpu.VMEM((2, 4 * groups, LANES, LANES), f32),
                pltpu.SemaphoreType.DMA((halves, 2)),
            ],
            compiler_params=pltpu.CompilerParams(vmem_limit_bytes=20 << 20),
            name="combine",
        )(parts, scale, u0, u1, u2, w3, mass_sum, lap_sum)
    )


def solution(mesh):
    in_specs = (P(None, "curve", "sub"), P("curve", "sub"), P("curve", "sub"), P())
    out_specs = (P(None, "curve", "sub"), P(None, "curve", "sub"))
    return jax.shard_map(
        shards, mesh=mesh, in_specs=in_specs, out_specs=out_specs, check_vma=False
    )
```

```python
import functools
import math

import jax
import jax.numpy as jnp
import numpy as np
from jax import lax
from jax.experimental import pallas as pl
from jax.experimental.pallas import tpu as pltpu
from jax.sharding import PartitionSpec as P

GHOST = 4
PACK = 4
LANES = 128
AXES = ("curve", "sub")


def gll_tables():
    points = np.array([-1.0, -1.0 / math.sqrt(5.0), 1.0 / math.sqrt(5.0), 1.0])
    weights = np.array([1.0 / 6.0, 5.0 / 6.0, 5.0 / 6.0, 1.0 / 6.0])
    factor = np.array(
        [np.prod([points[j] - points[m] for m in range(4) if m != j]) for j in range(4)]
    )
    slopes = np.zeros((4, 4))
    for i in range(4):
        for j in range(4):
            if i != j:
                slopes[i, j] = factor[i] / (factor[j] * (points[i] - points[j]))
        slopes[i, i] = sum((1.0 / (points[i] - points[m]) for m in range(4) if m != i))
    return (slopes, weights)


SLOPES, WEIGHTS = gll_tables()
PAIRS = [(a, k) for a in range(4) for k in range(a + 1, 4)]


def plane(group, a, b):
    return (group * 4 + a) * 4 + b


def strips_kernel(f_hbm, metric_hbm, jacobian_hbm, top, bottom, shared, sems):
    modes, rows, _ = f_hbm.shape
    halo = top.shape[1]
    copies = []
    for side, (out, at) in enumerate(((top, 0), (bottom, rows - halo))):
        span = pl.ds(at, halo)
        copies += [
            pltpu.make_async_copy(f_hbm.at[:, span, :], out.at[pl.ds(0, modes)], sems.at[side, 0]),
            pltpu.make_async_copy(metric_hbm.at[span, :], out.at[modes], sems.at[side, 1]),
            pltpu.make_async_copy(jacobian_hbm.at[span, :], out.at[modes + 1], sems.at[side, 2]),
        ]
    copies += [
        pltpu.make_async_copy(metric_hbm, shared.at[0], sems.at[2, 0]),
        pltpu.make_async_copy(jacobian_hbm, shared.at[1], sems.at[2, 1]),
    ]
    for copy in copies:
        copy.start()
    for copy in copies:
        copy.wait()


def spread_kernel(rows, f_ref, shared_ref, up_ref, down_ref, t_ref, low_ref, high_ref, xs, xt):
    half = pl.program_id(0)
    own = rows // 4
    groups = f_ref.shape[0] // PACK
    per_half = LANES // 4
    for group in range(groups + 1):
        for a in range(4):
            at = group * 4 + a
            for m in range(PACK):
                if group < groups:
                    index = group * PACK + m
                    mine = f_ref[index, pl.ds(a, own, stride=4), :]
                else:
                    index = groups * PACK + m % 2
                    mine = shared_ref[m % 2, pl.ds(a, own, stride=4), :]
                xs[at, pl.ds(m, own, stride=PACK), :] = mine
                xs[at, pl.ds(own * PACK + m, GHOST, stride=PACK), :] = down_ref[
                    index, pl.ds(a, GHOST, stride=4), :
                ]
                xs[at, pl.ds((own + GHOST) * PACK + m, GHOST, stride=PACK), :] = up_ref[
                    index, pl.ds(a, GHOST, stride=4), :
                ]
            xt[at] = xs[at].T
            for b in range(4):
                t_ref[at * 4 + b] = xt[at, pl.ds(b, per_half, stride=4), :]

    @pl.when(half == 0)
    def _():
        for p in range(t_ref.shape[0]):
            low_ref[p] = t_ref[p, :GHOST, :]

    @pl.when(half == pl.num_programs(0) - 1)
    def _():
        for p in range(t_ref.shape[0]):
            high_ref[p] = t_ref[p, per_half - GHOST :, :]


def line_operator(coefs, values):
    f01, f02, f03, f12, f13, f23 = [
        coef * (values[k] - values[a]) for (a, k), coef in zip(PAIRS, coefs)
    ]
    return f01 + f02 + f03, f12 + f13 - f01, f23 - f02 - f12, f03 + f13 + f23


def tile(t):
    return pl.ds(pl.multiple_of(t * 8, 8), 8)


def spare(t):
    return pl.ds(pl.multiple_of(t * 8 + 8, 8), 8)


def join_rows(first, last):
    shared = last + pltpu.roll(first, LANES - PACK, 1)
    return pltpu.roll(shared, PACK, 1), shared


def join_cols(edge, i, total):
    edge[2 * i, total + 8 : total + 16, :] = edge[2 * i, 8:16, :]
    edge[2 * i + 1, 0:8, :] = edge[2 * i + 1, total : total + 8, :]
    first = edge[2 * i, 8 : total + 8, :] + edge[2 * i + 1, 7 : total + 7, :]
    last = edge[2 * i + 1, 8 : total + 8, :] + edge[2 * i, 9 : total + 9, :]
    return first, last


def prepare(t, fetch, scale_ref, mass_ref, krow, kcol, mass_sum_ref, lap_sum_ref, minv, u0_ref, source_ref, cedge, redge):
    groups = u0_ref.shape[0] // 16
    lane = lax.broadcasted_iota(jnp.int32, (8, LANES), 1)
    even = lane % 2 == 0
    grid = [(a, b) for a in range(4) for b in range(4)]
    scales = [scale_ref[group : group + 1, :] for group in range(groups)]
    flux, mass, lap = {}, {}, {}
    for a, b in grid:
        x = fetch(plane(groups, a, b))
        w = np.float32(WEIGHTS[a] * WEIGHTS[b])
        flux[a, b] = jnp.where(even, x, pltpu.roll(x, 1, 1)) * w
        mass[a, b] = jnp.where(even, pltpu.roll(x, LANES - 1, 1), x) * w
    for group in range(groups):
        inverse = 1.0 / scales[group]
        for a, b in grid:
            mass_ref[plane(group, a, b), tile(t), :] = mass[a, b] * inverse
            source_ref[plane(group, a, b), tile(t), :] = fetch(plane(group, a, b)) * mass[a, b]

    def less(a, b, value):
        lap[a, b] = lap[a, b] + value if (a, b) in lap else value

    for line in range(4):
        for i, (p, q) in enumerate(PAIRS):
            c = [np.float32(SLOPES[j, p] * SLOPES[j, q]) for j in range(4)]
            kr = sum(flux[j, line] * c[j] for j in range(4))
            kc = sum(flux[line, j] * c[j] for j in range(4))
            krow[line * 6 + i, tile(t), :] = kr
            kcol[line * 6 + i, tile(t), :] = kc
            less(p, line, kr)
            less(q, line, kr)
            less(line, p, kc)
            less(line, q, kc)
    for a, b in grid:
        lap[a, b] = -lap[a, b]
    for values, out, base in ((mass, mass_sum_ref, 0), (lap, lap_sum_ref, 4)):
        for b in range(4):
            values[0, b], values[3, b] = join_rows(values[0, b], values[3, b])
            for a in range(4):
                if b in (1, 2):
                    out[a * 4 + b, tile(t), :] = values[a, b]
                else:
                    cedge[2 * (base + a) + b // 3, spare(t), :] = values[a, b]
    for group in range(groups):
        for b in range(4):
            column = [source_ref[plane(group, a, b), tile(t), :] for a in range(4)]
            column[0], column[3] = join_rows(column[0], column[3])
            for a in range(4):
                p = plane(group, a, b)
                if b in (1, 2):
                    inverse = 1.0 / (mass[a, b] + scales[group] * lap[a, b])
                    u0_ref[p, tile(t), :] = column[a] * inverse
                    minv[p, tile(t), :] = inverse * scales[group]
                else:
                    redge[2 * (group * 4 + a) + b // 3, spare(t), :] = column[a]


def prep_kernel(t_ref, scale_ref, *refs):
    @pl.loop(0, t_ref.shape[1] // 8)
    def _(t):
        prepare(t, lambda p: t_ref[p, tile(t), :], scale_ref, *refs)


def krylov_kernel(own_rows, cols, right_ref, left_ref, scale_ref, *refs):
    state = refs[10:20]
    u1_ref, u2_ref, part_ref, edge = refs[20:]
    mass_ref, krow, kcol, mass_sum_ref, lap_sum_ref, minv, u0_ref, w_ref, cedge, redge = state
    groups = u0_ref.shape[0] // 16
    total = u0_ref.shape[1]
    tiles = total // 8
    own_tiles = cols // 8
    scales = [scale_ref[group : group + 1, :] for group in range(groups)]
    prepare(
        own_tiles, lambda p: jnp.concatenate([right_ref[p], left_ref[p]], axis=0), scale_ref, *state
    )

    @pl.loop(0, 4)
    def _(a):
        mass_sums = join_cols(cedge, a, total)
        lap_sums = join_cols(cedge, 4 + a, total)
        for side, b in enumerate((0, 3)):
            mass_sum_ref[a * 4 + b] = mass_sums[side]
            lap_sum_ref[a * 4 + b] = lap_sums[side]
        for group in range(groups):
            source = join_cols(redge, group * 4 + a, total)
            for side, b in enumerate((0, 3)):
                inverse = 1.0 / (mass_sums[side] + scales[group] * lap_sums[side])
                u0_ref[plane(group, a, b)] = source[side] * inverse
                minv[plane(group, a, b)] = inverse * scales[group]

    zero = jnp.zeros((8, LANES), jnp.float32)

    def apply(now_ref, old_ref, new_ref):
        def body(t, sums):
            sums = list(sums)
            own = (t < own_tiles).astype(jnp.float32)
            for group in range(groups):
                u = [[now_ref[plane(group, a, b), tile(t), :] for b in range(4)] for a in range(4)]
                along_rows = [
                    line_operator(
                        [krow[line * 6 + i, tile(t), :] for i in range(6)],
                        [u[a][line] for a in range(4)],
                    )
                    for line in range(4)
                ]
                along_cols = [
                    line_operator([kcol[line * 6 + i, tile(t), :] for i in range(6)], u[line])
                    for line in range(4)
                ]
                with_now, with_old = zero, zero
                y = [[None] * 4 for _ in range(4)]
                for a in range(4):
                    for b in range(4):
                        p = plane(group, a, b)
                        value = mass_ref[p, tile(t), :] * u[a][b]
                        row, col = along_rows[b][a], along_cols[a][b]
                        value = value - row if a == 3 else value + row
                        value = value - col if b == 3 else value + col
                        y[a][b] = value
                        with_now += u[a][b] * value
                        if old_ref is None:
                            with_old += w_ref[p, tile(t), :] * u[a][b]
                        else:
                            with_old += old_ref[p, tile(t), :] * value
                sums[group] += own * with_now
                sums[groups + group] += own * with_old
                for b in range(4):
                    column = [y[a][b] for a in range(4)]
                    column[0], column[3] = join_rows(column[0], column[3])
                    for a in range(4):
                        p = plane(group, a, b)
                        if b in (1, 2):
                            if new_ref is None:
                                w_ref[p, tile(t), :] = column[a]
                            else:
                                new_ref[p, tile(t), :] = column[a] * minv[p, tile(t), :] - u[a][b]
                        else:
                            edge[2 * (group * 4 + a) + b // 3, spare(t), :] = column[a]
            return tuple(sums)

        sums = lax.fori_loop(0, tiles, body, (zero,) * (2 * groups))

        @pl.loop(0, groups * 4)
        def _(i):
            for b, value in zip((0, 3), join_cols(edge, i, total)):
                p = i * 4 + b
                if new_ref is None:
                    w_ref[p] = value
                else:
                    new_ref[p] = value * minv[p] - now_ref[p]

        return sums[:groups], sums[groups:]

    g00, b0 = apply(u0_ref, None, u1_ref)
    g11, g01 = apply(u1_ref, u0_ref, u2_ref)
    g22, g12 = apply(u2_ref, u1_ref, None)
    rows = [jnp.sum(x, axis=0, keepdims=True) for x in b0]
    for q in (g00, g01, g11, g12, g22):
        rows += [scale * jnp.sum(x, axis=0, keepdims=True) for scale, x in zip(scales, q)]
    rows += [jnp.zeros((1, LANES), jnp.float32)] * (-len(rows) % 8)
    table = jnp.concatenate(rows, axis=0)
    lanes = lax.broadcasted_iota(jnp.int32, table.shape, 1)
    lines = lax.broadcasted_iota(jnp.int32, table.shape, 0)
    table = jnp.where(lanes < own_rows // 4 * PACK, table, 0.0)
    shift = PACK
    while shift < LANES:
        table = table + pltpu.roll(table, shift, 1)
        shift *= 2
    table = jnp.where(lanes // PACK == lines, table, 0.0)
    part_ref[...] = jnp.broadcast_to(jnp.sum(table, axis=0, keepdims=True), part_ref.shape)


def combine_kernel(
    parts_ref, scale_ref, u0_ref, u1_ref, u2_ref, w_ref, mass_sum_ref, lap_sum_ref, sol_hbm, res_hbm, sol, res, xs, xt, sems
):
    halves, modes, rows, _ = sol.shape
    groups = modes // PACK
    own = rows // 4
    per_half = LANES // 4
    total = jnp.sum(parts_ref[...], axis=0, keepdims=True)
    table = jnp.broadcast_to(total, (24, LANES))
    lanes = lax.broadcasted_iota(jnp.int32, table.shape, 1)
    lines = lax.broadcasted_iota(jnp.int32, table.shape, 0)
    table = jnp.where(lanes // PACK == lines, table, 0.0)
    shift = PACK
    while shift < LANES:
        table = table + pltpu.roll(table, shift, 1)
        shift *= 2
    b0, g00, g01, g11, g12, g22 = [table[q * groups : (q + 1) * groups] for q in range(6)]
    g02 = g11
    b1 = g00 - b0
    b2 = g01 - b1
    l10 = g01 / g00
    l20 = g02 / g00
    d1 = g11 - l10 * g01
    t12 = g12 - l20 * g01
    l21 = t12 / d1
    d2 = g22 - l20 * g02 - l21 * t12
    y1 = b1 - l10 * b0
    y2 = b2 - l20 * b0 - l21 * y1
    c2 = y2 / d2
    c1 = y1 / d1 - l21 * c2
    c0 = b0 / g00 - l10 * c1 - l20 * c2
    copies = []
    for half in range(halves):
        span = slice(half * per_half, (half + 1) * per_half)
        for group in range(groups):
            k0, k1, k2 = [c[group : group + 1, :] for c in (c0, c1, c2)]
            scale = scale_ref[group : group + 1, :]
            for a in range(4):
                slot = group * 4 + a
                for b in range(4):
                    p = plane(group, a, b)
                    u0, u1, u2 = u0_ref[p, span, :], u1_ref[p, span, :], u2_ref[p, span, :]
                    diag = mass_sum_ref[a * 4 + b, span, :] + scale * lap_sum_ref[a * 4 + b, span, :]
                    xs[0, slot, pl.ds(b, per_half, stride=4), :] = k0 * u0 + k1 * u1 + k2 * u2
                    xs[1, slot, pl.ds(b, per_half, stride=4), :] = (
                        diag * (u0 - k0 * (u1 + u0) - k1 * (u2 + u1)) - (k2 * scale) * w_ref[p, span, :]
                    )
                for i, out in enumerate((sol, res)):
                    xt[i, slot] = xs[i, slot].T
                    for m in range(PACK):
                        out[half, group * PACK + m, pl.ds(a, own, stride=4), :] = xt[
                            i, slot, pl.ds(m, own, stride=PACK), :
                        ]
        for i, (out, hbm) in enumerate(((sol, sol_hbm), (res, res_hbm))):
            copy = pltpu.make_async_copy(
                out.at[half], hbm.at[:, :, pl.ds(half * LANES, LANES)], sems.at[half, i]
            )
            copy.start()
            copies.append(copy)
    for copy in copies:
        copy.wait()


def shards(forcing, metric, jacobian, mode_scale):
    modes, rows, cols = forcing.shape
    groups = modes // PACK
    halo = 4 * GHOST
    f32 = jnp.float32

    def shift(x, axis, step):
        count = lax.axis_size(axis)
        return lax.ppermute(x, axis, [(i, (i + step) % count) for i in range(count)])

    vmem = pl.BlockSpec(memory_space=pltpu.VMEM)
    anywhere = pl.BlockSpec(memory_space=pl.ANY)
    hbm = pl.BlockSpec(memory_space=pltpu.HBM)
    top, bottom, shared = pl.pallas_call(
        strips_kernel,
        in_specs=[hbm] * 3,
        out_specs=[vmem] * 3,
        out_shape=[jax.ShapeDtypeStruct((modes + 2, halo, cols), f32)] * 2
        + [jax.ShapeDtypeStruct((2, rows, cols), f32)],
        scratch_shapes=[pltpu.SemaphoreType.DMA((3, 3))],
        compiler_params=pltpu.CompilerParams(vmem_limit_bytes=4 << 20),
        name="strips",
    )(forcing, metric, jacobian)
    up = shift(bottom, "curve", 1)
    down = shift(top, "curve", -1)

    planes = 16 * (groups + 1)
    ecols = cols // 4
    halves = cols // LANES
    per_half = LANES // 4
    whole = lambda *shape: pl.BlockSpec(shape, lambda h: (0,) * len(shape))
    spread, low, high = pl.pallas_call(
        functools.partial(spread_kernel, rows),
        grid=(halves,),
        in_specs=[
            pl.BlockSpec((modes, rows, LANES), lambda h: (0, 0, h)),
            pl.BlockSpec((2, rows, LANES), lambda h: (0, 0, h)),
            pl.BlockSpec((modes + 2, halo, LANES), lambda h: (0, 0, h)),
            pl.BlockSpec((modes + 2, halo, LANES), lambda h: (0, 0, h)),
        ],
        out_specs=[
            pl.BlockSpec((planes, per_half, LANES), lambda h: (0, h, 0)),
            whole(planes, GHOST, LANES),
            whole(planes, GHOST, LANES),
        ],
        out_shape=[
            jax.ShapeDtypeStruct((planes, ecols, LANES), f32),
            jax.ShapeDtypeStruct((planes, GHOST, LANES), f32),
            jax.ShapeDtypeStruct((planes, GHOST, LANES), f32),
        ],
        scratch_shapes=[pltpu.VMEM((planes // 4, LANES, LANES), f32)] * 2,
        compiler_params=pltpu.CompilerParams(vmem_limit_bytes=12 << 20),
        name="spread",
    )(forcing, shared, up, down)

    left = shift(high, "sub", 1)
    right = shift(low, "sub", -1)
    scale = jnp.tile(mode_scale.reshape(groups, PACK), (1, LANES // PACK))

    total = ecols + 2 * GHOST
    array = lambda *shape: jax.ShapeDtypeStruct(shape, f32)
    field = array(16 * groups, total, LANES)
    lines = array(24, total, LANES)
    nodes = array(16, total, LANES)
    state = pl.pallas_call(
        prep_kernel,
        in_specs=[vmem] * 2,
        out_specs=[vmem] * 10,
        out_shape=[field, lines, lines, nodes, nodes, field, field, field]
        + [array(16, total + 16, LANES), array(8 * groups, total + 16, LANES)],
        compiler_params=pltpu.CompilerParams(vmem_limit_bytes=20 << 20),
        cost_estimate=pl.CostEstimate(flops=20_000_000, bytes_accessed=0, transcendentals=0),
        name="prep",
    )(spread, scale)
    devices = lax.axis_size(AXES[0]) * lax.axis_size(AXES[1])
    out = pl.pallas_call(
        functools.partial(krylov_kernel, rows, ecols),
        in_specs=[vmem] * 13,
        out_specs=[vmem] * 13,
        out_shape=[array(*x.shape) for x in state] + [field, field, array(devices, LANES)],
        scratch_shapes=[pltpu.VMEM((8 * groups, total + 16, LANES), f32)],
        input_output_aliases={3 + i: i for i in range(10)},
        compiler_params=pltpu.CompilerParams(vmem_limit_bytes=24 << 20),
        name="krylov",
    )(right, left, scale, *state)
    mass_sum, lap_sum, u0, w3 = out[3], out[4], out[6], out[7]
    u1, u2, part = out[10:]

    parts = lax.all_to_all(part, AXES, 0, 0, tiled=True)

    out = jax.ShapeDtypeStruct((modes, rows, cols), f32)
    return tuple(
        pl.pallas_call(
            combine_kernel,
            in_specs=[vmem] * 8,
            out_specs=[anywhere] * 2,
            out_shape=[out] * 2,
            scratch_shapes=[
                pltpu.VMEM((halves, modes, rows, LANES), f32),
                pltpu.VMEM((halves, modes, rows, LANES), f32),
                pltpu.VMEM((2, 4 * groups, LANES, LANES), f32),
                pltpu.VMEM((2, 4 * groups, LANES, LANES), f32),
                pltpu.SemaphoreType.DMA((halves, 2)),
            ],
            compiler_params=pltpu.CompilerParams(vmem_limit_bytes=20 << 20),
            name="combine",
        )(parts, scale, u0, u1, u2, w3, mass_sum, lap_sum)
    )


def solution(mesh):
    in_specs = (P(None, "curve", "sub"), P("curve", "sub"), P("curve", "sub"), P())
    out_specs = (P(None, "curve", "sub"), P(None, "curve", "sub"))
    return jax.shard_map(
        shards, mesh=mesh, in_specs=in_specs, out_specs=out_specs, check_vma=False
    )
```

```python
import functools
import math

import jax
import jax.numpy as jnp
import numpy as np
from jax import lax
from jax.experimental import pallas as pl
from jax.experimental.pallas import tpu as pltpu
from jax.sharding import PartitionSpec as P

GHOST = 4
PACK = 4
LANES = 128
AXES = ("curve", "sub")
LOAD_LIMIT = 4 << 20


def gll_tables():
    points = np.array([-1.0, -1.0 / math.sqrt(5.0), 1.0 / math.sqrt(5.0), 1.0])
    weights = np.array([1.0 / 6.0, 5.0 / 6.0, 5.0 / 6.0, 1.0 / 6.0])
    factor = np.array(
        [np.prod([points[j] - points[m] for m in range(4) if m != j]) for j in range(4)]
    )
    slopes = np.zeros((4, 4))
    for i in range(4):
        for j in range(4):
            if i != j:
                slopes[i, j] = factor[i] / (factor[j] * (points[i] - points[j]))
        slopes[i, i] = sum((1.0 / (points[i] - points[m]) for m in range(4) if m != i))
    return (slopes, weights)


SLOPES, WEIGHTS = gll_tables()
PAIRS = [(a, k) for a in range(4) for k in range(a + 1, 4)]


def plane(group, a, b):
    return (group * 4 + a) * 4 + b


def load_kernel(f_hbm, metric_hbm, jacobian_hbm, scale_hbm, top, bottom, fields, scale_ref, scales, sems):
    modes, rows, _ = f_hbm.shape
    halo = top.shape[1]
    scale_copy = pltpu.make_async_copy(scale_hbm, scales, sems.at[3, 0])
    scale_copy.start()
    copies = []
    for part, (out, at, size) in enumerate(
        ((top, 0, halo), (bottom, rows - halo, halo), (fields, 0, rows))
    ):
        span = pl.ds(at, size)
        copies += [
            pltpu.make_async_copy(f_hbm.at[:, span, :], out.at[pl.ds(0, modes)], sems.at[part, 0]),
            pltpu.make_async_copy(metric_hbm.at[span, :], out.at[modes], sems.at[part, 1]),
            pltpu.make_async_copy(jacobian_hbm.at[span, :], out.at[modes + 1], sems.at[part, 2]),
        ]
    for copy in copies:
        copy.start()
    scale_copy.wait()
    member = lax.broadcasted_iota(jnp.int32, (1, LANES), 1) % PACK
    for group in range(modes // PACK):
        row = jnp.zeros((1, LANES), jnp.float32)
        for m in range(PACK):
            row = jnp.where(member == m, scales[group * PACK + m], row)
        scale_ref[group : group + 1, :] = row
    for copy in copies:
        copy.wait()


def spread_kernel(rows, f_ref, up_ref, down_ref, t_ref, low_ref, high_ref, xs, xt):
    half = pl.program_id(0)
    own = rows // 4
    groups = (f_ref.shape[0] - 2) // PACK
    per_half = LANES // 4
    for group in range(groups + 1):
        for a in range(4):
            at = group * 4 + a
            for m in range(PACK):
                index = group * PACK + (m if group < groups else m % 2)
                mine = f_ref[index, pl.ds(a, own, stride=4), :]
                xs[at, pl.ds(m, own, stride=PACK), :] = mine
                xs[at, pl.ds(own * PACK + m, GHOST, stride=PACK), :] = down_ref[
                    index, pl.ds(a, GHOST, stride=4), :
                ]
                xs[at, pl.ds((own + GHOST) * PACK + m, GHOST, stride=PACK), :] = up_ref[
                    index, pl.ds(a, GHOST, stride=4), :
                ]
            xt[at] = xs[at].T
            for b in range(4):
                t_ref[at * 4 + b] = xt[at, pl.ds(b, per_half, stride=4), :]

    @pl.when(half == 0)
    def _():
        for p in range(t_ref.shape[0]):
            low_ref[p] = t_ref[p, :GHOST, :]

    @pl.when(half == pl.num_programs(0) - 1)
    def _():
        for p in range(t_ref.shape[0]):
            high_ref[p] = t_ref[p, per_half - GHOST :, :]


def line_operator(coefs, values):
    f01, f02, f03, f12, f13, f23 = [
        coef * (values[k] - values[a]) for (a, k), coef in zip(PAIRS, coefs)
    ]
    return f01 + f02 + f03, f12 + f13 - f01, f23 - f02 - f12, f03 + f13 + f23


def tile(t):
    return pl.ds(pl.multiple_of(t * 8, 8), 8)


def spare(t):
    return pl.ds(pl.multiple_of(t * 8 + 8, 8), 8)


def join_rows(first, last):
    shared = last + pltpu.roll(first, LANES - PACK, 1)
    return pltpu.roll(shared, PACK, 1), shared


def join_cols(edge, i, total):
    edge[2 * i, total + 8 : total + 16, :] = edge[2 * i, 8:16, :]
    edge[2 * i + 1, 0:8, :] = edge[2 * i + 1, total : total + 8, :]
    first = edge[2 * i, 8 : total + 8, :] + edge[2 * i + 1, 7 : total + 7, :]
    last = edge[2 * i + 1, 8 : total + 8, :] + edge[2 * i, 9 : total + 9, :]
    return first, last


def prepare(t, fetch, scale_ref, mass_ref, krow, kcol, mass_sum_ref, lap_sum_ref, minv, u0_ref, source_ref, cedge, redge):
    groups = u0_ref.shape[0] // 16
    lane = lax.broadcasted_iota(jnp.int32, (8, LANES), 1)
    even = lane % 2 == 0
    grid = [(a, b) for a in range(4) for b in range(4)]
    scales = [scale_ref[group : group + 1, :] for group in range(groups)]
    flux, mass, lap = {}, {}, {}
    for a, b in grid:
        x = fetch(plane(groups, a, b))
        w = np.float32(WEIGHTS[a] * WEIGHTS[b])
        flux[a, b] = jnp.where(even, x, pltpu.roll(x, 1, 1)) * w
        mass[a, b] = jnp.where(even, pltpu.roll(x, LANES - 1, 1), x) * w
    for group in range(groups):
        inverse = 1.0 / scales[group]
        for a, b in grid:
            mass_ref[plane(group, a, b), tile(t), :] = mass[a, b] * inverse
            source_ref[plane(group, a, b), tile(t), :] = fetch(plane(group, a, b)) * mass[a, b]

    def less(a, b, value):
        lap[a, b] = lap[a, b] + value if (a, b) in lap else value

    for line in range(4):
        for i, (p, q) in enumerate(PAIRS):
            c = [np.float32(SLOPES[j, p] * SLOPES[j, q]) for j in range(4)]
            kr = sum(flux[j, line] * c[j] for j in range(4))
            kc = sum(flux[line, j] * c[j] for j in range(4))
            krow[line * 6 + i, tile(t), :] = kr
            kcol[line * 6 + i, tile(t), :] = kc
            less(p, line, kr)
            less(q, line, kr)
            less(line, p, kc)
            less(line, q, kc)
    for a, b in grid:
        lap[a, b] = -lap[a, b]
    for values, out, base in ((mass, mass_sum_ref, 0), (lap, lap_sum_ref, 4)):
        for b in range(4):
            values[0, b], values[3, b] = join_rows(values[0, b], values[3, b])
            for a in range(4):
                if b in (1, 2):
                    out[a * 4 + b, tile(t), :] = values[a, b]
                else:
                    cedge[2 * (base + a) + b // 3, spare(t), :] = values[a, b]
    for group in range(groups):
        for b in range(4):
            column = [source_ref[plane(group, a, b), tile(t), :] for a in range(4)]
            column[0], column[3] = join_rows(column[0], column[3])
            for a in range(4):
                p = plane(group, a, b)
                if b in (1, 2):
                    inverse = 1.0 / (mass[a, b] + scales[group] * lap[a, b])
                    u0_ref[p, tile(t), :] = column[a] * inverse
                    minv[p, tile(t), :] = inverse * scales[group]
                else:
                    redge[2 * (group * 4 + a) + b // 3, spare(t), :] = column[a]


def prep_kernel(t_ref, scale_ref, *refs):
    @pl.loop(0, t_ref.shape[1] // 8)
    def _(t):
        prepare(t, lambda p: t_ref[p, tile(t), :], scale_ref, *refs)


def krylov_kernel(own_rows, cols, right_ref, left_ref, scale_ref, *refs):
    state = refs[10:20]
    u1_ref, u2_ref, part_ref, edge = refs[20:]
    mass_ref, krow, kcol, mass_sum_ref, lap_sum_ref, minv, u0_ref, w_ref, cedge, redge = state
    groups = u0_ref.shape[0] // 16
    total = u0_ref.shape[1]
    tiles = total // 8
    own_tiles = cols // 8
    scales = [scale_ref[group : group + 1, :] for group in range(groups)]
    prepare(
        own_tiles, lambda p: jnp.concatenate([right_ref[p], left_ref[p]], axis=0), scale_ref, *state
    )

    @pl.loop(0, 4)
    def _(a):
        mass_sums = join_cols(cedge, a, total)
        lap_sums = join_cols(cedge, 4 + a, total)
        for side, b in enumerate((0, 3)):
            mass_sum_ref[a * 4 + b] = mass_sums[side]
            lap_sum_ref[a * 4 + b] = lap_sums[side]
        for group in range(groups):
            source = join_cols(redge, group * 4 + a, total)
            for side, b in enumerate((0, 3)):
                inverse = 1.0 / (mass_sums[side] + scales[group] * lap_sums[side])
                u0_ref[plane(group, a, b)] = source[side] * inverse
                minv[plane(group, a, b)] = inverse * scales[group]

    zero = jnp.zeros((8, LANES), jnp.float32)

    def apply(now_ref, old_ref, new_ref):
        def body(t, sums):
            sums = list(sums)
            own = (t < own_tiles).astype(jnp.float32)
            for group in range(groups):
                u = [[now_ref[plane(group, a, b), tile(t), :] for b in range(4)] for a in range(4)]
                along_rows = [
                    line_operator(
                        [krow[line * 6 + i, tile(t), :] for i in range(6)],
                        [u[a][line] for a in range(4)],
                    )
                    for line in range(4)
                ]
                along_cols = [
                    line_operator([kcol[line * 6 + i, tile(t), :] for i in range(6)], u[line])
                    for line in range(4)
                ]
                with_now, with_old = zero, zero
                y = [[None] * 4 for _ in range(4)]
                for a in range(4):
                    for b in range(4):
                        p = plane(group, a, b)
                        value = mass_ref[p, tile(t), :] * u[a][b]
                        row, col = along_rows[b][a], along_cols[a][b]
                        value = value - row if a == 3 else value + row
                        value = value - col if b == 3 else value + col
                        y[a][b] = value
                        with_now += u[a][b] * value
                        if old_ref is None:
                            with_old += w_ref[p, tile(t), :] * u[a][b]
                        else:
                            with_old += old_ref[p, tile(t), :] * value
                sums[group] += own * with_now
                sums[groups + group] += own * with_old
                for b in range(4):
                    column = [y[a][b] for a in range(4)]
                    column[0], column[3] = join_rows(column[0], column[3])
                    for a in range(4):
                        p = plane(group, a, b)
                        if b in (1, 2):
                            if new_ref is None:
                                w_ref[p, tile(t), :] = column[a]
                            else:
                                new_ref[p, tile(t), :] = column[a] * minv[p, tile(t), :] - u[a][b]
                        else:
                            edge[2 * (group * 4 + a) + b // 3, spare(t), :] = column[a]
            return tuple(sums)

        sums = lax.fori_loop(0, tiles, body, (zero,) * (2 * groups))

        @pl.loop(0, groups * 4)
        def _(i):
            for b, value in zip((0, 3), join_cols(edge, i, total)):
                p = i * 4 + b
                if new_ref is None:
                    w_ref[p] = value
                else:
                    new_ref[p] = value * minv[p] - now_ref[p]

        return sums[:groups], sums[groups:]

    g00, b0 = apply(u0_ref, None, u1_ref)
    g11, g01 = apply(u1_ref, u0_ref, u2_ref)
    g22, g12 = apply(u2_ref, u1_ref, None)
    rows = [jnp.sum(x, axis=0, keepdims=True) for x in b0]
    for q in (g00, g01, g11, g12, g22):
        rows += [scale * jnp.sum(x, axis=0, keepdims=True) for scale, x in zip(scales, q)]
    rows += [jnp.zeros((1, LANES), jnp.float32)] * (-len(rows) % 8)
    table = jnp.concatenate(rows, axis=0)
    lanes = lax.broadcasted_iota(jnp.int32, table.shape, 1)
    lines = lax.broadcasted_iota(jnp.int32, table.shape, 0)
    table = jnp.where(lanes < own_rows // 4 * PACK, table, 0.0)
    shift = PACK
    while shift < LANES:
        table = table + pltpu.roll(table, shift, 1)
        shift *= 2
    table = jnp.where(lanes // PACK == lines, table, 0.0)
    part_ref[...] = jnp.broadcast_to(jnp.sum(table, axis=0, keepdims=True), part_ref.shape)


def combine_kernel(
    parts_ref, scale_ref, u0_ref, u1_ref, u2_ref, w_ref, mass_sum_ref, lap_sum_ref, sol_hbm, res_hbm, sol, res, xs, xt, sems
):
    halves, modes, rows, _ = sol.shape
    groups = modes // PACK
    own = rows // 4
    per_half = LANES // 4
    total = jnp.sum(parts_ref[...], axis=0, keepdims=True)
    table = jnp.broadcast_to(total, (24, LANES))
    lanes = lax.broadcasted_iota(jnp.int32, table.shape, 1)
    lines = lax.broadcasted_iota(jnp.int32, table.shape, 0)
    table = jnp.where(lanes // PACK == lines, table, 0.0)
    shift = PACK
    while shift < LANES:
        table = table + pltpu.roll(table, shift, 1)
        shift *= 2
    b0, g00, g01, g11, g12, g22 = [table[q * groups : (q + 1) * groups] for q in range(6)]
    g02 = g11
    b1 = g00 - b0
    b2 = g01 - b1
    l10 = g01 / g00
    l20 = g02 / g00
    d1 = g11 - l10 * g01
    t12 = g12 - l20 * g01
    l21 = t12 / d1
    d2 = g22 - l20 * g02 - l21 * t12
    y1 = b1 - l10 * b0
    y2 = b2 - l20 * b0 - l21 * y1
    c2 = y2 / d2
    c1 = y1 / d1 - l21 * c2
    c0 = b0 / g00 - l10 * c1 - l20 * c2
    copies = []
    for half in range(halves):
        span = slice(half * per_half, (half + 1) * per_half)
        for group in range(groups):
            k0, k1, k2 = [c[group : group + 1, :] for c in (c0, c1, c2)]
            scale = scale_ref[group : group + 1, :]
            for a in range(4):
                slot = group * 4 + a
                for b in range(4):
                    p = plane(group, a, b)
                    u0, u1, u2 = u0_ref[p, span, :], u1_ref[p, span, :], u2_ref[p, span, :]
                    diag = mass_sum_ref[a * 4 + b, span, :] + scale * lap_sum_ref[a * 4 + b, span, :]
                    xs[0, slot, pl.ds(b, per_half, stride=4), :] = k0 * u0 + k1 * u1 + k2 * u2
                    xs[1, slot, pl.ds(b, per_half, stride=4), :] = (
                        diag * (u0 - k0 * (u1 + u0) - k1 * (u2 + u1)) - (k2 * scale) * w_ref[p, span, :]
                    )
                for i, out in enumerate((sol, res)):
                    xt[i, slot] = xs[i, slot].T
                    for m in range(PACK):
                        out[half, group * PACK + m, pl.ds(a, own, stride=4), :] = xt[
                            i, slot, pl.ds(m, own, stride=PACK), :
                        ]
            span_modes = pl.ds(group * PACK, PACK)
            for i, (out, hbm) in enumerate(((sol, sol_hbm), (res, res_hbm))):
                copy = pltpu.make_async_copy(
                    out.at[half, span_modes],
                    hbm.at[span_modes, :, pl.ds(half * LANES, LANES)],
                    sems.at[half, group, i],
                )
                copy.start()
                copies.append(copy)
    for copy in copies:
        copy.wait()


def shards(forcing, metric, jacobian, mode_scale):
    modes, rows, cols = forcing.shape
    groups = modes // PACK
    halo = 4 * GHOST
    f32 = jnp.float32

    def shift(x, axis, step):
        count = lax.axis_size(axis)
        return lax.ppermute(x, axis, [(i, (i + step) % count) for i in range(count)])

    vmem = pl.BlockSpec(memory_space=pltpu.VMEM)
    anywhere = pl.BlockSpec(memory_space=pl.ANY)
    array = lambda *shape: jax.ShapeDtypeStruct(shape, f32)
    top, bottom, fields, scale = pl.pallas_call(
        load_kernel,
        in_specs=[anywhere] * 4,
        out_specs=[vmem] * 4,
        out_shape=[array(modes + 2, halo, cols)] * 2
        + [array(modes + 2, rows, cols), array(groups, LANES)],
        scratch_shapes=[pltpu.SMEM((modes,), f32), pltpu.SemaphoreType.DMA((4, 3))],
        compiler_params=pltpu.CompilerParams(vmem_limit_bytes=LOAD_LIMIT),
        name="load",
    )(*[pltpu.with_memory_space_constraint(x, pltpu.HBM) for x in (forcing, metric, jacobian, mode_scale)])
    up = shift(bottom, "curve", 1)
    down = shift(top, "curve", -1)

    planes = 16 * (groups + 1)
    ecols = cols // 4
    halves = cols // LANES
    per_half = LANES // 4
    whole = lambda *shape: pl.BlockSpec(shape, lambda h: (0,) * len(shape))
    spread, low, high = pl.pallas_call(
        functools.partial(spread_kernel, rows),
        grid=(halves,),
        in_specs=[
            pl.BlockSpec((modes + 2, rows, LANES), lambda h: (0, 0, h)),
            pl.BlockSpec((modes + 2, halo, LANES), lambda h: (0, 0, h)),
            pl.BlockSpec((modes + 2, halo, LANES), lambda h: (0, 0, h)),
        ],
        out_specs=[
            pl.BlockSpec((planes, per_half, LANES), lambda h: (0, h, 0)),
            whole(planes, GHOST, LANES),
            whole(planes, GHOST, LANES),
        ],
        out_shape=[
            jax.ShapeDtypeStruct((planes, ecols, LANES), f32),
            jax.ShapeDtypeStruct((planes, GHOST, LANES), f32),
            jax.ShapeDtypeStruct((planes, GHOST, LANES), f32),
        ],
        scratch_shapes=[pltpu.VMEM((planes // 4, LANES, LANES), f32)] * 2,
        compiler_params=pltpu.CompilerParams(vmem_limit_bytes=12 << 20),
        name="spread",
    )(fields, up, down)

    left = shift(high, "sub", 1)
    right = shift(low, "sub", -1)

    total = ecols + 2 * GHOST
    field = array(16 * groups, total, LANES)
    lines = array(24, total, LANES)
    nodes = array(16, total, LANES)
    state = pl.pallas_call(
        prep_kernel,
        in_specs=[vmem] * 2,
        out_specs=[vmem] * 10,
        out_shape=[field, lines, lines, nodes, nodes, field, field, field]
        + [array(16, total + 16, LANES), array(8 * groups, total + 16, LANES)],
        compiler_params=pltpu.CompilerParams(vmem_limit_bytes=20 << 20),
        cost_estimate=pl.CostEstimate(flops=20_000_000, bytes_accessed=0, transcendentals=0),
        name="prep",
    )(spread, scale)
    devices = lax.axis_size(AXES[0]) * lax.axis_size(AXES[1])
    out = pl.pallas_call(
        functools.partial(krylov_kernel, rows, ecols),
        in_specs=[vmem] * 13,
        out_specs=[vmem] * 13,
        out_shape=[array(*x.shape) for x in state] + [field, field, array(devices, LANES)],
        scratch_shapes=[pltpu.VMEM((8 * groups, total + 16, LANES), f32)],
        input_output_aliases={3 + i: i for i in range(10)},
        compiler_params=pltpu.CompilerParams(vmem_limit_bytes=24 << 20),
        name="krylov",
    )(right, left, scale, *state)
    mass_sum, lap_sum, u0, w3 = out[3], out[4], out[6], out[7]
    u1, u2, part = out[10:]

    parts = lax.all_to_all(part, AXES, 0, 0, tiled=True)

    out = jax.ShapeDtypeStruct((modes, rows, cols), f32)
    return tuple(
        pl.pallas_call(
            combine_kernel,
            in_specs=[vmem] * 8,
            out_specs=[anywhere] * 2,
            out_shape=[out] * 2,
            scratch_shapes=[
                pltpu.VMEM((halves, modes, rows, LANES), f32),
                pltpu.VMEM((halves, modes, rows, LANES), f32),
                pltpu.VMEM((2, 4 * groups, LANES, LANES), f32),
                pltpu.VMEM((2, 4 * groups, LANES, LANES), f32),
                pltpu.SemaphoreType.DMA((halves, groups, 2)),
            ],
            compiler_params=pltpu.CompilerParams(vmem_limit_bytes=20 << 20),
            name="combine",
        )(parts, scale, u0, u1, u2, w3, mass_sum, lap_sum)
    )


def solution(mesh):
    in_specs = (P(None, "curve", "sub"), P("curve", "sub"), P("curve", "sub"), P())
    out_specs = (P(None, "curve", "sub"), P(None, "curve", "sub"))
    return jax.shard_map(
        shards, mesh=mesh, in_specs=in_specs, out_specs=out_specs, check_vma=False
    )
```

```python
import functools
import math

import jax
import jax.numpy as jnp
import numpy as np
from jax import lax
from jax.experimental import pallas as pl
from jax.experimental.pallas import tpu as pltpu
from jax.sharding import PartitionSpec as P

GHOST = 4
PACK = 4
LANES = 128
AXES = ("curve", "sub")
LOAD_LIMIT = 4 << 20


def gll_tables():
    points = np.array([-1.0, -1.0 / math.sqrt(5.0), 1.0 / math.sqrt(5.0), 1.0])
    weights = np.array([1.0 / 6.0, 5.0 / 6.0, 5.0 / 6.0, 1.0 / 6.0])
    factor = np.array(
        [np.prod([points[j] - points[m] for m in range(4) if m != j]) for j in range(4)]
    )
    slopes = np.zeros((4, 4))
    for i in range(4):
        for j in range(4):
            if i != j:
                slopes[i, j] = factor[i] / (factor[j] * (points[i] - points[j]))
        slopes[i, i] = sum((1.0 / (points[i] - points[m]) for m in range(4) if m != i))
    return (slopes, weights)


SLOPES, WEIGHTS = gll_tables()
PAIRS = [(a, k) for a in range(4) for k in range(a + 1, 4)]


def plane(group, a, b):
    return (group * 4 + a) * 4 + b


def load_kernel(f_hbm, metric_hbm, jacobian_hbm, scale_hbm, top, bottom, fields, scale_ref, scales, sems):
    modes, rows, _ = f_hbm.shape
    halo = top.shape[1]
    scale_copy = pltpu.make_async_copy(scale_hbm, scales, sems.at[3, 0])
    scale_copy.start()
    copies = []
    for part, (out, at, size) in enumerate(
        ((top, 0, halo), (bottom, rows - halo, halo), (fields, 0, rows))
    ):
        span = pl.ds(at, size)
        copies += [
            pltpu.make_async_copy(f_hbm.at[:, span, :], out.at[pl.ds(0, modes)], sems.at[part, 0]),
            pltpu.make_async_copy(metric_hbm.at[span, :], out.at[modes], sems.at[part, 1]),
            pltpu.make_async_copy(jacobian_hbm.at[span, :], out.at[modes + 1], sems.at[part, 2]),
        ]
    for copy in copies:
        copy.start()
    scale_copy.wait()
    member = lax.broadcasted_iota(jnp.int32, (1, LANES), 1) % PACK
    for group in range(modes // PACK):
        row = jnp.zeros((1, LANES), jnp.float32)
        for m in range(PACK):
            row = jnp.where(member == m, scales[group * PACK + m], row)
        scale_ref[group : group + 1, :] = row
    for copy in copies:
        copy.wait()


def spread_kernel(rows, f_ref, up_ref, down_ref, t_ref, low_ref, high_ref, xs, xt):
    half = pl.program_id(0)
    own = rows // 4
    groups = (f_ref.shape[0] - 2) // PACK
    per_half = LANES // 4
    for group in range(groups + 1):
        for a in range(4):
            at = group * 4 + a
            for m in range(PACK):
                index = group * PACK + (m if group < groups else m % 2)
                mine = f_ref[index, pl.ds(a, own, stride=4), :]
                xs[at, pl.ds(m, own, stride=PACK), :] = mine
                xs[at, pl.ds(own * PACK + m, GHOST, stride=PACK), :] = down_ref[
                    index, pl.ds(a, GHOST, stride=4), :
                ]
                xs[at, pl.ds((own + GHOST) * PACK + m, GHOST, stride=PACK), :] = up_ref[
                    index, pl.ds(a, GHOST, stride=4), :
                ]
            xt[at] = xs[at].T
            for b in range(4):
                t_ref[at * 4 + b] = xt[at, pl.ds(b, per_half, stride=4), :]

    @pl.when(half == 0)
    def _():
        for p in range(t_ref.shape[0]):
            low_ref[p] = t_ref[p, :GHOST, :]

    @pl.when(half == pl.num_programs(0) - 1)
    def _():
        for p in range(t_ref.shape[0]):
            high_ref[p] = t_ref[p, per_half - GHOST :, :]


def line_operator(coefs, values):
    f01, f02, f03, f12, f13, f23 = [
        coef * (values[k] - values[a]) for (a, k), coef in zip(PAIRS, coefs)
    ]
    return f01 + f02 + f03, f12 + f13 - f01, f23 - f02 - f12, f03 + f13 + f23


def tile(t):
    return pl.ds(pl.multiple_of(t * 8, 8), 8)


def spare(t):
    return pl.ds(pl.multiple_of(t * 8 + 8, 8), 8)


def join_rows(first, last):
    shared = last + pltpu.roll(first, LANES - PACK, 1)
    return pltpu.roll(shared, PACK, 1), shared


def wrap_cols(edge, i, total):
    edge[2 * i, total + 8 : total + 16, :] = edge[2 * i, 8:16, :]
    edge[2 * i + 1, 0:8, :] = edge[2 * i + 1, total : total + 8, :]


def join_cols(edge, i, low, high):
    first = edge[2 * i, low + 8 : high + 8, :] + edge[2 * i + 1, low + 7 : high + 7, :]
    last = edge[2 * i + 1, low + 8 : high + 8, :] + edge[2 * i, low + 9 : high + 9, :]
    return first, last


def prepare(t, fetch, scale_ref, mass_ref, krow, kcol, mass_sum_ref, lap_sum_ref, minv, u0_ref, source_ref, cedge, redge):
    groups = u0_ref.shape[0] // 16
    lane = lax.broadcasted_iota(jnp.int32, (8, LANES), 1)
    even = lane % 2 == 0
    grid = [(a, b) for a in range(4) for b in range(4)]
    scales = [scale_ref[group : group + 1, :] for group in range(groups)]
    flux, mass, lap = {}, {}, {}
    for a, b in grid:
        x = fetch(plane(groups, a, b))
        w = np.float32(WEIGHTS[a] * WEIGHTS[b])
        flux[a, b] = jnp.where(even, x, pltpu.roll(x, 1, 1)) * w
        mass[a, b] = jnp.where(even, pltpu.roll(x, LANES - 1, 1), x) * w
    for group in range(groups):
        inverse = 1.0 / scales[group]
        for a, b in grid:
            mass_ref[plane(group, a, b), tile(t), :] = mass[a, b] * inverse
            source_ref[plane(group, a, b), tile(t), :] = fetch(plane(group, a, b)) * mass[a, b]

    def less(a, b, value):
        lap[a, b] = lap[a, b] + value if (a, b) in lap else value

    for line in range(4):
        for i, (p, q) in enumerate(PAIRS):
            c = [np.float32(SLOPES[j, p] * SLOPES[j, q]) for j in range(4)]
            kr = sum(flux[j, line] * c[j] for j in range(4))
            kc = sum(flux[line, j] * c[j] for j in range(4))
            krow[line * 6 + i, tile(t), :] = kr
            kcol[line * 6 + i, tile(t), :] = kc
            less(p, line, kr)
            less(q, line, kr)
            less(line, p, kc)
            less(line, q, kc)
    for a, b in grid:
        lap[a, b] = -lap[a, b]
    for values, out, base in ((mass, mass_sum_ref, 0), (lap, lap_sum_ref, 4)):
        for b in range(4):
            values[0, b], values[3, b] = join_rows(values[0, b], values[3, b])
            for a in range(4):
                if b in (1, 2):
                    out[a * 4 + b, tile(t), :] = values[a, b]
                else:
                    cedge[2 * (base + a) + b // 3, spare(t), :] = values[a, b]
    for group in range(groups):
        for b in range(4):
            column = [source_ref[plane(group, a, b), tile(t), :] for a in range(4)]
            column[0], column[3] = join_rows(column[0], column[3])
            for a in range(4):
                p = plane(group, a, b)
                if b in (1, 2):
                    inverse = 1.0 / (mass[a, b] + scales[group] * lap[a, b])
                    u0_ref[p, tile(t), :] = column[a] * inverse
                    minv[p, tile(t), :] = inverse * scales[group]
                else:
                    redge[2 * (group * 4 + a) + b // 3, spare(t), :] = column[a]


def finish(a, low, high, scale_ref, mass_sum_ref, lap_sum_ref, minv, u0_ref, cedge, redge):
    groups = u0_ref.shape[0] // 16
    span = slice(low, high)
    mass_sums = join_cols(cedge, a, low, high)
    lap_sums = join_cols(cedge, 4 + a, low, high)
    for side, b in enumerate((0, 3)):
        mass_sum_ref[a * 4 + b, span, :] = mass_sums[side]
        lap_sum_ref[a * 4 + b, span, :] = lap_sums[side]
    for group in range(groups):
        scale = scale_ref[group : group + 1, :]
        source = join_cols(redge, group * 4 + a, low, high)
        for side, b in enumerate((0, 3)):
            inverse = 1.0 / (mass_sums[side] + scale * lap_sums[side])
            u0_ref[plane(group, a, b), span, :] = source[side] * inverse
            minv[plane(group, a, b), span, :] = inverse * scale


def operator_tile(t, own, sums, now_ref, old_ref, new_ref, mass_ref, krow, kcol, minv, w_ref, edge):
    groups = now_ref.shape[0] // 16
    zero = jnp.zeros((8, LANES), jnp.float32)
    sums = list(sums)
    for group in range(groups):
        u = [[now_ref[plane(group, a, b), tile(t), :] for b in range(4)] for a in range(4)]
        along_rows = [
            line_operator(
                [krow[line * 6 + i, tile(t), :] for i in range(6)], [u[a][line] for a in range(4)]
            )
            for line in range(4)
        ]
        along_cols = [
            line_operator([kcol[line * 6 + i, tile(t), :] for i in range(6)], u[line])
            for line in range(4)
        ]
        with_now, with_old = zero, zero
        y = [[None] * 4 for _ in range(4)]
        for a in range(4):
            for b in range(4):
                p = plane(group, a, b)
                value = mass_ref[p, tile(t), :] * u[a][b]
                row, col = along_rows[b][a], along_cols[a][b]
                value = value - row if a == 3 else value + row
                value = value - col if b == 3 else value + col
                y[a][b] = value
                with_now += u[a][b] * value
                if old_ref is None:
                    with_old += w_ref[p, tile(t), :] * u[a][b]
                else:
                    with_old += old_ref[p, tile(t), :] * value
        sums[group] += with_now if own is None else own * with_now
        sums[groups + group] += with_old if own is None else own * with_old
        for b in range(4):
            column = [y[a][b] for a in range(4)]
            column[0], column[3] = join_rows(column[0], column[3])
            for a in range(4):
                p = plane(group, a, b)
                if b in (1, 2):
                    if new_ref is None:
                        w_ref[p, tile(t), :] = column[a]
                    else:
                        new_ref[p, tile(t), :] = column[a] * minv[p, tile(t), :] - u[a][b]
                else:
                    edge[2 * (group * 4 + a) + b // 3, spare(t), :] = column[a]
    return tuple(sums)


def prep_kernel(t_ref, scale_ref, *refs):
    state, (u1_ref, edge, sums_ref) = refs[:10], refs[10:]
    mass_ref, krow, kcol, mass_sum_ref, lap_sum_ref, minv, u0_ref, w_ref, cedge, redge = state
    cols = t_ref.shape[1]

    @pl.loop(0, cols // 8)
    def _(t):
        prepare(t, lambda p: t_ref[p, tile(t), :], scale_ref, *state)

    @pl.loop(0, 4)
    def _(a):
        finish(a, 8, cols - 8, scale_ref, mass_sum_ref, lap_sum_ref, minv, u0_ref, cedge, redge)

    zero = jnp.zeros((8, LANES), jnp.float32)
    sums = lax.fori_loop(
        1,
        cols // 8 - 1,
        lambda t, sums: operator_tile(
            t, None, sums, u0_ref, None, u1_ref, mass_ref, krow, kcol, minv, w_ref, edge
        ),
        (zero,) * sums_ref.shape[0],
    )
    for i, value in enumerate(sums):
        sums_ref[i] = value


def krylov_kernel(own_rows, cols, count, right_ref, left_ref, scale_ref, *refs):
    state = refs[count : count + 10]
    u1_ref, edge, sums_ref, u2_ref, part_ref = refs[count + 10 :]
    mass_ref, krow, kcol, mass_sum_ref, lap_sum_ref, minv, u0_ref, w_ref, cedge, redge = state
    groups = u0_ref.shape[0] // 16
    total = u0_ref.shape[1]
    tiles = total // 8
    own_tiles = cols // 8
    scales = [scale_ref[group : group + 1, :] for group in range(groups)]
    prepare(
        own_tiles, lambda p: jnp.concatenate([right_ref[p], left_ref[p]], axis=0), scale_ref, *state
    )

    @pl.loop(0, 4)
    def _(a):
        wrap_cols(cedge, a, total)
        wrap_cols(cedge, 4 + a, total)
        for group in range(groups):
            wrap_cols(redge, group * 4 + a, total)
        for low, high in ((0, 8), (cols - 8, total)):
            finish(a, low, high, scale_ref, mass_sum_ref, lap_sum_ref, minv, u0_ref, cedge, redge)

    zero = jnp.zeros((8, LANES), jnp.float32)
    shared = (mass_ref, krow, kcol, minv, w_ref, edge)

    def apply(now_ref, old_ref, new_ref):
        def body(i, sums):
            if old_ref is None:
                t = jnp.where(i == 0, 0, i + own_tiles - 2)
            else:
                t = i
            own = (t < own_tiles).astype(jnp.float32)
            return operator_tile(t, own, sums, now_ref, old_ref, new_ref, *shared)

        if old_ref is None:
            sums = lax.fori_loop(0, 3, body, tuple(sums_ref[i] for i in range(2 * groups)))
        else:
            sums = lax.fori_loop(0, tiles, body, (zero,) * (2 * groups))

        @pl.loop(0, groups * 4)
        def _(i):
            wrap_cols(edge, i, total)
            for b, value in zip((0, 3), join_cols(edge, i, 0, total)):
                p = i * 4 + b
                if new_ref is None:
                    w_ref[p] = value
                else:
                    new_ref[p] = value * minv[p] - now_ref[p]

        return sums[:groups], sums[groups:]

    g00, b0 = apply(u0_ref, None, u1_ref)
    g11, g01 = apply(u1_ref, u0_ref, u2_ref)
    g22, g12 = apply(u2_ref, u1_ref, None)
    rows = [jnp.sum(x, axis=0, keepdims=True) for x in b0]
    for q in (g00, g01, g11, g12, g22):
        rows += [scale * jnp.sum(x, axis=0, keepdims=True) for scale, x in zip(scales, q)]
    rows += [jnp.zeros((1, LANES), jnp.float32)] * (-len(rows) % 8)
    table = jnp.concatenate(rows, axis=0)
    lanes = lax.broadcasted_iota(jnp.int32, table.shape, 1)
    lines = lax.broadcasted_iota(jnp.int32, table.shape, 0)
    table = jnp.where(lanes < own_rows // 4 * PACK, table, 0.0)
    shift = PACK
    while shift < LANES:
        table = table + pltpu.roll(table, shift, 1)
        shift *= 2
    table = jnp.where(lanes // PACK == lines, table, 0.0)
    part_ref[...] = jnp.broadcast_to(jnp.sum(table, axis=0, keepdims=True), part_ref.shape)


def combine_kernel(
    parts_ref, scale_ref, u0_ref, u1_ref, u2_ref, w_ref, mass_sum_ref, lap_sum_ref, sol_hbm, res_hbm, sol, res, xs, xt, sems
):
    halves, modes, rows, _ = sol.shape
    groups = modes // PACK
    own = rows // 4
    per_half = LANES // 4
    total = jnp.sum(parts_ref[...], axis=0, keepdims=True)
    table = jnp.broadcast_to(total, (24, LANES))
    lanes = lax.broadcasted_iota(jnp.int32, table.shape, 1)
    lines = lax.broadcasted_iota(jnp.int32, table.shape, 0)
    table = jnp.where(lanes // PACK == lines, table, 0.0)
    shift = PACK
    while shift < LANES:
        table = table + pltpu.roll(table, shift, 1)
        shift *= 2
    b0, g00, g01, g11, g12, g22 = [table[q * groups : (q + 1) * groups] for q in range(6)]
    g02 = g11
    b1 = g00 - b0
    b2 = g01 - b1
    l10 = g01 / g00
    l20 = g02 / g00
    d1 = g11 - l10 * g01
    t12 = g12 - l20 * g01
    l21 = t12 / d1
    d2 = g22 - l20 * g02 - l21 * t12
    y1 = b1 - l10 * b0
    y2 = b2 - l20 * b0 - l21 * y1
    c2 = y2 / d2
    c1 = y1 / d1 - l21 * c2
    c0 = b0 / g00 - l10 * c1 - l20 * c2
    copies = []
    for half in range(halves):
        span = slice(half * per_half, (half + 1) * per_half)
        for group in range(groups):
            k0, k1, k2 = [c[group : group + 1, :] for c in (c0, c1, c2)]
            scale = scale_ref[group : group + 1, :]
            for a in range(4):
                slot = group * 4 + a
                for b in range(4):
                    p = plane(group, a, b)
                    u0, u1, u2 = u0_ref[p, span, :], u1_ref[p, span, :], u2_ref[p, span, :]
                    diag = mass_sum_ref[a * 4 + b, span, :] + scale * lap_sum_ref[a * 4 + b, span, :]
                    xs[0, slot, pl.ds(b, per_half, stride=4), :] = k0 * u0 + k1 * u1 + k2 * u2
                    xs[1, slot, pl.ds(b, per_half, stride=4), :] = (
                        diag * (u0 - k0 * (u1 + u0) - k1 * (u2 + u1)) - (k2 * scale) * w_ref[p, span, :]
                    )
                for i, out in enumerate((sol, res)):
                    xt[i, slot] = xs[i, slot].T
                    for m in range(PACK):
                        out[half, group * PACK + m, pl.ds(a, own, stride=4), :] = xt[
                            i, slot, pl.ds(m, own, stride=PACK), :
                        ]
            span_modes = pl.ds(group * PACK, PACK)
            for i, (out, hbm) in enumerate(((sol, sol_hbm), (res, res_hbm))):
                copy = pltpu.make_async_copy(
                    out.at[half, span_modes],
                    hbm.at[span_modes, :, pl.ds(half * LANES, LANES)],
                    sems.at[half, group, i],
                )
                copy.start()
                copies.append(copy)
    for copy in copies:
        copy.wait()


def shards(forcing, metric, jacobian, mode_scale):
    modes, rows, cols = forcing.shape
    groups = modes // PACK
    halo = 4 * GHOST
    f32 = jnp.float32

    def shift(x, axis, step):
        count = lax.axis_size(axis)
        return lax.ppermute(x, axis, [(i, (i + step) % count) for i in range(count)])

    vmem = pl.BlockSpec(memory_space=pltpu.VMEM)
    anywhere = pl.BlockSpec(memory_space=pl.ANY)
    array = lambda *shape: jax.ShapeDtypeStruct(shape, f32)
    top, bottom, fields, scale = pl.pallas_call(
        load_kernel,
        in_specs=[anywhere] * 4,
        out_specs=[vmem] * 4,
        out_shape=[array(modes + 2, halo, cols)] * 2
        + [array(modes + 2, rows, cols), array(groups, LANES)],
        scratch_shapes=[pltpu.SMEM((modes,), f32), pltpu.SemaphoreType.DMA((4, 3))],
        compiler_params=pltpu.CompilerParams(vmem_limit_bytes=LOAD_LIMIT),
        name="load",
    )(*[pltpu.with_memory_space_constraint(x, pltpu.HBM) for x in (forcing, metric, jacobian, mode_scale)])
    up = shift(bottom, "curve", 1)
    down = shift(top, "curve", -1)

    planes = 16 * (groups + 1)
    ecols = cols // 4
    halves = cols // LANES
    per_half = LANES // 4
    whole = lambda *shape: pl.BlockSpec(shape, lambda h: (0,) * len(shape))
    spread, low, high = pl.pallas_call(
        functools.partial(spread_kernel, rows),
        grid=(halves,),
        in_specs=[
            pl.BlockSpec((modes + 2, rows, LANES), lambda h: (0, 0, h)),
            pl.BlockSpec((modes + 2, halo, LANES), lambda h: (0, 0, h)),
            pl.BlockSpec((modes + 2, halo, LANES), lambda h: (0, 0, h)),
        ],
        out_specs=[
            pl.BlockSpec((planes, per_half, LANES), lambda h: (0, h, 0)),
            whole(planes, GHOST, LANES),
            whole(planes, GHOST, LANES),
        ],
        out_shape=[
            jax.ShapeDtypeStruct((planes, ecols, LANES), f32),
            jax.ShapeDtypeStruct((planes, GHOST, LANES), f32),
            jax.ShapeDtypeStruct((planes, GHOST, LANES), f32),
        ],
        scratch_shapes=[pltpu.VMEM((planes // 4, LANES, LANES), f32)] * 2,
        compiler_params=pltpu.CompilerParams(vmem_limit_bytes=12 << 20),
        name="spread",
    )(fields, up, down)

    left = shift(high, "sub", 1)
    right = shift(low, "sub", -1)

    total = ecols + 2 * GHOST
    field = array(16 * groups, total, LANES)
    lines = array(24, total, LANES)
    nodes = array(16, total, LANES)
    state = pl.pallas_call(
        prep_kernel,
        in_specs=[vmem] * 2,
        out_specs=[vmem] * 13,
        out_shape=[field, lines, lines, nodes, nodes, field, field, field]
        + [array(16, total + 16, LANES), array(8 * groups, total + 16, LANES)]
        + [field, array(8 * groups, total + 16, LANES), array(2 * groups, 8, LANES)],
        compiler_params=pltpu.CompilerParams(vmem_limit_bytes=24 << 20),
        cost_estimate=pl.CostEstimate(flops=20_000_000, bytes_accessed=0, transcendentals=0),
        name="prep",
    )(spread, scale)
    devices = lax.axis_size(AXES[0]) * lax.axis_size(AXES[1])
    count = len(state)
    out = pl.pallas_call(
        functools.partial(krylov_kernel, rows, ecols, count),
        in_specs=[vmem] * (3 + count),
        out_specs=[vmem] * (count + 2),
        out_shape=[array(*x.shape) for x in state] + [field, array(devices, LANES)],
        input_output_aliases={3 + i: i for i in range(count)},
        compiler_params=pltpu.CompilerParams(vmem_limit_bytes=24 << 20),
        name="krylov",
    )(right, left, scale, *state)
    mass_sum, lap_sum, u0, w3, u1 = out[3], out[4], out[6], out[7], out[10]
    u2, part = out[count:]

    parts = lax.all_to_all(part, AXES, 0, 0, tiled=True)

    out = jax.ShapeDtypeStruct((modes, rows, cols), f32)
    return tuple(
        pl.pallas_call(
            combine_kernel,
            in_specs=[vmem] * 8,
            out_specs=[anywhere] * 2,
            out_shape=[out] * 2,
            scratch_shapes=[
                pltpu.VMEM((halves, modes, rows, LANES), f32),
                pltpu.VMEM((halves, modes, rows, LANES), f32),
                pltpu.VMEM((2, 4 * groups, LANES, LANES), f32),
                pltpu.VMEM((2, 4 * groups, LANES, LANES), f32),
                pltpu.SemaphoreType.DMA((halves, groups, 2)),
            ],
            compiler_params=pltpu.CompilerParams(vmem_limit_bytes=20 << 20),
            name="combine",
        )(parts, scale, u0, u1, u2, w3, mass_sum, lap_sum)
    )


def solution(mesh):
    in_specs = (P(None, "curve", "sub"), P("curve", "sub"), P("curve", "sub"), P())
    out_specs = (P(None, "curve", "sub"), P(None, "curve", "sub"))
    return jax.shard_map(
        shards, mesh=mesh, in_specs=in_specs, out_specs=out_specs, check_vma=False
    )
```

```python
import functools
import math

import jax
import jax.numpy as jnp
import numpy as np
from jax import lax
from jax.experimental import pallas as pl
from jax.experimental.pallas import tpu as pltpu
from jax.sharding import PartitionSpec as P

GHOST = 4
PACK = 4
LANES = 128
AXES = ("curve", "sub")
LOAD_LIMIT = 4 << 20


def gll_tables():
    points = np.array([-1.0, -1.0 / math.sqrt(5.0), 1.0 / math.sqrt(5.0), 1.0])
    weights = np.array([1.0 / 6.0, 5.0 / 6.0, 5.0 / 6.0, 1.0 / 6.0])
    factor = np.array(
        [np.prod([points[j] - points[m] for m in range(4) if m != j]) for j in range(4)]
    )
    slopes = np.zeros((4, 4))
    for i in range(4):
        for j in range(4):
            if i != j:
                slopes[i, j] = factor[i] / (factor[j] * (points[i] - points[j]))
        slopes[i, i] = sum((1.0 / (points[i] - points[m]) for m in range(4) if m != i))
    return (slopes, weights)


SLOPES, WEIGHTS = gll_tables()
PAIRS = [(a, k) for a in range(4) for k in range(a + 1, 4)]


def plane(group, a, b):
    return (group * 4 + a) * 4 + b


def load_kernel(f_hbm, metric_hbm, jacobian_hbm, scale_hbm, top, bottom, fields, scale_ref, scales, sems):
    modes, rows, _ = f_hbm.shape
    halo = top.shape[1]
    scale_copy = pltpu.make_async_copy(scale_hbm, scales, sems.at[3, 0])
    scale_copy.start()
    copies = []
    for part, (out, at, size) in enumerate(
        ((top, 0, halo), (bottom, rows - halo, halo), (fields, 0, rows))
    ):
        span = pl.ds(at, size)
        copies += [
            pltpu.make_async_copy(f_hbm.at[:, span, :], out.at[pl.ds(0, modes)], sems.at[part, 0]),
            pltpu.make_async_copy(metric_hbm.at[span, :], out.at[modes], sems.at[part, 1]),
            pltpu.make_async_copy(jacobian_hbm.at[span, :], out.at[modes + 1], sems.at[part, 2]),
        ]
    for copy in copies:
        copy.start()
    scale_copy.wait()
    member = lax.broadcasted_iota(jnp.int32, (1, LANES), 1) % PACK
    for group in range(modes // PACK):
        row = jnp.zeros((1, LANES), jnp.float32)
        for m in range(PACK):
            row = jnp.where(member == m, scales[group * PACK + m], row)
        scale_ref[group : group + 1, :] = row
    for copy in copies:
        copy.wait()


def spread_kernel(rows, f_ref, up_ref, down_ref, t_ref, low_ref, high_ref, xs, xt):
    half = pl.program_id(0)
    own = rows // 4
    groups = (f_ref.shape[0] - 2) // PACK
    per_half = LANES // 4
    for group in range(groups + 1):
        for a in range(4):
            at = group * 4 + a
            for m in range(PACK):
                index = group * PACK + (m if group < groups else m % 2)
                mine = f_ref[index, pl.ds(a, own, stride=4), :]
                xs[at, pl.ds(m, own, stride=PACK), :] = mine
                xs[at, pl.ds(own * PACK + m, GHOST, stride=PACK), :] = down_ref[
                    index, pl.ds(a, GHOST, stride=4), :
                ]
                xs[at, pl.ds((own + GHOST) * PACK + m, GHOST, stride=PACK), :] = up_ref[
                    index, pl.ds(a, GHOST, stride=4), :
                ]
            xt[at] = xs[at].T
            for b in range(4):
                t_ref[at * 4 + b] = xt[at, pl.ds(b, per_half, stride=4), :]

    @pl.when(half == 0)
    def _():
        for p in range(t_ref.shape[0]):
            low_ref[p] = t_ref[p, :GHOST, :]

    @pl.when(half == pl.num_programs(0) - 1)
    def _():
        for p in range(t_ref.shape[0]):
            high_ref[p] = t_ref[p, per_half - GHOST :, :]


def line_operator(coefs, values):
    f01, f02, f03, f12, f13, f23 = [
        coef * (values[k] - values[a]) for (a, k), coef in zip(PAIRS, coefs)
    ]
    return f01 + f02 + f03, f12 + f13 - f01, f23 - f02 - f12, f03 + f13 + f23


def over_rows(table):
    i = lax.broadcasted_iota(jnp.int32, (LANES, LANES), 0)
    j = lax.broadcasted_iota(jnp.int32, (LANES, LANES), 1)
    same = jnp.where(i % PACK == j % PACK, 1.0, 0.0).astype(jnp.float32)
    return jnp.dot(
        table, same, precision=lax.Precision.HIGHEST, preferred_element_type=jnp.float32
    )


def tile(t):
    return pl.ds(pl.multiple_of(t * 8, 8), 8)


def spare(t):
    return pl.ds(pl.multiple_of(t * 8 + 8, 8), 8)


def join_rows(first, last):
    shared = last + pltpu.roll(first, LANES - PACK, 1)
    return pltpu.roll(shared, PACK, 1), shared


def wrap_cols(edge, i, total):
    edge[2 * i, total + 8 : total + 16, :] = edge[2 * i, 8:16, :]
    edge[2 * i + 1, 0:8, :] = edge[2 * i + 1, total : total + 8, :]


def join_cols(edge, i, low, high):
    first = edge[2 * i, low + 8 : high + 8, :] + edge[2 * i + 1, low + 7 : high + 7, :]
    last = edge[2 * i + 1, low + 8 : high + 8, :] + edge[2 * i, low + 9 : high + 9, :]
    return first, last


def prepare(t, fetch, scale_ref, mass_ref, krow, kcol, diag_ref, minv, u0_ref, source_ref, cedge, redge):
    groups = u0_ref.shape[0] // 16
    lane = lax.broadcasted_iota(jnp.int32, (8, LANES), 1)
    even = lane % 2 == 0
    grid = [(a, b) for a in range(4) for b in range(4)]
    scales = [scale_ref[group : group + 1, :] for group in range(groups)]
    flux, mass, lap = {}, {}, {}
    for a, b in grid:
        x = fetch(plane(groups, a, b))
        w = np.float32(WEIGHTS[a] * WEIGHTS[b])
        flux[a, b] = jnp.where(even, x, pltpu.roll(x, 1, 1)) * w
        mass[a, b] = jnp.where(even, pltpu.roll(x, LANES - 1, 1), x) * w
    for group in range(groups):
        inverse = 1.0 / scales[group]
        for a, b in grid:
            mass_ref[plane(group, a, b), tile(t), :] = mass[a, b] * inverse
            source_ref[plane(group, a, b), tile(t), :] = fetch(plane(group, a, b)) * mass[a, b]

    def less(a, b, value):
        lap[a, b] = lap[a, b] + value if (a, b) in lap else value

    for line in range(4):
        for i, (p, q) in enumerate(PAIRS):
            c = [np.float32(SLOPES[j, p] * SLOPES[j, q]) for j in range(4)]
            kr = sum(flux[j, line] * c[j] for j in range(4))
            kc = sum(flux[line, j] * c[j] for j in range(4))
            krow[line * 6 + i, tile(t), :] = kr
            kcol[line * 6 + i, tile(t), :] = kc
            less(p, line, kr)
            less(q, line, kr)
            less(line, p, kc)
            less(line, q, kc)
    for a, b in grid:
        lap[a, b] = -lap[a, b]
    for values, base in ((mass, 0), (lap, 4)):
        for b in range(4):
            values[0, b], values[3, b] = join_rows(values[0, b], values[3, b])
            for a in range(4):
                if b in (0, 3):
                    cedge[2 * (base + a) + b // 3, spare(t), :] = values[a, b]
    for group in range(groups):
        for b in range(4):
            column = [source_ref[plane(group, a, b), tile(t), :] for a in range(4)]
            column[0], column[3] = join_rows(column[0], column[3])
            for a in range(4):
                p = plane(group, a, b)
                if b in (1, 2):
                    diag = mass[a, b] + scales[group] * lap[a, b]
                    inverse = 1.0 / diag
                    diag_ref[p, tile(t), :] = diag
                    u0_ref[p, tile(t), :] = column[a] * inverse
                    minv[p, tile(t), :] = inverse * scales[group]
                else:
                    redge[2 * (group * 4 + a) + b // 3, spare(t), :] = column[a]


def finish(a, low, high, scale_ref, diag_ref, minv, u0_ref, cedge, redge):
    groups = u0_ref.shape[0] // 16
    span = slice(low, high)
    mass_sums = join_cols(cedge, a, low, high)
    lap_sums = join_cols(cedge, 4 + a, low, high)
    for group in range(groups):
        scale = scale_ref[group : group + 1, :]
        source = join_cols(redge, group * 4 + a, low, high)
        for side, b in enumerate((0, 3)):
            diag = mass_sums[side] + scale * lap_sums[side]
            inverse = 1.0 / diag
            diag_ref[plane(group, a, b), span, :] = diag
            u0_ref[plane(group, a, b), span, :] = source[side] * inverse
            minv[plane(group, a, b), span, :] = inverse * scale


def operator_tile(t, own, sums, now_ref, old_ref, new_ref, mass_ref, krow, kcol, minv, w_ref, edge):
    groups = now_ref.shape[0] // 16
    zero = jnp.zeros((8, LANES), jnp.float32)
    sums = list(sums)
    for group in range(groups):
        u = [[now_ref[plane(group, a, b), tile(t), :] for b in range(4)] for a in range(4)]
        along_rows = [
            line_operator(
                [krow[line * 6 + i, tile(t), :] for i in range(6)], [u[a][line] for a in range(4)]
            )
            for line in range(4)
        ]
        along_cols = [
            line_operator([kcol[line * 6 + i, tile(t), :] for i in range(6)], u[line])
            for line in range(4)
        ]
        with_now, with_old = zero, zero
        y = [[None] * 4 for _ in range(4)]
        for a in range(4):
            for b in range(4):
                p = plane(group, a, b)
                value = mass_ref[p, tile(t), :] * u[a][b]
                row, col = along_rows[b][a], along_cols[a][b]
                value = value - row if a == 3 else value + row
                value = value - col if b == 3 else value + col
                y[a][b] = value
                with_now += u[a][b] * value
                if old_ref is None:
                    with_old += w_ref[p, tile(t), :] * u[a][b]
                else:
                    with_old += old_ref[p, tile(t), :] * value
        sums[group] += with_now if own is None else own * with_now
        sums[groups + group] += with_old if own is None else own * with_old
        for b in range(4):
            column = [y[a][b] for a in range(4)]
            column[0], column[3] = join_rows(column[0], column[3])
            for a in range(4):
                p = plane(group, a, b)
                if b in (1, 2):
                    if new_ref is None:
                        w_ref[p, tile(t), :] = column[a]
                    else:
                        new_ref[p, tile(t), :] = column[a] * minv[p, tile(t), :] - u[a][b]
                else:
                    edge[2 * (group * 4 + a) + b // 3, spare(t), :] = column[a]
    return tuple(sums)


def prep_kernel(t_ref, scale_ref, *refs):
    state, (u1_ref, edge, sums_ref) = refs[:9], refs[9:]
    mass_ref, krow, kcol, diag_ref, minv, u0_ref, w_ref, cedge, redge = state
    cols = t_ref.shape[1]

    @pl.loop(0, cols // 8)
    def _(t):
        prepare(t, lambda p: t_ref[p, tile(t), :], scale_ref, *state)

    @pl.loop(0, 4)
    def _(a):
        finish(a, 8, cols - 8, scale_ref, diag_ref, minv, u0_ref, cedge, redge)

    zero = jnp.zeros((8, LANES), jnp.float32)
    sums = lax.fori_loop(
        1,
        cols // 8 - 1,
        lambda t, sums: operator_tile(
            t, None, sums, u0_ref, None, u1_ref, mass_ref, krow, kcol, minv, w_ref, edge
        ),
        (zero,) * sums_ref.shape[0],
    )
    for i, value in enumerate(sums):
        sums_ref[i] = value


def krylov_kernel(own_rows, cols, count, right_ref, left_ref, scale_ref, *refs):
    state = refs[count : count + 9]
    u1_ref, edge, sums_ref, u2_ref, part_ref = refs[count + 9 :]
    mass_ref, krow, kcol, diag_ref, minv, u0_ref, w_ref, cedge, redge = state
    groups = u0_ref.shape[0] // 16
    total = u0_ref.shape[1]
    tiles = total // 8
    own_tiles = cols // 8
    scales = [scale_ref[group : group + 1, :] for group in range(groups)]
    prepare(
        own_tiles, lambda p: jnp.concatenate([right_ref[p], left_ref[p]], axis=0), scale_ref, *state
    )

    @pl.loop(0, 4)
    def _(a):
        wrap_cols(cedge, a, total)
        wrap_cols(cedge, 4 + a, total)
        for group in range(groups):
            wrap_cols(redge, group * 4 + a, total)
        for low, high in ((0, 8), (cols - 8, total)):
            finish(a, low, high, scale_ref, diag_ref, minv, u0_ref, cedge, redge)

    zero = jnp.zeros((8, LANES), jnp.float32)
    shared = (mass_ref, krow, kcol, minv, w_ref, edge)

    def apply(now_ref, old_ref, new_ref):
        def body(i, sums):
            if old_ref is None:
                t = jnp.where(i == 0, 0, i + own_tiles - 2)
            else:
                t = i
            own = (t < own_tiles).astype(jnp.float32)
            return operator_tile(t, own, sums, now_ref, old_ref, new_ref, *shared)

        if old_ref is None:
            sums = lax.fori_loop(0, 3, body, tuple(sums_ref[i] for i in range(2 * groups)))
        else:
            sums = lax.fori_loop(0, tiles, body, (zero,) * (2 * groups))

        @pl.loop(0, groups * 4)
        def _(i):
            wrap_cols(edge, i, total)
            for b, value in zip((0, 3), join_cols(edge, i, 0, total)):
                p = i * 4 + b
                if new_ref is None:
                    w_ref[p] = value
                else:
                    new_ref[p] = value * minv[p] - now_ref[p]

        return sums[:groups], sums[groups:]

    g00, b0 = apply(u0_ref, None, u1_ref)
    g11, g01 = apply(u1_ref, u0_ref, u2_ref)
    g22, g12 = apply(u2_ref, u1_ref, None)
    rows = [jnp.sum(x, axis=0, keepdims=True) for x in b0]
    for q in (g00, g01, g11, g12, g22):
        rows += [scale * jnp.sum(x, axis=0, keepdims=True) for scale, x in zip(scales, q)]
    rows += [jnp.zeros((1, LANES), jnp.float32)] * (-len(rows) % 8)
    table = jnp.concatenate(rows, axis=0)
    lanes = lax.broadcasted_iota(jnp.int32, table.shape, 1)
    lines = lax.broadcasted_iota(jnp.int32, table.shape, 0)
    table = jnp.where(lanes < own_rows // 4 * PACK, table, 0.0)
    table = over_rows(table)
    table = jnp.where(lanes // PACK == lines, table, 0.0)
    part_ref[...] = jnp.broadcast_to(jnp.sum(table, axis=0, keepdims=True), part_ref.shape)


def combine_kernel(
    parts_ref, scale_ref, u0_ref, u1_ref, u2_ref, w_ref, diag_ref, sol_hbm, res_hbm, sol, res, xs, xt, sems
):
    halves, modes, rows, _ = sol.shape
    groups = modes // PACK
    own = rows // 4
    per_half = LANES // 4
    total = jnp.sum(parts_ref[...], axis=0, keepdims=True)
    table = jnp.broadcast_to(total, (24, LANES))
    lanes = lax.broadcasted_iota(jnp.int32, table.shape, 1)
    lines = lax.broadcasted_iota(jnp.int32, table.shape, 0)
    table = jnp.where(lanes // PACK == lines, table, 0.0)
    table = over_rows(table)
    b0, g00, g01, g11, g12, g22 = [table[q * groups : (q + 1) * groups] for q in range(6)]
    g02 = g11
    b1 = g00 - b0
    b2 = g01 - b1
    l10 = g01 / g00
    l20 = g02 / g00
    d1 = g11 - l10 * g01
    t12 = g12 - l20 * g01
    l21 = t12 / d1
    d2 = g22 - l20 * g02 - l21 * t12
    y1 = b1 - l10 * b0
    y2 = b2 - l20 * b0 - l21 * y1
    c2 = y2 / d2
    c1 = y1 / d1 - l21 * c2
    c0 = b0 / g00 - l10 * c1 - l20 * c2
    copies = []
    for half in range(halves):
        span = slice(half * per_half, (half + 1) * per_half)
        for group in range(groups):
            k0, k1, k2 = [c[group : group + 1, :] for c in (c0, c1, c2)]
            r0, r1, r2 = 1.0 - k0, k0 + k1, k2 * scale_ref[group : group + 1, :]
            for a in range(4):
                slot = group * 4 + a
                for b in range(4):
                    p = plane(group, a, b)
                    u0, u1, u2 = u0_ref[p, span, :], u1_ref[p, span, :], u2_ref[p, span, :]
                    xs[0, slot, pl.ds(b, per_half, stride=4), :] = k0 * u0 + k1 * u1 + k2 * u2
                    xs[1, slot, pl.ds(b, per_half, stride=4), :] = (
                        diag_ref[p, span, :] * (r0 * u0 - r1 * u1 - k1 * u2) - r2 * w_ref[p, span, :]
                    )
                for i, out in enumerate((sol, res)):
                    xt[i, slot] = xs[i, slot].T
                    for m in range(PACK):
                        out[half, group * PACK + m, pl.ds(a, own, stride=4), :] = xt[
                            i, slot, pl.ds(m, own, stride=PACK), :
                        ]
            span_modes = pl.ds(group * PACK, PACK)
            for i, (out, hbm) in enumerate(((sol, sol_hbm), (res, res_hbm))):
                copy = pltpu.make_async_copy(
                    out.at[half, span_modes],
                    hbm.at[span_modes, :, pl.ds(half * LANES, LANES)],
                    sems.at[half, group, i],
                )
                copy.start()
                copies.append(copy)
    for copy in copies:
        copy.wait()


def shards(forcing, metric, jacobian, mode_scale):
    modes, rows, cols = forcing.shape
    groups = modes // PACK
    halo = 4 * GHOST
    f32 = jnp.float32

    def shift(x, axis, step):
        count = lax.axis_size(axis)
        return lax.ppermute(x, axis, [(i, (i + step) % count) for i in range(count)])

    vmem = pl.BlockSpec(memory_space=pltpu.VMEM)
    anywhere = pl.BlockSpec(memory_space=pl.ANY)
    array = lambda *shape: jax.ShapeDtypeStruct(shape, f32)
    top, bottom, fields, scale = pl.pallas_call(
        load_kernel,
        in_specs=[anywhere] * 4,
        out_specs=[vmem] * 4,
        out_shape=[array(modes + 2, halo, cols)] * 2
        + [array(modes + 2, rows, cols), array(groups, LANES)],
        scratch_shapes=[pltpu.SMEM((modes,), f32), pltpu.SemaphoreType.DMA((4, 3))],
        compiler_params=pltpu.CompilerParams(vmem_limit_bytes=LOAD_LIMIT),
        name="load",
    )(*[pltpu.with_memory_space_constraint(x, pltpu.HBM) for x in (forcing, metric, jacobian, mode_scale)])
    up = shift(bottom, "curve", 1)
    down = shift(top, "curve", -1)

    planes = 16 * (groups + 1)
    ecols = cols // 4
    halves = cols // LANES
    per_half = LANES // 4
    whole = lambda *shape: pl.BlockSpec(shape, lambda h: (0,) * len(shape))
    spread, low, high = pl.pallas_call(
        functools.partial(spread_kernel, rows),
        grid=(halves,),
        in_specs=[
            pl.BlockSpec((modes + 2, rows, LANES), lambda h: (0, 0, h)),
            pl.BlockSpec((modes + 2, halo, LANES), lambda h: (0, 0, h)),
            pl.BlockSpec((modes + 2, halo, LANES), lambda h: (0, 0, h)),
        ],
        out_specs=[
            pl.BlockSpec((planes, per_half, LANES), lambda h: (0, h, 0)),
            whole(planes, GHOST, LANES),
            whole(planes, GHOST, LANES),
        ],
        out_shape=[
            jax.ShapeDtypeStruct((planes, ecols, LANES), f32),
            jax.ShapeDtypeStruct((planes, GHOST, LANES), f32),
            jax.ShapeDtypeStruct((planes, GHOST, LANES), f32),
        ],
        scratch_shapes=[pltpu.VMEM((planes // 4, LANES, LANES), f32)] * 2,
        compiler_params=pltpu.CompilerParams(vmem_limit_bytes=12 << 20),
        name="spread",
    )(fields, up, down)

    left = shift(high, "sub", 1)
    right = shift(low, "sub", -1)

    total = ecols + 2 * GHOST
    field = array(16 * groups, total, LANES)
    lines = array(24, total, LANES)
    state = pl.pallas_call(
        prep_kernel,
        in_specs=[vmem] * 2,
        out_specs=[vmem] * 12,
        out_shape=[field, lines, lines, field, field, field, field]
        + [array(16, total + 16, LANES), array(8 * groups, total + 16, LANES)]
        + [field, array(8 * groups, total + 16, LANES), array(2 * groups, 8, LANES)],
        compiler_params=pltpu.CompilerParams(vmem_limit_bytes=24 << 20),
        cost_estimate=pl.CostEstimate(flops=20_000_000, bytes_accessed=0, transcendentals=0),
        name="prep",
    )(spread, scale)
    devices = lax.axis_size(AXES[0]) * lax.axis_size(AXES[1])
    count = len(state)
    out = pl.pallas_call(
        functools.partial(krylov_kernel, rows, ecols, count),
        in_specs=[vmem] * (3 + count),
        out_specs=[vmem] * (count + 2),
        out_shape=[array(*x.shape) for x in state] + [field, array(devices, LANES)],
        input_output_aliases={3 + i: i for i in range(count)},
        compiler_params=pltpu.CompilerParams(vmem_limit_bytes=24 << 20),
        name="krylov",
    )(right, left, scale, *state)
    diag, u0, w3, u1 = out[3], out[5], out[6], out[9]
    u2, part = out[count:]

    parts = lax.all_to_all(part, AXES, 0, 0, tiled=True)

    out = jax.ShapeDtypeStruct((modes, rows, cols), f32)
    return tuple(
        pl.pallas_call(
            combine_kernel,
            in_specs=[vmem] * 7,
            out_specs=[anywhere] * 2,
            out_shape=[out] * 2,
            scratch_shapes=[
                pltpu.VMEM((halves, modes, rows, LANES), f32),
                pltpu.VMEM((halves, modes, rows, LANES), f32),
                pltpu.VMEM((2, 4 * groups, LANES, LANES), f32),
                pltpu.VMEM((2, 4 * groups, LANES, LANES), f32),
                pltpu.SemaphoreType.DMA((halves, groups, 2)),
            ],
            compiler_params=pltpu.CompilerParams(vmem_limit_bytes=20 << 20),
            name="combine",
        )(parts, scale, u0, u1, u2, w3, diag)
    )


def solution(mesh):
    in_specs = (P(None, "curve", "sub"), P("curve", "sub"), P("curve", "sub"), P())
    out_specs = (P(None, "curve", "sub"), P(None, "curve", "sub"))
    return jax.shard_map(
        shards, mesh=mesh, in_specs=in_specs, out_specs=out_specs, check_vma=False
    )
```

```python
import functools
import math

import jax
import jax.numpy as jnp
import numpy as np
from jax import lax
from jax.experimental import pallas as pl
from jax.experimental.pallas import tpu as pltpu
from jax.sharding import PartitionSpec as P

GHOST = 4
PACK = 4
LANES = 128
AXES = ("curve", "sub")
RIM = 2 * GHOST * PACK


def gll_tables():
    points = np.array([-1.0, -1.0 / math.sqrt(5.0), 1.0 / math.sqrt(5.0), 1.0])
    weights = np.array([1.0 / 6.0, 5.0 / 6.0, 5.0 / 6.0, 1.0 / 6.0])
    factor = np.array(
        [np.prod([points[j] - points[m] for m in range(4) if m != j]) for j in range(4)]
    )
    slopes = np.zeros((4, 4))
    for i in range(4):
        for j in range(4):
            if i != j:
                slopes[i, j] = factor[i] / (factor[j] * (points[i] - points[j]))
        slopes[i, i] = sum((1.0 / (points[i] - points[m]) for m in range(4) if m != i))
    return (slopes, weights)


SLOPES, WEIGHTS = gll_tables()
PAIRS = [(a, k) for a in range(4) for k in range(a + 1, 4)]


def plane(group, a, b):
    return (group * 4 + a) * 4 + b


def load_kernel(f_hbm, metric_hbm, jacobian_hbm, scale_hbm, top, bottom, fields, scale_ref, scales, sems, scale_sem):
    modes, rows, _ = f_hbm.shape
    halves, _, halo, _ = top.shape
    scale_copy = pltpu.make_async_copy(scale_hbm, scales, scale_sem)
    scale_copy.start()
    copies = []
    for part, (out, at, size) in enumerate(
        ((top, 0, halo), (bottom, rows - halo, halo), (fields, 0, rows))
    ):
        span = pl.ds(at, size)
        for half in range(halves):
            columns = pl.ds(half * LANES, LANES)
            for i, (source, target) in enumerate(
                (
                    (f_hbm.at[:, span, columns], out.at[half, pl.ds(0, modes)]),
                    (metric_hbm.at[span, columns], out.at[half, modes]),
                    (jacobian_hbm.at[span, columns], out.at[half, modes + 1]),
                )
            ):
                copies.append(pltpu.make_async_copy(source, target, sems.at[part, half, i]))
    for copy in copies:
        copy.start()
    scale_copy.wait()
    member = lax.broadcasted_iota(jnp.int32, (1, LANES), 1) % PACK
    for group in range(modes // PACK):
        row = jnp.zeros((1, LANES), jnp.float32)
        for m in range(PACK):
            row = jnp.where(member == m, scales[group * PACK + m], row)
        scale_ref[group : group + 1, :] = row
    for copy in copies:
        copy.wait()


def spread_kernel(fields_ref, t_ref, xs, xt):
    halves, stack, rows, _ = fields_ref.shape
    own = rows // 4
    groups = (stack - 2) // PACK
    per_half = LANES // 4
    for half in range(halves):
        for group in range(groups + 1):
            for a in range(4):
                at = (half * (groups + 1) + group) * 4 + a
                for m in range(PACK):
                    index = group * PACK + (m if group < groups else m % 2)
                    xs[at, pl.ds(RIM + m, own, stride=PACK), :] = fields_ref[
                        half, index, pl.ds(a, own, stride=4), :
                    ]
                xs[at, :RIM, :] = jnp.zeros((RIM, LANES), jnp.float32)
                xt[at] = xs[at].T
                for b in range(4):
                    t_ref[plane(group, a, b), half * per_half : (half + 1) * per_half, :] = xt[
                        at, pl.ds(b, per_half, stride=4), :
                    ]


def ghost_kernel(up_ref, down_ref, own_ref, rim_ref, low_ref, high_ref, xs, ends):
    halves, stack, _, _ = up_ref.shape
    groups = (stack - 2) // PACK
    per_half = rim_ref.shape[0] // halves
    height = rim_ref.shape[2]
    rim = lax.broadcasted_iota(jnp.int32, (GHOST, LANES), 1) < RIM
    for half in range(halves):
        for group in range(groups + 1):
            at = half * (groups + 1) + group
            for a in range(4):
                for m in range(PACK):
                    index = group * PACK + (m if group < groups else m % 2)
                    for side, ref in enumerate((down_ref, up_ref)):
                        start = a * RIM + side * GHOST * PACK + m
                        xs[at, pl.ds(start, GHOST, stride=PACK), :] = ref[
                            half, index, pl.ds(a, GHOST, stride=4), :
                        ]
            turned = xs[at].T
            for i in range(per_half):
                rim_ref[half * per_half + i, group] = turned[i * height : (i + 1) * height]
    last = rim_ref.shape[0] - 1
    total = own_ref.shape[1]
    size = 4 * GHOST
    for group in range(groups + 1):
        for a in range(4):
            at = group * 4 + a
            for side, x in enumerate((rim_ref[0, group, :size], rim_ref[last, group, height - size :])):
                ends[side, at] = pltpu.roll(x, LANES - a * RIM, 1) if a else x
            for b in range(4):
                p = at * 4 + b
                picked = pl.ds(b, GHOST, stride=4)
                low_ref[p] = jnp.where(rim, ends[0, at, picked, :], own_ref[p, :GHOST, :])
                high_ref[p] = jnp.where(rim, ends[1, at, picked, :], own_ref[p, total - GHOST :, :])


def line_operator(coefs, values):
    f01, f02, f03, f12, f13, f23 = [
        coef * (values[k] - values[a]) for (a, k), coef in zip(PAIRS, coefs)
    ]
    return f01 + f02 + f03, f12 + f13 - f01, f23 - f02 - f12, f03 + f13 + f23


def over_rows(table):
    i = lax.broadcasted_iota(jnp.int32, (LANES, LANES), 0)
    j = lax.broadcasted_iota(jnp.int32, (LANES, LANES), 1)
    same = jnp.where(i % PACK == j % PACK, 1.0, 0.0).astype(jnp.float32)
    return jnp.dot(
        table, same, precision=lax.Precision.HIGHEST, preferred_element_type=jnp.float32
    )


def tile(t):
    return pl.ds(pl.multiple_of(t * 8, 8), 8)


def spare(t):
    return pl.ds(pl.multiple_of(t * 8 + 8, 8), 8)


def join_rows(first, last):
    shared = last + pltpu.roll(first, LANES - PACK, 1)
    return pltpu.roll(shared, PACK, 1), shared


def wrap_cols(edge, i, total):
    edge[2 * i, total + 8 : total + 16, :] = edge[2 * i, 8:16, :]
    edge[2 * i + 1, 0:8, :] = edge[2 * i + 1, total : total + 8, :]


def join_cols(edge, i, low, high):
    first = edge[2 * i, low + 8 : high + 8, :] + edge[2 * i + 1, low + 7 : high + 7, :]
    last = edge[2 * i + 1, low + 8 : high + 8, :] + edge[2 * i, low + 9 : high + 9, :]
    return first, last


def prepare(t, fetch, scale_ref, mass_ref, krow, kcol, diag_ref, minv, u0_ref, source_ref, cedge, redge):
    groups = u0_ref.shape[0] // 16
    lane = lax.broadcasted_iota(jnp.int32, (8, LANES), 1)
    even = lane % 2 == 0
    grid = [(a, b) for a in range(4) for b in range(4)]
    scales = [scale_ref[group : group + 1, :] for group in range(groups)]
    flux, mass, lap = {}, {}, {}
    for a, b in grid:
        x = fetch(plane(groups, a, b))
        w = np.float32(WEIGHTS[a] * WEIGHTS[b])
        flux[a, b] = jnp.where(even, x, pltpu.roll(x, 1, 1)) * w
        mass[a, b] = jnp.where(even, pltpu.roll(x, LANES - 1, 1), x) * w
    for group in range(groups):
        inverse = 1.0 / scales[group]
        for a, b in grid:
            mass_ref[plane(group, a, b), tile(t), :] = mass[a, b] * inverse
            source_ref[plane(group, a, b), tile(t), :] = fetch(plane(group, a, b)) * mass[a, b]

    def less(a, b, value):
        lap[a, b] = lap[a, b] + value if (a, b) in lap else value

    for line in range(4):
        for i, (p, q) in enumerate(PAIRS):
            c = [np.float32(SLOPES[j, p] * SLOPES[j, q]) for j in range(4)]
            kr = sum(flux[j, line] * c[j] for j in range(4))
            kc = sum(flux[line, j] * c[j] for j in range(4))
            krow[line * 6 + i, tile(t), :] = kr
            kcol[line * 6 + i, tile(t), :] = kc
            less(p, line, kr)
            less(q, line, kr)
            less(line, p, kc)
            less(line, q, kc)
    for a, b in grid:
        lap[a, b] = -lap[a, b]
    for values, base in ((mass, 0), (lap, 4)):
        for b in range(4):
            values[0, b], values[3, b] = join_rows(values[0, b], values[3, b])
            for a in range(4):
                if b in (0, 3):
                    cedge[2 * (base + a) + b // 3, spare(t), :] = values[a, b]
    for group in range(groups):
        for b in range(4):
            column = [source_ref[plane(group, a, b), tile(t), :] for a in range(4)]
            column[0], column[3] = join_rows(column[0], column[3])
            for a in range(4):
                p = plane(group, a, b)
                if b in (1, 2):
                    diag = mass[a, b] + scales[group] * lap[a, b]
                    inverse = 1.0 / diag
                    diag_ref[p, tile(t), :] = diag
                    u0_ref[p, tile(t), :] = column[a] * inverse
                    minv[p, tile(t), :] = inverse * scales[group]
                else:
                    redge[2 * (group * 4 + a) + b // 3, spare(t), :] = column[a]


def finish(a, low, high, scale_ref, diag_ref, minv, u0_ref, cedge, redge):
    groups = u0_ref.shape[0] // 16
    span = slice(low, high)
    mass_sums = join_cols(cedge, a, low, high)
    lap_sums = join_cols(cedge, 4 + a, low, high)
    for group in range(groups):
        scale = scale_ref[group : group + 1, :]
        source = join_cols(redge, group * 4 + a, low, high)
        for side, b in enumerate((0, 3)):
            diag = mass_sums[side] + scale * lap_sums[side]
            inverse = 1.0 / diag
            diag_ref[plane(group, a, b), span, :] = diag
            u0_ref[plane(group, a, b), span, :] = source[side] * inverse
            minv[plane(group, a, b), span, :] = inverse * scale


def operator_tile(t, own, sums, now_ref, old_ref, new_ref, mass_ref, krow, kcol, minv, w_ref, edge):
    groups = now_ref.shape[0] // 16
    zero = jnp.zeros((8, LANES), jnp.float32)
    sums = list(sums)
    for group in range(groups):
        u = [[now_ref[plane(group, a, b), tile(t), :] for b in range(4)] for a in range(4)]
        along_rows = [
            line_operator(
                [krow[line * 6 + i, tile(t), :] for i in range(6)], [u[a][line] for a in range(4)]
            )
            for line in range(4)
        ]
        along_cols = [
            line_operator([kcol[line * 6 + i, tile(t), :] for i in range(6)], u[line])
            for line in range(4)
        ]
        with_now, with_old = zero, zero
        y = [[None] * 4 for _ in range(4)]
        for a in range(4):
            for b in range(4):
                p = plane(group, a, b)
                value = mass_ref[p, tile(t), :] * u[a][b]
                row, col = along_rows[b][a], along_cols[a][b]
                value = value - row if a == 3 else value + row
                value = value - col if b == 3 else value + col
                y[a][b] = value
                with_now += u[a][b] * value
                if old_ref is None:
                    with_old += w_ref[p, tile(t), :] * u[a][b]
                else:
                    with_old += old_ref[p, tile(t), :] * value
        sums[group] += with_now if own is None else own * with_now
        sums[groups + group] += with_old if own is None else own * with_old
        for b in range(4):
            column = [y[a][b] for a in range(4)]
            column[0], column[3] = join_rows(column[0], column[3])
            for a in range(4):
                p = plane(group, a, b)
                if b in (1, 2):
                    if new_ref is None:
                        w_ref[p, tile(t), :] = column[a]
                    else:
                        new_ref[p, tile(t), :] = column[a] * minv[p, tile(t), :] - u[a][b]
                else:
                    edge[2 * (group * 4 + a) + b // 3, spare(t), :] = column[a]
    return tuple(sums)


def prep_kernel(t_ref, rim_ref, scale_ref, *refs):
    state, (u1_ref, edge, sums_ref) = refs[:9], refs[9:]
    mass_ref, krow, kcol, diag_ref, minv, u0_ref, w_ref, cedge, redge = state
    cols = t_ref.shape[1]
    rim = lax.broadcasted_iota(jnp.int32, (8, LANES), 1) < RIM

    @pl.loop(0, cols // 8)
    def _(t):
        def fetch(p):
            group, a, b = p // 16, p // 4 % 4, p % 4
            outer = rim_ref[t, group, pl.ds(b, 8, stride=4), :]
            if a:
                outer = pltpu.roll(outer, LANES - a * RIM, 1)
            return jnp.where(rim, outer, t_ref[p, tile(t), :])

        prepare(t, fetch, scale_ref, *state)

    @pl.loop(0, 4)
    def _(a):
        finish(a, 8, cols - 8, scale_ref, diag_ref, minv, u0_ref, cedge, redge)

    zero = jnp.zeros((8, LANES), jnp.float32)
    sums = lax.fori_loop(
        1,
        cols // 8 - 1,
        lambda t, sums: operator_tile(
            t, None, sums, u0_ref, None, u1_ref, mass_ref, krow, kcol, minv, w_ref, edge
        ),
        (zero,) * sums_ref.shape[0],
    )
    for i, value in enumerate(sums):
        sums_ref[i] = value


def krylov_kernel(cols, count, right_ref, left_ref, scale_ref, *refs):
    state = refs[count : count + 9]
    u1_ref, edge, sums_ref, u2_ref, part_ref = refs[count + 9 :]
    mass_ref, krow, kcol, diag_ref, minv, u0_ref, w_ref, cedge, redge = state
    groups = u0_ref.shape[0] // 16
    total = u0_ref.shape[1]
    tiles = total // 8
    own_tiles = cols // 8
    scales = [scale_ref[group : group + 1, :] for group in range(groups)]
    prepare(
        own_tiles, lambda p: jnp.concatenate([right_ref[p], left_ref[p]], axis=0), scale_ref, *state
    )

    @pl.loop(0, 4)
    def _(a):
        wrap_cols(cedge, a, total)
        wrap_cols(cedge, 4 + a, total)
        for group in range(groups):
            wrap_cols(redge, group * 4 + a, total)
        for low, high in ((0, 8), (cols - 8, total)):
            finish(a, low, high, scale_ref, diag_ref, minv, u0_ref, cedge, redge)

    zero = jnp.zeros((8, LANES), jnp.float32)
    shared = (mass_ref, krow, kcol, minv, w_ref, edge)

    def apply(now_ref, old_ref, new_ref):
        def body(i, sums):
            if old_ref is None:
                t = jnp.where(i == 0, 0, i + own_tiles - 2)
            else:
                t = i
            own = (t < own_tiles).astype(jnp.float32)
            return operator_tile(t, own, sums, now_ref, old_ref, new_ref, *shared)

        if old_ref is None:
            sums = lax.fori_loop(0, 3, body, tuple(sums_ref[i] for i in range(2 * groups)))
        else:
            sums = lax.fori_loop(0, tiles, body, (zero,) * (2 * groups))

        @pl.loop(0, groups * 4)
        def _(i):
            wrap_cols(edge, i, total)
            for b, value in zip((0, 3), join_cols(edge, i, 0, total)):
                p = i * 4 + b
                if new_ref is None:
                    w_ref[p] = value
                else:
                    new_ref[p] = value * minv[p] - now_ref[p]

        return sums[:groups], sums[groups:]

    g00, b0 = apply(u0_ref, None, u1_ref)
    g11, g01 = apply(u1_ref, u0_ref, u2_ref)
    g22, g12 = apply(u2_ref, u1_ref, None)
    rows = [jnp.sum(x, axis=0, keepdims=True) for x in b0]
    for q in (g00, g01, g11, g12, g22):
        rows += [scale * jnp.sum(x, axis=0, keepdims=True) for scale, x in zip(scales, q)]
    rows += [jnp.zeros((1, LANES), jnp.float32)] * (-len(rows) % 8)
    table = jnp.concatenate(rows, axis=0)
    lanes = lax.broadcasted_iota(jnp.int32, table.shape, 1)
    lines = lax.broadcasted_iota(jnp.int32, table.shape, 0)
    table = jnp.where(lanes >= RIM, table, 0.0)
    table = over_rows(table)
    table = jnp.where(lanes // PACK == lines, table, 0.0)
    part_ref[...] = jnp.broadcast_to(jnp.sum(table, axis=0, keepdims=True), part_ref.shape)


def combine_kernel(
    parts_ref, scale_ref, u0_ref, u1_ref, u2_ref, w_ref, diag_ref, sol_hbm, res_hbm, sol, res, xs, xt, sems
):
    halves, modes, rows, _ = sol.shape
    groups = modes // PACK
    own = rows // 4
    per_half = LANES // 4
    total = jnp.sum(parts_ref[...], axis=0, keepdims=True)
    table = jnp.broadcast_to(total, (24, LANES))
    lanes = lax.broadcasted_iota(jnp.int32, table.shape, 1)
    lines = lax.broadcasted_iota(jnp.int32, table.shape, 0)
    table = jnp.where(lanes // PACK == lines, table, 0.0)
    table = over_rows(table)
    b0, g00, g01, g11, g12, g22 = [table[q * groups : (q + 1) * groups] for q in range(6)]
    g02 = g11
    b1 = g00 - b0
    b2 = g01 - b1
    l10 = g01 / g00
    l20 = g02 / g00
    d1 = g11 - l10 * g01
    t12 = g12 - l20 * g01
    l21 = t12 / d1
    d2 = g22 - l20 * g02 - l21 * t12
    y1 = b1 - l10 * b0
    y2 = b2 - l20 * b0 - l21 * y1
    c2 = y2 / d2
    c1 = y1 / d1 - l21 * c2
    c0 = b0 / g00 - l10 * c1 - l20 * c2
    copies = []
    for half in range(halves):
        span = slice(half * per_half, (half + 1) * per_half)
        for group in range(groups):
            k0, k1, k2 = [c[group : group + 1, :] for c in (c0, c1, c2)]
            r0, r1, r2 = 1.0 - k0, k0 + k1, k2 * scale_ref[group : group + 1, :]
            for a in range(4):
                slot = group * 4 + a
                for b in range(4):
                    p = plane(group, a, b)
                    u0, u1, u2 = u0_ref[p, span, :], u1_ref[p, span, :], u2_ref[p, span, :]
                    xs[0, slot, pl.ds(b, per_half, stride=4), :] = k0 * u0 + k1 * u1 + k2 * u2
                    xs[1, slot, pl.ds(b, per_half, stride=4), :] = (
                        diag_ref[p, span, :] * (r0 * u0 - r1 * u1 - k1 * u2) - r2 * w_ref[p, span, :]
                    )
                for i, out in enumerate((sol, res)):
                    xt[i, slot] = xs[i, slot].T
                    for m in range(PACK):
                        out[half, group * PACK + m, pl.ds(a, own, stride=4), :] = xt[
                            i, slot, pl.ds(RIM + m, own, stride=PACK), :
                        ]
            span_modes = pl.ds(group * PACK, PACK)
            for i, (out, hbm) in enumerate(((sol, sol_hbm), (res, res_hbm))):
                copy = pltpu.make_async_copy(
                    out.at[half, span_modes],
                    hbm.at[span_modes, :, pl.ds(half * LANES, LANES)],
                    sems.at[half, group, i],
                )
                copy.start()
                copies.append(copy)
    for copy in copies:
        copy.wait()


def shards(forcing, metric, jacobian, mode_scale):
    modes, rows, cols = forcing.shape
    groups = modes // PACK
    halo = 4 * GHOST
    f32 = jnp.float32

    def shift(x, axis, step):
        count = lax.axis_size(axis)
        return lax.ppermute(x, axis, [(i, (i + step) % count) for i in range(count)])

    vmem = pl.BlockSpec(memory_space=pltpu.VMEM)
    anywhere = pl.BlockSpec(memory_space=pl.ANY)
    array = lambda *shape: jax.ShapeDtypeStruct(shape, f32)
    planes = 16 * (groups + 1)
    ecols = cols // 4
    halves = cols // LANES
    top, bottom, fields, scale = pl.pallas_call(
        load_kernel,
        in_specs=[anywhere] * 4,
        out_specs=[vmem] * 4,
        out_shape=[array(halves, modes + 2, halo, LANES)] * 2
        + [array(halves, modes + 2, rows, LANES), array(groups, LANES)],
        scratch_shapes=[
            pltpu.SMEM((modes,), f32),
            pltpu.SemaphoreType.DMA((3, halves, 3)),
            pltpu.SemaphoreType.DMA,
        ],
        compiler_params=pltpu.CompilerParams(vmem_limit_bytes=4 << 20),
        name="load",
    )(*[pltpu.with_memory_space_constraint(x, pltpu.HBM) for x in (forcing, metric, jacobian, mode_scale)])
    up = shift(bottom, "curve", 1)
    down = shift(top, "curve", -1)

    spread = pl.pallas_call(
        spread_kernel,
        in_specs=[vmem],
        out_specs=vmem,
        out_shape=array(planes, ecols, LANES),
        scratch_shapes=[pltpu.VMEM((halves * planes // 4, LANES, LANES), f32)] * 2,
        compiler_params=pltpu.CompilerParams(vmem_limit_bytes=12 << 20),
        cost_estimate=pl.CostEstimate(flops=10_000_000, bytes_accessed=0, transcendentals=0),
        name="spread",
    )(fields)
    rim, low, high = pl.pallas_call(
        ghost_kernel,
        in_specs=[vmem] * 3,
        out_specs=[vmem] * 3,
        out_shape=[array(ecols // 8, groups + 1, 32, LANES)] + [array(planes, GHOST, LANES)] * 2,
        scratch_shapes=[
            pltpu.VMEM((halves * (groups + 1), LANES, LANES), f32),
            pltpu.VMEM((2, planes // 4, 4 * GHOST, LANES), f32),
        ],
        compiler_params=pltpu.CompilerParams(vmem_limit_bytes=12 << 20),
        name="ghost",
    )(up, down, spread)

    left = shift(high, "sub", 1)
    right = shift(low, "sub", -1)

    total = ecols + 2 * GHOST
    field = array(16 * groups, total, LANES)
    lines = array(24, total, LANES)
    state = pl.pallas_call(
        prep_kernel,
        in_specs=[vmem] * 3,
        out_specs=[vmem] * 12,
        out_shape=[field, lines, lines, field, field, field, field]
        + [array(16, total + 16, LANES), array(8 * groups, total + 16, LANES)]
        + [field, array(8 * groups, total + 16, LANES), array(2 * groups, 8, LANES)],
        compiler_params=pltpu.CompilerParams(vmem_limit_bytes=24 << 20),
        cost_estimate=pl.CostEstimate(flops=20_000_000, bytes_accessed=0, transcendentals=0),
        name="prep",
    )(spread, rim, scale)
    devices = lax.axis_size(AXES[0]) * lax.axis_size(AXES[1])
    count = len(state)
    out = pl.pallas_call(
        functools.partial(krylov_kernel, ecols, count),
        in_specs=[vmem] * (3 + count),
        out_specs=[vmem] * (count + 2),
        out_shape=[array(*x.shape) for x in state] + [field, array(devices, LANES)],
        input_output_aliases={3 + i: i for i in range(count)},
        compiler_params=pltpu.CompilerParams(vmem_limit_bytes=24 << 20),
        name="krylov",
    )(right, left, scale, *state)
    diag, u0, w3, u1 = out[3], out[5], out[6], out[9]
    u2, part = out[count:]

    parts = lax.all_to_all(part, AXES, 0, 0, tiled=True)

    out = jax.ShapeDtypeStruct((modes, rows, cols), f32)
    return tuple(
        pl.pallas_call(
            combine_kernel,
            in_specs=[vmem] * 7,
            out_specs=[anywhere] * 2,
            out_shape=[out] * 2,
            scratch_shapes=[
                pltpu.VMEM((halves, modes, rows, LANES), f32),
                pltpu.VMEM((halves, modes, rows, LANES), f32),
                pltpu.VMEM((2, 4 * groups, LANES, LANES), f32),
                pltpu.VMEM((2, 4 * groups, LANES, LANES), f32),
                pltpu.SemaphoreType.DMA((halves, groups, 2)),
            ],
            compiler_params=pltpu.CompilerParams(vmem_limit_bytes=20 << 20),
            name="combine",
        )(parts, scale, u0, u1, u2, w3, diag)
    )


def solution(mesh):
    in_specs = (P(None, "curve", "sub"), P("curve", "sub"), P("curve", "sub"), P())
    out_specs = (P(None, "curve", "sub"), P(None, "curve", "sub"))
    return jax.shard_map(
        shards, mesh=mesh, in_specs=in_specs, out_specs=out_specs, check_vma=False
    )
```

```python
import functools
import math

import jax
import jax.numpy as jnp
import numpy as np
from jax import lax
from jax.experimental import pallas as pl
from jax.experimental.pallas import tpu as pltpu
from jax.sharding import PartitionSpec as P

GHOST = 4
PACK = 4
LANES = 128
AXES = ("curve", "sub")
RIM = 2 * GHOST * PACK


def gll_tables():
    points = np.array([-1.0, -1.0 / math.sqrt(5.0), 1.0 / math.sqrt(5.0), 1.0])
    weights = np.array([1.0 / 6.0, 5.0 / 6.0, 5.0 / 6.0, 1.0 / 6.0])
    factor = np.array(
        [np.prod([points[j] - points[m] for m in range(4) if m != j]) for j in range(4)]
    )
    slopes = np.zeros((4, 4))
    for i in range(4):
        for j in range(4):
            if i != j:
                slopes[i, j] = factor[i] / (factor[j] * (points[i] - points[j]))
        slopes[i, i] = sum((1.0 / (points[i] - points[m]) for m in range(4) if m != i))
    return (slopes, weights)


SLOPES, WEIGHTS = gll_tables()
PAIRS = [(a, k) for a in range(4) for k in range(a + 1, 4)]


def plane(group, a, b):
    return (group * 4 + a) * 4 + b


def stack_copies(f_hbm, metric_hbm, jacobian_hbm, out, at, sems):
    halves, stack, size, _ = out.shape
    span = pl.ds(at, size)
    copies = []
    for half in range(halves):
        columns = pl.ds(half * LANES, LANES)
        pairs = (
            (f_hbm.at[:, span, columns], out.at[half, pl.ds(0, stack - 2)]),
            (metric_hbm.at[span, columns], out.at[half, stack - 2]),
            (jacobian_hbm.at[span, columns], out.at[half, stack - 1]),
        )
        copies.append(
            [pltpu.make_async_copy(x, y, sems.at[half, i]) for i, (x, y) in enumerate(pairs)]
        )
    for per_half in copies:
        for copy in per_half:
            copy.start()
    return copies


def load_kernel(f_hbm, metric_hbm, jacobian_hbm, scale_hbm, top, bottom, scale_ref, scales, sems, scale_sem):
    modes, rows, _ = f_hbm.shape
    halo = top.shape[2]
    scale_copy = pltpu.make_async_copy(scale_hbm, scales, scale_sem)
    scale_copy.start()
    copies = stack_copies(f_hbm, metric_hbm, jacobian_hbm, top, 0, sems.at[0])
    copies += stack_copies(f_hbm, metric_hbm, jacobian_hbm, bottom, rows - halo, sems.at[1])
    scale_copy.wait()
    member = lax.broadcasted_iota(jnp.int32, (1, LANES), 1) % PACK
    for group in range(modes // PACK):
        row = jnp.zeros((1, LANES), jnp.float32)
        for m in range(PACK):
            row = jnp.where(member == m, scales[group * PACK + m], row)
        scale_ref[group : group + 1, :] = row
    for per_half in copies:
        for copy in per_half:
            copy.wait()


def spread_kernel(f_hbm, metric_hbm, jacobian_hbm, t_ref, fields_ref, xs, xt, sems):
    halves, stack, rows, _ = fields_ref.shape
    own = rows // 4
    groups = (stack - 2) // PACK
    per_half = LANES // 4
    copies = stack_copies(f_hbm, metric_hbm, jacobian_hbm, fields_ref, 0, sems)
    for half in range(halves):
        for copy in copies[half]:
            copy.wait()
        for group in range(groups + 1):
            for a in range(4):
                at = (half * (groups + 1) + group) * 4 + a
                for m in range(PACK):
                    index = group * PACK + (m if group < groups else m % 2)
                    xs[at, pl.ds(RIM + m, own, stride=PACK), :] = fields_ref[
                        half, index, pl.ds(a, own, stride=4), :
                    ]
                xs[at, :RIM, :] = jnp.zeros((RIM, LANES), jnp.float32)
                xt[at] = xs[at].T
                for b in range(4):
                    t_ref[plane(group, a, b), half * per_half : (half + 1) * per_half, :] = xt[
                        at, pl.ds(b, per_half, stride=4), :
                    ]


def ghost_kernel(up_ref, down_ref, own_ref, rim_ref, low_ref, high_ref, xs, ends):
    halves, stack, _, _ = up_ref.shape
    groups = (stack - 2) // PACK
    per_half = rim_ref.shape[0] // halves
    height = rim_ref.shape[2]
    rim = lax.broadcasted_iota(jnp.int32, (GHOST, LANES), 1) < RIM
    for half in range(halves):
        for group in range(groups + 1):
            at = half * (groups + 1) + group
            for a in range(4):
                for m in range(PACK):
                    index = group * PACK + (m if group < groups else m % 2)
                    for side, ref in enumerate((down_ref, up_ref)):
                        start = a * RIM + side * GHOST * PACK + m
                        xs[at, pl.ds(start, GHOST, stride=PACK), :] = ref[
                            half, index, pl.ds(a, GHOST, stride=4), :
                        ]
            turned = xs[at].T
            for i in range(per_half):
                rim_ref[half * per_half + i, group] = turned[i * height : (i + 1) * height]
    last = rim_ref.shape[0] - 1
    total = own_ref.shape[1]
    size = 4 * GHOST
    for group in range(groups + 1):
        for a in range(4):
            at = group * 4 + a
            for side, x in enumerate((rim_ref[0, group, :size], rim_ref[last, group, height - size :])):
                ends[side, at] = pltpu.roll(x, LANES - a * RIM, 1) if a else x
            for b in range(4):
                p = at * 4 + b
                picked = pl.ds(b, GHOST, stride=4)
                low_ref[p] = jnp.where(rim, ends[0, at, picked, :], own_ref[p, :GHOST, :])
                high_ref[p] = jnp.where(rim, ends[1, at, picked, :], own_ref[p, total - GHOST :, :])


def line_operator(coefs, values):
    f01, f02, f03, f12, f13, f23 = [
        coef * (values[k] - values[a]) for (a, k), coef in zip(PAIRS, coefs)
    ]
    return f01 + f02 + f03, f12 + f13 - f01, f23 - f02 - f12, f03 + f13 + f23


def over_rows(table):
    i = lax.broadcasted_iota(jnp.int32, (LANES, LANES), 0)
    j = lax.broadcasted_iota(jnp.int32, (LANES, LANES), 1)
    same = jnp.where(i % PACK == j % PACK, 1.0, 0.0).astype(jnp.float32)
    return jnp.dot(
        table, same, precision=lax.Precision.HIGHEST, preferred_element_type=jnp.float32
    )


def tile(t):
    return pl.ds(pl.multiple_of(t * 8, 8), 8)


def spare(t):
    return pl.ds(pl.multiple_of(t * 8 + 8, 8), 8)


def join_rows(first, last):
    return first + pltpu.roll(last, PACK, 1), last + pltpu.roll(first, LANES - PACK, 1)


def join_rows_in_turn(first, last):
    shared = last + pltpu.roll(first, LANES - PACK, 1)
    return pltpu.roll(shared, PACK, 1), shared


def wrap_cols(edge, i, total):
    edge[2 * i, total + 8 : total + 16, :] = edge[2 * i, 8:16, :]
    edge[2 * i + 1, 0:8, :] = edge[2 * i + 1, total : total + 8, :]


def join_cols(edge, i, low, high):
    first = edge[2 * i, low + 8 : high + 8, :] + edge[2 * i + 1, low + 7 : high + 7, :]
    last = edge[2 * i + 1, low + 8 : high + 8, :] + edge[2 * i, low + 9 : high + 9, :]
    return first, last


def prepare(t, fetch, scale_ref, mass_ref, krow, kcol, diag_ref, minv, u0_ref, source_ref, cedge, redge):
    groups = u0_ref.shape[0] // 16
    lane = lax.broadcasted_iota(jnp.int32, (8, LANES), 1)
    even = lane % 2 == 0
    grid = [(a, b) for a in range(4) for b in range(4)]
    scales = [scale_ref[group : group + 1, :] for group in range(groups)]
    flux, mass, lap = {}, {}, {}
    for a, b in grid:
        x = fetch(plane(groups, a, b))
        w = np.float32(WEIGHTS[a] * WEIGHTS[b])
        flux[a, b] = jnp.where(even, x, pltpu.roll(x, 1, 1)) * w
        mass[a, b] = jnp.where(even, pltpu.roll(x, LANES - 1, 1), x) * w
    for group in range(groups):
        inverse = 1.0 / scales[group]
        for a, b in grid:
            mass_ref[plane(group, a, b), tile(t), :] = mass[a, b] * inverse
            source_ref[plane(group, a, b), tile(t), :] = fetch(plane(group, a, b)) * mass[a, b]

    def less(a, b, value):
        lap[a, b] = lap[a, b] + value if (a, b) in lap else value

    for line in range(4):
        for i, (p, q) in enumerate(PAIRS):
            c = [np.float32(SLOPES[j, p] * SLOPES[j, q]) for j in range(4)]
            kr = sum(flux[j, line] * c[j] for j in range(4))
            kc = sum(flux[line, j] * c[j] for j in range(4))
            krow[line * 6 + i, tile(t), :] = kr
            kcol[line * 6 + i, tile(t), :] = kc
            less(p, line, kr)
            less(q, line, kr)
            less(line, p, kc)
            less(line, q, kc)
    for a, b in grid:
        lap[a, b] = -lap[a, b]
    for values, base in ((mass, 0), (lap, 4)):
        for b in range(4):
            values[0, b], values[3, b] = join_rows(values[0, b], values[3, b])
            for a in range(4):
                if b in (0, 3):
                    cedge[2 * (base + a) + b // 3, spare(t), :] = values[a, b]
    for group in range(groups):
        for b in range(4):
            column = [source_ref[plane(group, a, b), tile(t), :] for a in range(4)]
            column[0], column[3] = join_rows(column[0], column[3])
            for a in range(4):
                p = plane(group, a, b)
                if b in (1, 2):
                    diag = mass[a, b] + scales[group] * lap[a, b]
                    inverse = 1.0 / diag
                    diag_ref[p, tile(t), :] = diag
                    u0_ref[p, tile(t), :] = column[a] * inverse
                    minv[p, tile(t), :] = inverse * scales[group]
                else:
                    redge[2 * (group * 4 + a) + b // 3, spare(t), :] = column[a]


def finish(a, low, high, scale_ref, diag_ref, minv, u0_ref, cedge, redge):
    groups = u0_ref.shape[0] // 16
    span = slice(low, high)
    mass_sums = join_cols(cedge, a, low, high)
    lap_sums = join_cols(cedge, 4 + a, low, high)
    for group in range(groups):
        scale = scale_ref[group : group + 1, :]
        source = join_cols(redge, group * 4 + a, low, high)
        for side, b in enumerate((0, 3)):
            diag = mass_sums[side] + scale * lap_sums[side]
            inverse = 1.0 / diag
            diag_ref[plane(group, a, b), span, :] = diag
            u0_ref[plane(group, a, b), span, :] = source[side] * inverse
            minv[plane(group, a, b), span, :] = inverse * scale


def operator_tile(t, own, sums, now_ref, old_ref, new_ref, mass_ref, krow, kcol, minv, w_ref, edge):
    groups = now_ref.shape[0] // 16
    zero = jnp.zeros((8, LANES), jnp.float32)
    sums = list(sums)
    for group in range(groups):
        u = [[now_ref[plane(group, a, b), tile(t), :] for b in range(4)] for a in range(4)]
        along_rows = [
            line_operator(
                [krow[line * 6 + i, tile(t), :] for i in range(6)], [u[a][line] for a in range(4)]
            )
            for line in range(4)
        ]
        along_cols = [
            line_operator([kcol[line * 6 + i, tile(t), :] for i in range(6)], u[line])
            for line in range(4)
        ]
        with_now, with_old = zero, zero
        y = [[None] * 4 for _ in range(4)]
        for a in range(4):
            for b in range(4):
                p = plane(group, a, b)
                value = mass_ref[p, tile(t), :] * u[a][b]
                row, col = along_rows[b][a], along_cols[a][b]
                value = value - row if a == 3 else value + row
                value = value - col if b == 3 else value + col
                y[a][b] = value
                with_now += u[a][b] * value
                if old_ref is None:
                    with_old += w_ref[p, tile(t), :] * u[a][b]
                else:
                    with_old += old_ref[p, tile(t), :] * value
        sums[group] += with_now if own is None else own * with_now
        sums[groups + group] += with_old if own is None else own * with_old
        for b in range(4):
            column = [y[a][b] for a in range(4)]
            column[0], column[3] = join_rows_in_turn(column[0], column[3])
            for a in range(4):
                p = plane(group, a, b)
                if b in (1, 2):
                    if new_ref is None:
                        w_ref[p, tile(t), :] = column[a]
                    else:
                        new_ref[p, tile(t), :] = column[a] * minv[p, tile(t), :] - u[a][b]
                else:
                    edge[2 * (group * 4 + a) + b // 3, spare(t), :] = column[a]
    return tuple(sums)


def prep_kernel(t_ref, rim_ref, scale_ref, *refs):
    state, (u1_ref, edge, sums_ref) = refs[:9], refs[9:]
    mass_ref, krow, kcol, diag_ref, minv, u0_ref, w_ref, cedge, redge = state
    cols = t_ref.shape[1]
    rim = lax.broadcasted_iota(jnp.int32, (8, LANES), 1) < RIM

    @pl.loop(0, cols // 8)
    def _(t):
        def fetch(p):
            group, a, b = p // 16, p // 4 % 4, p % 4
            outer = rim_ref[t, group, pl.ds(b, 8, stride=4), :]
            if a:
                outer = pltpu.roll(outer, LANES - a * RIM, 1)
            return jnp.where(rim, outer, t_ref[p, tile(t), :])

        prepare(t, fetch, scale_ref, *state)

    @pl.loop(0, 4)
    def _(a):
        finish(a, 8, cols - 8, scale_ref, diag_ref, minv, u0_ref, cedge, redge)

    zero = jnp.zeros((8, LANES), jnp.float32)
    sums = lax.fori_loop(
        1,
        cols // 8 - 1,
        lambda t, sums: operator_tile(
            t, None, sums, u0_ref, None, u1_ref, mass_ref, krow, kcol, minv, w_ref, edge
        ),
        (zero,) * sums_ref.shape[0],
    )
    for i, value in enumerate(sums):
        sums_ref[i] = value


def krylov_kernel(cols, count, right_ref, left_ref, scale_ref, *refs):
    state = refs[count : count + 9]
    u1_ref, edge, sums_ref, u2_ref, part_ref = refs[count + 9 :]
    mass_ref, krow, kcol, diag_ref, minv, u0_ref, w_ref, cedge, redge = state
    groups = u0_ref.shape[0] // 16
    total = u0_ref.shape[1]
    tiles = total // 8
    own_tiles = cols // 8
    scales = [scale_ref[group : group + 1, :] for group in range(groups)]
    prepare(
        own_tiles, lambda p: jnp.concatenate([right_ref[p], left_ref[p]], axis=0), scale_ref, *state
    )

    @pl.loop(0, 4)
    def _(a):
        wrap_cols(cedge, a, total)
        wrap_cols(cedge, 4 + a, total)
        for group in range(groups):
            wrap_cols(redge, group * 4 + a, total)
        for low, high in ((0, 8), (cols - 8, total)):
            finish(a, low, high, scale_ref, diag_ref, minv, u0_ref, cedge, redge)

    zero = jnp.zeros((8, LANES), jnp.float32)
    shared = (mass_ref, krow, kcol, minv, w_ref, edge)

    def apply(now_ref, old_ref, new_ref):
        def body(i, sums):
            if old_ref is None:
                t = jnp.where(i == 0, 0, i + own_tiles - 2)
            else:
                t = i
            own = (t < own_tiles).astype(jnp.float32)
            return operator_tile(t, own, sums, now_ref, old_ref, new_ref, *shared)

        if old_ref is None:
            sums = lax.fori_loop(0, 3, body, tuple(sums_ref[i] for i in range(2 * groups)))
        else:
            sums = lax.fori_loop(0, tiles, body, (zero,) * (2 * groups))

        @pl.loop(0, groups * 4)
        def _(i):
            wrap_cols(edge, i, total)
            for b, value in zip((0, 3), join_cols(edge, i, 0, total)):
                p = i * 4 + b
                if new_ref is None:
                    w_ref[p] = value
                else:
                    new_ref[p] = value * minv[p] - now_ref[p]

        return sums[:groups], sums[groups:]

    g00, b0 = apply(u0_ref, None, u1_ref)
    g11, g01 = apply(u1_ref, u0_ref, u2_ref)
    g22, g12 = apply(u2_ref, u1_ref, None)
    rows = [jnp.sum(x, axis=0, keepdims=True) for x in b0]
    for q in (g00, g01, g11, g12, g22):
        rows += [scale * jnp.sum(x, axis=0, keepdims=True) for scale, x in zip(scales, q)]
    rows += [jnp.zeros((1, LANES), jnp.float32)] * (-len(rows) % 8)
    table = jnp.concatenate(rows, axis=0)
    lanes = lax.broadcasted_iota(jnp.int32, table.shape, 1)
    lines = lax.broadcasted_iota(jnp.int32, table.shape, 0)
    table = jnp.where(lanes >= RIM, table, 0.0)
    table = over_rows(table)
    table = jnp.where(lanes // PACK == lines, table, 0.0)
    part_ref[...] = jnp.broadcast_to(jnp.sum(table, axis=0, keepdims=True), part_ref.shape)


def combine_kernel(
    parts_ref, scale_ref, u0_ref, u1_ref, u2_ref, w_ref, diag_ref, sol_hbm, res_hbm, sol, res, xs, xt, sems
):
    halves, modes, rows, _ = sol.shape
    groups = modes // PACK
    own = rows // 4
    per_half = LANES // 4
    total = jnp.sum(parts_ref[...], axis=0, keepdims=True)
    table = jnp.broadcast_to(total, (24, LANES))
    lanes = lax.broadcasted_iota(jnp.int32, table.shape, 1)
    lines = lax.broadcasted_iota(jnp.int32, table.shape, 0)
    table = jnp.where(lanes // PACK == lines, table, 0.0)
    table = over_rows(table)
    b0, g00, g01, g11, g12, g22 = [table[q * groups : (q + 1) * groups] for q in range(6)]
    g02 = g11
    b1 = g00 - b0
    b2 = g01 - b1
    l10 = g01 / g00
    l20 = g02 / g00
    d1 = g11 - l10 * g01
    t12 = g12 - l20 * g01
    l21 = t12 / d1
    d2 = g22 - l20 * g02 - l21 * t12
    y1 = b1 - l10 * b0
    y2 = b2 - l20 * b0 - l21 * y1
    c2 = y2 / d2
    c1 = y1 / d1 - l21 * c2
    c0 = b0 / g00 - l10 * c1 - l20 * c2
    copies = []
    for half in range(halves):
        span = slice(half * per_half, (half + 1) * per_half)
        for group in range(groups):
            k0, k1, k2 = [c[group : group + 1, :] for c in (c0, c1, c2)]
            r0, r1, r2 = 1.0 - k0, k0 + k1, k2 * scale_ref[group : group + 1, :]
            for a in range(4):
                slot = group * 4 + a
                for b in range(4):
                    p = plane(group, a, b)
                    u0, u1, u2 = u0_ref[p, span, :], u1_ref[p, span, :], u2_ref[p, span, :]
                    xs[0, slot, pl.ds(b, per_half, stride=4), :] = k0 * u0 + k1 * u1 + k2 * u2
                    xs[1, slot, pl.ds(b, per_half, stride=4), :] = (
                        diag_ref[p, span, :] * (r0 * u0 - r1 * u1 - k1 * u2) - r2 * w_ref[p, span, :]
                    )
                for i, out in enumerate((sol, res)):
                    xt[i, slot] = xs[i, slot].T
                    for m in range(PACK):
                        out[half, group * PACK + m, pl.ds(a, own, stride=4), :] = xt[
                            i, slot, pl.ds(RIM + m, own, stride=PACK), :
                        ]
            span_modes = pl.ds(group * PACK, PACK)
            for i, (out, hbm) in enumerate(((sol, sol_hbm), (res, res_hbm))):
                copy = pltpu.make_async_copy(
                    out.at[half, span_modes],
                    hbm.at[span_modes, :, pl.ds(half * LANES, LANES)],
                    sems.at[half, group, i],
                )
                copy.start()
                copies.append(copy)
    for copy in copies:
        copy.wait()


def shards(forcing, metric, jacobian, mode_scale):
    modes, rows, cols = forcing.shape
    groups = modes // PACK
    halo = 4 * GHOST
    f32 = jnp.float32

    def shift(x, axis, step):
        count = lax.axis_size(axis)
        return lax.ppermute(x, axis, [(i, (i + step) % count) for i in range(count)])

    vmem = pl.BlockSpec(memory_space=pltpu.VMEM)
    anywhere = pl.BlockSpec(memory_space=pl.ANY)
    array = lambda *shape: jax.ShapeDtypeStruct(shape, f32)
    planes = 16 * (groups + 1)
    ecols = cols // 4
    halves = cols // LANES
    inputs = [
        pltpu.with_memory_space_constraint(x, pltpu.HBM)
        for x in (forcing, metric, jacobian, mode_scale)
    ]
    top, bottom, scale = pl.pallas_call(
        load_kernel,
        in_specs=[anywhere] * 4,
        out_specs=[vmem] * 3,
        out_shape=[array(halves, modes + 2, halo, LANES)] * 2 + [array(groups, LANES)],
        scratch_shapes=[
            pltpu.SMEM((modes,), f32),
            pltpu.SemaphoreType.DMA((2, halves, 3)),
            pltpu.SemaphoreType.DMA,
        ],
        compiler_params=pltpu.CompilerParams(vmem_limit_bytes=4 << 20),
        name="load",
    )(*inputs)
    up = shift(bottom, "curve", 1)
    down = shift(top, "curve", -1)

    spread = pl.pallas_call(
        spread_kernel,
        in_specs=[anywhere] * 3,
        out_specs=vmem,
        out_shape=array(planes, ecols, LANES),
        scratch_shapes=[
            pltpu.VMEM((halves, modes + 2, rows, LANES), f32),
            pltpu.VMEM((halves * planes // 4, LANES, LANES), f32),
            pltpu.VMEM((halves * planes // 4, LANES, LANES), f32),
            pltpu.SemaphoreType.DMA((halves, 3)),
        ],
        compiler_params=pltpu.CompilerParams(vmem_limit_bytes=12 << 20),
        cost_estimate=pl.CostEstimate(flops=10_000_000, bytes_accessed=0, transcendentals=0),
        name="spread",
    )(*inputs[:3])
    rim, low, high = pl.pallas_call(
        ghost_kernel,
        in_specs=[vmem] * 3,
        out_specs=[vmem] * 3,
        out_shape=[array(ecols // 8, groups + 1, 32, LANES)] + [array(planes, GHOST, LANES)] * 2,
        scratch_shapes=[
            pltpu.VMEM((halves * (groups + 1), LANES, LANES), f32),
            pltpu.VMEM((2, planes // 4, 4 * GHOST, LANES), f32),
        ],
        compiler_params=pltpu.CompilerParams(vmem_limit_bytes=12 << 20),
        name="ghost",
    )(up, down, spread)

    left = shift(high, "sub", 1)
    right = shift(low, "sub", -1)

    total = ecols + 2 * GHOST
    field = array(16 * groups, total, LANES)
    lines = array(24, total, LANES)
    state = pl.pallas_call(
        prep_kernel,
        in_specs=[vmem] * 3,
        out_specs=[vmem] * 12,
        out_shape=[field, lines, lines, field, field, field, field]
        + [array(16, total + 16, LANES), array(8 * groups, total + 16, LANES)]
        + [field, array(8 * groups, total + 16, LANES), array(2 * groups, 8, LANES)],
        compiler_params=pltpu.CompilerParams(vmem_limit_bytes=24 << 20),
        cost_estimate=pl.CostEstimate(flops=20_000_000, bytes_accessed=0, transcendentals=0),
        name="prep",
    )(spread, rim, scale)
    devices = lax.axis_size(AXES[0]) * lax.axis_size(AXES[1])
    count = len(state)
    out = pl.pallas_call(
        functools.partial(krylov_kernel, ecols, count),
        in_specs=[vmem] * (3 + count),
        out_specs=[vmem] * (count + 2),
        out_shape=[array(*x.shape) for x in state] + [field, array(devices, LANES)],
        input_output_aliases={3 + i: i for i in range(count)},
        compiler_params=pltpu.CompilerParams(vmem_limit_bytes=24 << 20),
        name="krylov",
    )(right, left, scale, *state)
    diag, u0, w3, u1 = out[3], out[5], out[6], out[9]
    u2, part = out[count:]

    parts = lax.all_to_all(part, AXES, 0, 0, tiled=True)

    out = jax.ShapeDtypeStruct((modes, rows, cols), f32)
    return tuple(
        pl.pallas_call(
            combine_kernel,
            in_specs=[vmem] * 7,
            out_specs=[anywhere] * 2,
            out_shape=[out] * 2,
            scratch_shapes=[
                pltpu.VMEM((halves, modes, rows, LANES), f32),
                pltpu.VMEM((halves, modes, rows, LANES), f32),
                pltpu.VMEM((2, 4 * groups, LANES, LANES), f32),
                pltpu.VMEM((2, 4 * groups, LANES, LANES), f32),
                pltpu.SemaphoreType.DMA((halves, groups, 2)),
            ],
            compiler_params=pltpu.CompilerParams(vmem_limit_bytes=20 << 20),
            name="combine",
        )(parts, scale, u0, u1, u2, w3, diag)
    )


def solution(mesh):
    in_specs = (P(None, "curve", "sub"), P("curve", "sub"), P("curve", "sub"), P())
    out_specs = (P(None, "curve", "sub"), P(None, "curve", "sub"))
    return jax.shard_map(
        shards, mesh=mesh, in_specs=in_specs, out_specs=out_specs, check_vma=False
    )
```

```python
import functools
import math

import jax
import jax.numpy as jnp
import numpy as np
from jax import lax
from jax.experimental import pallas as pl
from jax.experimental.pallas import tpu as pltpu
from jax.sharding import PartitionSpec as P

GHOST = 4
PACK = 4
LANES = 128
AXES = ("curve", "sub")
RIM = 2 * GHOST * PACK


def gll_tables():
    points = np.array([-1.0, -1.0 / math.sqrt(5.0), 1.0 / math.sqrt(5.0), 1.0])
    weights = np.array([1.0 / 6.0, 5.0 / 6.0, 5.0 / 6.0, 1.0 / 6.0])
    factor = np.array(
        [np.prod([points[j] - points[m] for m in range(4) if m != j]) for j in range(4)]
    )
    slopes = np.zeros((4, 4))
    for i in range(4):
        for j in range(4):
            if i != j:
                slopes[i, j] = factor[i] / (factor[j] * (points[i] - points[j]))
        slopes[i, i] = sum((1.0 / (points[i] - points[m]) for m in range(4) if m != i))
    return (slopes, weights)


SLOPES, WEIGHTS = gll_tables()
PAIRS = [(a, k) for a in range(4) for k in range(a + 1, 4)]


def plane(group, a, b):
    return (group * 4 + a) * 4 + b


def stack_copies(f_hbm, metric_hbm, jacobian_hbm, out, at, sems):
    halves, stack, size, _ = out.shape
    span = pl.ds(at, size)
    copies = []
    for half in range(halves):
        columns = pl.ds(half * LANES, LANES)
        pairs = (
            (f_hbm.at[:, span, columns], out.at[half, pl.ds(0, stack - 2)]),
            (metric_hbm.at[span, columns], out.at[half, stack - 2]),
            (jacobian_hbm.at[span, columns], out.at[half, stack - 1]),
        )
        copies.append(
            [pltpu.make_async_copy(x, y, sems.at[half, i]) for i, (x, y) in enumerate(pairs)]
        )
    for per_half in copies:
        for copy in per_half:
            copy.start()
    return copies


def load_kernel(f_hbm, metric_hbm, jacobian_hbm, scale_hbm, top, bottom, scale_ref, scales, sems, scale_sem):
    modes, rows, _ = f_hbm.shape
    halo = top.shape[2]
    scale_copy = pltpu.make_async_copy(scale_hbm, scales, scale_sem)
    scale_copy.start()
    copies = stack_copies(f_hbm, metric_hbm, jacobian_hbm, top, 0, sems.at[0])
    copies += stack_copies(f_hbm, metric_hbm, jacobian_hbm, bottom, rows - halo, sems.at[1])
    scale_copy.wait()
    member = lax.broadcasted_iota(jnp.int32, (1, LANES), 1) % PACK
    for group in range(modes // PACK):
        row = jnp.zeros((1, LANES), jnp.float32)
        for m in range(PACK):
            row = jnp.where(member == m, scales[group * PACK + m], row)
        scale_ref[group : group + 1, :] = row
    for per_half in copies:
        for copy in per_half:
            copy.wait()


def spread_kernel(f_hbm, metric_hbm, jacobian_hbm, t_ref, fields_ref, xs, xt, sems):
    halves, stack, rows, _ = fields_ref.shape
    own = rows // 4
    groups = (stack - 2) // PACK
    per_half = LANES // 4
    copies = stack_copies(f_hbm, metric_hbm, jacobian_hbm, fields_ref, 0, sems)
    for half in range(halves):
        for copy in copies[half]:
            copy.wait()
        for group in range(groups + 1):
            for a in range(4):
                at = (half * (groups + 1) + group) * 4 + a
                for m in range(PACK):
                    index = group * PACK + (m if group < groups else m % 2)
                    xs[at, pl.ds(RIM + m, own, stride=PACK), :] = fields_ref[
                        half, index, pl.ds(a, own, stride=4), :
                    ]
                xs[at, :RIM, :] = jnp.zeros((RIM, LANES), jnp.float32)
                xt[at] = xs[at].T
                for b in range(4):
                    t_ref[plane(group, a, b), half * per_half : (half + 1) * per_half, :] = xt[
                        at, pl.ds(b, per_half, stride=4), :
                    ]


def ghost_kernel(up_ref, down_ref, own_ref, rim_ref, low_ref, high_ref, xs, ends):
    halves, stack, _, _ = up_ref.shape
    groups = (stack - 2) // PACK
    per_half = rim_ref.shape[0] // halves
    height = rim_ref.shape[2]
    rim = lax.broadcasted_iota(jnp.int32, (GHOST, LANES), 1) < RIM
    for half in range(halves):
        for group in range(groups + 1):
            at = half * (groups + 1) + group
            for a in range(4):
                for m in range(PACK):
                    index = group * PACK + (m if group < groups else m % 2)
                    for side, ref in enumerate((down_ref, up_ref)):
                        start = a * RIM + side * GHOST * PACK + m
                        xs[at, pl.ds(start, GHOST, stride=PACK), :] = ref[
                            half, index, pl.ds(a, GHOST, stride=4), :
                        ]
            turned = xs[at].T
            for i in range(per_half):
                rim_ref[half * per_half + i, group] = turned[i * height : (i + 1) * height]
    last = rim_ref.shape[0] - 1
    total = own_ref.shape[1]
    size = 4 * GHOST
    for group in range(groups + 1):
        for a in range(4):
            at = group * 4 + a
            for side, x in enumerate((rim_ref[0, group, :size], rim_ref[last, group, height - size :])):
                ends[side, at] = pltpu.roll(x, LANES - a * RIM, 1) if a else x
            for b in range(4):
                p = at * 4 + b
                picked = pl.ds(b, GHOST, stride=4)
                low_ref[p] = jnp.where(rim, ends[0, at, picked, :], own_ref[p, :GHOST, :])
                high_ref[p] = jnp.where(rim, ends[1, at, picked, :], own_ref[p, total - GHOST :, :])


def line_operator(coefs, values):
    f01, f02, f03, f12, f13, f23 = [
        coef * (values[k] - values[a]) for (a, k), coef in zip(PAIRS, coefs)
    ]
    return f01 + f02 + f03, f12 + f13 - f01, f23 - f02 - f12, f03 + f13 + f23


def over_rows(table):
    i = lax.broadcasted_iota(jnp.int32, (LANES, LANES), 0)
    j = lax.broadcasted_iota(jnp.int32, (LANES, LANES), 1)
    same = jnp.where(i % PACK == j % PACK, 1.0, 0.0).astype(jnp.float32)
    return jnp.dot(
        table, same, precision=lax.Precision.HIGHEST, preferred_element_type=jnp.float32
    )


def tile(t):
    return pl.ds(pl.multiple_of(t * 8, 8), 8)


def spare(t):
    return pl.ds(pl.multiple_of(t * 8 + 8, 8), 8)


def join_rows(first, last):
    return first + pltpu.roll(last, PACK, 1), last + pltpu.roll(first, LANES - PACK, 1)


def join_rows_in_turn(first, last):
    shared = last + pltpu.roll(first, LANES - PACK, 1)
    return pltpu.roll(shared, PACK, 1), shared


def wrap_cols(edge, i, total):
    edge[2 * i, total + 8 : total + 16, :] = edge[2 * i, 8:16, :]
    edge[2 * i + 1, 0:8, :] = edge[2 * i + 1, total : total + 8, :]


def join_cols(edge, i, low, high):
    first = edge[2 * i, low + 8 : high + 8, :] + edge[2 * i + 1, low + 7 : high + 7, :]
    last = edge[2 * i + 1, low + 8 : high + 8, :] + edge[2 * i, low + 9 : high + 9, :]
    return first, last


def prepare(t, fetch, scale_ref, mass_ref, krow, kcol, diag_ref, minv, u0_ref, source_ref, cedge, redge):
    groups = u0_ref.shape[0] // 16
    lane = lax.broadcasted_iota(jnp.int32, (8, LANES), 1)
    even = lane % 2 == 0
    grid = [(a, b) for a in range(4) for b in range(4)]
    scales = [scale_ref[group : group + 1, :] for group in range(groups)]
    flux, mass, lap = {}, {}, {}
    for a, b in grid:
        x = fetch(plane(groups, a, b))
        w = np.float32(WEIGHTS[a] * WEIGHTS[b])
        flux[a, b] = jnp.where(even, x, pltpu.roll(x, 1, 1)) * w
        mass[a, b] = jnp.where(even, pltpu.roll(x, LANES - 1, 1), x) * w
    for group in range(groups):
        inverse = 1.0 / scales[group]
        for a, b in grid:
            mass_ref[plane(group, a, b), tile(t), :] = mass[a, b] * inverse
            source_ref[plane(group, a, b), tile(t), :] = fetch(plane(group, a, b)) * mass[a, b]

    def less(a, b, value):
        lap[a, b] = lap[a, b] + value if (a, b) in lap else value

    for line in range(4):
        for i, (p, q) in enumerate(PAIRS):
            c = [np.float32(SLOPES[j, p] * SLOPES[j, q]) for j in range(4)]
            kr = sum(flux[j, line] * c[j] for j in range(4))
            kc = sum(flux[line, j] * c[j] for j in range(4))
            krow[line * 6 + i, tile(t), :] = kr
            kcol[line * 6 + i, tile(t), :] = kc
            less(p, line, kr)
            less(q, line, kr)
            less(line, p, kc)
            less(line, q, kc)
    for a, b in grid:
        lap[a, b] = -lap[a, b]
    for values, base in ((mass, 0), (lap, 4)):
        for b in range(4):
            values[0, b], values[3, b] = join_rows(values[0, b], values[3, b])
            for a in range(4):
                if b in (0, 3):
                    cedge[2 * (base + a) + b // 3, spare(t), :] = values[a, b]
    for group in range(groups):
        for b in range(4):
            column = [source_ref[plane(group, a, b), tile(t), :] for a in range(4)]
            column[0], column[3] = join_rows(column[0], column[3])
            for a in range(4):
                p = plane(group, a, b)
                if b in (1, 2):
                    diag = mass[a, b] + scales[group] * lap[a, b]
                    inverse = 1.0 / diag
                    diag_ref[p, tile(t), :] = diag
                    u0_ref[p, tile(t), :] = column[a] * inverse
                    minv[p, tile(t), :] = inverse * scales[group]
                else:
                    redge[2 * (group * 4 + a) + b // 3, spare(t), :] = column[a]


def finish(a, low, high, scale_ref, diag_ref, minv, u0_ref, cedge, redge):
    groups = u0_ref.shape[0] // 16
    span = slice(low, high)
    mass_sums = join_cols(cedge, a, low, high)
    lap_sums = join_cols(cedge, 4 + a, low, high)
    for group in range(groups):
        scale = scale_ref[group : group + 1, :]
        source = join_cols(redge, group * 4 + a, low, high)
        for side, b in enumerate((0, 3)):
            diag = mass_sums[side] + scale * lap_sums[side]
            inverse = 1.0 / diag
            diag_ref[plane(group, a, b), span, :] = diag
            u0_ref[plane(group, a, b), span, :] = source[side] * inverse
            minv[plane(group, a, b), span, :] = inverse * scale


def operator_tile(t, own, sums, now_ref, old_ref, new_ref, mass_ref, krow, kcol, minv, w_ref, edge):
    groups = now_ref.shape[0] // 16
    zero = jnp.zeros((8, LANES), jnp.float32)
    sums = list(sums)
    for group in range(groups):
        u = [[now_ref[plane(group, a, b), tile(t), :] for b in range(4)] for a in range(4)]
        along_rows = [
            line_operator(
                [krow[line * 6 + i, tile(t), :] for i in range(6)], [u[a][line] for a in range(4)]
            )
            for line in range(4)
        ]
        along_cols = [
            line_operator([kcol[line * 6 + i, tile(t), :] for i in range(6)], u[line])
            for line in range(4)
        ]
        with_now, with_old = zero, zero
        y = [[None] * 4 for _ in range(4)]
        for a in range(4):
            for b in range(4):
                p = plane(group, a, b)
                value = mass_ref[p, tile(t), :] * u[a][b]
                row, col = along_rows[b][a], along_cols[a][b]
                value = value - row if a == 3 else value + row
                value = value - col if b == 3 else value + col
                y[a][b] = value
                with_now += u[a][b] * value
                if old_ref is None:
                    with_old += w_ref[p, tile(t), :] * u[a][b]
                else:
                    with_old += old_ref[p, tile(t), :] * value
        sums[group] += with_now if own is None else own * with_now
        sums[groups + group] += with_old if own is None else own * with_old
        for b in range(4):
            column = [y[a][b] for a in range(4)]
            column[0], column[3] = join_rows_in_turn(column[0], column[3])
            for a in range(4):
                p = plane(group, a, b)
                if b in (1, 2):
                    if new_ref is None:
                        w_ref[p, tile(t), :] = column[a]
                    else:
                        new_ref[p, tile(t), :] = column[a] * minv[p, tile(t), :] - u[a][b]
                else:
                    edge[2 * (group * 4 + a) + b // 3, spare(t), :] = column[a]
    return tuple(sums)


def several(low, high, count, body, sums):
    def step(i, sums):
        for j in range(count):
            sums = body(low + i * count + j, sums)
        return sums

    steps = (high - low) // count
    sums = lax.fori_loop(0, steps, step, sums)
    for t in range(low + steps * count, high):
        sums = body(jnp.int32(t), sums)
    return sums


def prep_kernel(t_ref, rim_ref, scale_ref, *refs):
    state, (u1_ref, edge, sums_ref) = refs[:9], refs[9:]
    mass_ref, krow, kcol, diag_ref, minv, u0_ref, w_ref, cedge, redge = state
    cols = t_ref.shape[1]
    rim = lax.broadcasted_iota(jnp.int32, (8, LANES), 1) < RIM

    @pl.loop(0, cols // 8)
    def _(t):
        def fetch(p):
            group, a, b = p // 16, p // 4 % 4, p % 4
            outer = rim_ref[t, group, pl.ds(b, 8, stride=4), :]
            if a:
                outer = pltpu.roll(outer, LANES - a * RIM, 1)
            return jnp.where(rim, outer, t_ref[p, tile(t), :])

        prepare(t, fetch, scale_ref, *state)

    @pl.loop(0, 4)
    def _(a):
        finish(a, 8, cols - 8, scale_ref, diag_ref, minv, u0_ref, cedge, redge)

    zero = jnp.zeros((8, LANES), jnp.float32)
    sums = several(
        1,
        cols // 8 - 1,
        3,
        lambda t, sums: operator_tile(
            t, None, sums, u0_ref, None, u1_ref, mass_ref, krow, kcol, minv, w_ref, edge
        ),
        (zero,) * sums_ref.shape[0],
    )
    for i, value in enumerate(sums):
        sums_ref[i] = value


def krylov_kernel(cols, count, right_ref, left_ref, scale_ref, *refs):
    state = refs[count : count + 9]
    u1_ref, edge, sums_ref, u2_ref, part_ref = refs[count + 9 :]
    mass_ref, krow, kcol, diag_ref, minv, u0_ref, w_ref, cedge, redge = state
    groups = u0_ref.shape[0] // 16
    total = u0_ref.shape[1]
    tiles = total // 8
    own_tiles = cols // 8
    scales = [scale_ref[group : group + 1, :] for group in range(groups)]
    prepare(
        own_tiles, lambda p: jnp.concatenate([right_ref[p], left_ref[p]], axis=0), scale_ref, *state
    )

    @pl.loop(0, 4)
    def _(a):
        wrap_cols(cedge, a, total)
        wrap_cols(cedge, 4 + a, total)
        for group in range(groups):
            wrap_cols(redge, group * 4 + a, total)
        for low, high in ((0, 8), (cols - 8, total)):
            finish(a, low, high, scale_ref, diag_ref, minv, u0_ref, cedge, redge)

    zero = jnp.zeros((8, LANES), jnp.float32)
    shared = (mass_ref, krow, kcol, minv, w_ref, edge)

    def apply(now_ref, old_ref, new_ref):
        def body(i, sums):
            if old_ref is None:
                t = jnp.where(i == 0, 0, i + own_tiles - 2)
            else:
                t = i
            own = (t < own_tiles).astype(jnp.float32)
            return operator_tile(t, own, sums, now_ref, old_ref, new_ref, *shared)

        if old_ref is None:
            sums = several(0, 3, 3, body, tuple(sums_ref[i] for i in range(2 * groups)))
        else:
            sums = several(0, tiles, 3, body, (zero,) * (2 * groups))

        @pl.loop(0, groups * 4)
        def _(i):
            wrap_cols(edge, i, total)
            for b, value in zip((0, 3), join_cols(edge, i, 0, total)):
                p = i * 4 + b
                if new_ref is None:
                    w_ref[p] = value
                else:
                    new_ref[p] = value * minv[p] - now_ref[p]

        return sums[:groups], sums[groups:]

    g00, b0 = apply(u0_ref, None, u1_ref)
    g11, g01 = apply(u1_ref, u0_ref, u2_ref)
    g22, g12 = apply(u2_ref, u1_ref, None)
    rows = [jnp.sum(x, axis=0, keepdims=True) for x in b0]
    for q in (g00, g01, g11, g12, g22):
        rows += [scale * jnp.sum(x, axis=0, keepdims=True) for scale, x in zip(scales, q)]
    rows += [jnp.zeros((1, LANES), jnp.float32)] * (-len(rows) % 8)
    table = jnp.concatenate(rows, axis=0)
    lanes = lax.broadcasted_iota(jnp.int32, table.shape, 1)
    lines = lax.broadcasted_iota(jnp.int32, table.shape, 0)
    table = jnp.where(lanes >= RIM, table, 0.0)
    table = over_rows(table)
    table = jnp.where(lanes // PACK == lines, table, 0.0)
    part_ref[...] = jnp.broadcast_to(jnp.sum(table, axis=0, keepdims=True), part_ref.shape)


def combine_kernel(
    parts_ref, scale_ref, u0_ref, u1_ref, u2_ref, w_ref, diag_ref, sol_hbm, res_hbm, sol, res, xs, xt, sems
):
    halves, modes, rows, _ = sol.shape
    groups = modes // PACK
    own = rows // 4
    per_half = LANES // 4
    total = jnp.sum(parts_ref[...], axis=0, keepdims=True)
    table = jnp.broadcast_to(total, (24, LANES))
    lanes = lax.broadcasted_iota(jnp.int32, table.shape, 1)
    lines = lax.broadcasted_iota(jnp.int32, table.shape, 0)
    table = jnp.where(lanes // PACK == lines, table, 0.0)
    table = over_rows(table)
    b0, g00, g01, g11, g12, g22 = [table[q * groups : (q + 1) * groups] for q in range(6)]
    g02 = g11
    b1 = g00 - b0
    b2 = g01 - b1
    l10 = g01 / g00
    l20 = g02 / g00
    d1 = g11 - l10 * g01
    t12 = g12 - l20 * g01
    l21 = t12 / d1
    d2 = g22 - l20 * g02 - l21 * t12
    y1 = b1 - l10 * b0
    y2 = b2 - l20 * b0 - l21 * y1
    c2 = y2 / d2
    c1 = y1 / d1 - l21 * c2
    c0 = b0 / g00 - l10 * c1 - l20 * c2
    copies = []
    for half in range(halves):
        span = slice(half * per_half, (half + 1) * per_half)
        for group in range(groups):
            k0, k1, k2 = [c[group : group + 1, :] for c in (c0, c1, c2)]
            r0, r1, r2 = 1.0 - k0, k0 + k1, k2 * scale_ref[group : group + 1, :]
            for a in range(4):
                slot = group * 4 + a
                for b in range(4):
                    p = plane(group, a, b)
                    u0, u1, u2 = u0_ref[p, span, :], u1_ref[p, span, :], u2_ref[p, span, :]
                    xs[0, slot, pl.ds(b, per_half, stride=4), :] = k0 * u0 + k1 * u1 + k2 * u2
                    xs[1, slot, pl.ds(b, per_half, stride=4), :] = (
                        diag_ref[p, span, :] * (r0 * u0 - r1 * u1 - k1 * u2) - r2 * w_ref[p, span, :]
                    )
                for i, out in enumerate((sol, res)):
                    xt[i, slot] = xs[i, slot].T
                    for m in range(PACK):
                        out[half, group * PACK + m, pl.ds(a, own, stride=4), :] = xt[
                            i, slot, pl.ds(RIM + m, own, stride=PACK), :
                        ]
            span_modes = pl.ds(group * PACK, PACK)
            for i, (out, hbm) in enumerate(((sol, sol_hbm), (res, res_hbm))):
                copy = pltpu.make_async_copy(
                    out.at[half, span_modes],
                    hbm.at[span_modes, :, pl.ds(half * LANES, LANES)],
                    sems.at[half, group, i],
                )
                copy.start()
                copies.append(copy)
    for copy in copies:
        copy.wait()


def shards(forcing, metric, jacobian, mode_scale):
    modes, rows, cols = forcing.shape
    groups = modes // PACK
    halo = 4 * GHOST
    f32 = jnp.float32

    def shift(x, axis, step):
        count = lax.axis_size(axis)
        return lax.ppermute(x, axis, [(i, (i + step) % count) for i in range(count)])

    vmem = pl.BlockSpec(memory_space=pltpu.VMEM)
    anywhere = pl.BlockSpec(memory_space=pl.ANY)
    array = lambda *shape: jax.ShapeDtypeStruct(shape, f32)
    planes = 16 * (groups + 1)
    ecols = cols // 4
    halves = cols // LANES
    inputs = [
        pltpu.with_memory_space_constraint(x, pltpu.HBM)
        for x in (forcing, metric, jacobian, mode_scale)
    ]
    top, bottom, scale = pl.pallas_call(
        load_kernel,
        in_specs=[anywhere] * 4,
        out_specs=[vmem] * 3,
        out_shape=[array(halves, modes + 2, halo, LANES)] * 2 + [array(groups, LANES)],
        scratch_shapes=[
            pltpu.SMEM((modes,), f32),
            pltpu.SemaphoreType.DMA((2, halves, 3)),
            pltpu.SemaphoreType.DMA,
        ],
        compiler_params=pltpu.CompilerParams(vmem_limit_bytes=4 << 20),
        name="load",
    )(*inputs)
    up = shift(bottom, "curve", 1)
    down = shift(top, "curve", -1)

    spread = pl.pallas_call(
        spread_kernel,
        in_specs=[anywhere] * 3,
        out_specs=vmem,
        out_shape=array(planes, ecols, LANES),
        scratch_shapes=[
            pltpu.VMEM((halves, modes + 2, rows, LANES), f32),
            pltpu.VMEM((halves * planes // 4, LANES, LANES), f32),
            pltpu.VMEM((halves * planes // 4, LANES, LANES), f32),
            pltpu.SemaphoreType.DMA((halves, 3)),
        ],
        compiler_params=pltpu.CompilerParams(vmem_limit_bytes=12 << 20),
        cost_estimate=pl.CostEstimate(flops=10_000_000, bytes_accessed=0, transcendentals=0),
        name="spread",
    )(*inputs[:3])
    rim, low, high = pl.pallas_call(
        ghost_kernel,
        in_specs=[vmem] * 3,
        out_specs=[vmem] * 3,
        out_shape=[array(ecols // 8, groups + 1, 32, LANES)] + [array(planes, GHOST, LANES)] * 2,
        scratch_shapes=[
            pltpu.VMEM((halves * (groups + 1), LANES, LANES), f32),
            pltpu.VMEM((2, planes // 4, 4 * GHOST, LANES), f32),
        ],
        compiler_params=pltpu.CompilerParams(vmem_limit_bytes=12 << 20),
        name="ghost",
    )(up, down, spread)

    left = shift(high, "sub", 1)
    right = shift(low, "sub", -1)

    total = ecols + 2 * GHOST
    field = array(16 * groups, total, LANES)
    lines = array(24, total, LANES)
    state = pl.pallas_call(
        prep_kernel,
        in_specs=[vmem] * 3,
        out_specs=[vmem] * 12,
        out_shape=[field, lines, lines, field, field, field, field]
        + [array(16, total + 16, LANES), array(8 * groups, total + 16, LANES)]
        + [field, array(8 * groups, total + 16, LANES), array(2 * groups, 8, LANES)],
        compiler_params=pltpu.CompilerParams(vmem_limit_bytes=24 << 20),
        cost_estimate=pl.CostEstimate(flops=20_000_000, bytes_accessed=0, transcendentals=0),
        name="prep",
    )(spread, rim, scale)
    devices = lax.axis_size(AXES[0]) * lax.axis_size(AXES[1])
    count = len(state)
    out = pl.pallas_call(
        functools.partial(krylov_kernel, ecols, count),
        in_specs=[vmem] * (3 + count),
        out_specs=[vmem] * (count + 2),
        out_shape=[array(*x.shape) for x in state] + [field, array(devices, LANES)],
        input_output_aliases={3 + i: i for i in range(count)},
        compiler_params=pltpu.CompilerParams(vmem_limit_bytes=24 << 20),
        name="krylov",
    )(right, left, scale, *state)
    diag, u0, w3, u1 = out[3], out[5], out[6], out[9]
    u2, part = out[count:]

    parts = lax.all_to_all(part, AXES, 0, 0, tiled=True)

    out = jax.ShapeDtypeStruct((modes, rows, cols), f32)
    return tuple(
        pl.pallas_call(
            combine_kernel,
            in_specs=[vmem] * 7,
            out_specs=[anywhere] * 2,
            out_shape=[out] * 2,
            scratch_shapes=[
                pltpu.VMEM((halves, modes, rows, LANES), f32),
                pltpu.VMEM((halves, modes, rows, LANES), f32),
                pltpu.VMEM((2, 4 * groups, LANES, LANES), f32),
                pltpu.VMEM((2, 4 * groups, LANES, LANES), f32),
                pltpu.SemaphoreType.DMA((halves, groups, 2)),
            ],
            compiler_params=pltpu.CompilerParams(vmem_limit_bytes=20 << 20),
            name="combine",
        )(parts, scale, u0, u1, u2, w3, diag)
    )


def solution(mesh):
    in_specs = (P(None, "curve", "sub"), P("curve", "sub"), P("curve", "sub"), P())
    out_specs = (P(None, "curve", "sub"), P(None, "curve", "sub"))
    return jax.shard_map(
        shards, mesh=mesh, in_specs=in_specs, out_specs=out_specs, check_vma=False
    )
```

```python
import functools
import math

import jax
import jax.numpy as jnp
import numpy as np
from jax import lax
from jax.experimental import pallas as pl
from jax.experimental.pallas import tpu as pltpu
from jax.sharding import PartitionSpec as P

GHOST = 4
PACK = 4
LANES = 128
AXES = ("curve", "sub")
RIM = 2 * GHOST * PACK


def gll_tables():
    points = np.array([-1.0, -1.0 / math.sqrt(5.0), 1.0 / math.sqrt(5.0), 1.0])
    weights = np.array([1.0 / 6.0, 5.0 / 6.0, 5.0 / 6.0, 1.0 / 6.0])
    factor = np.array(
        [np.prod([points[j] - points[m] for m in range(4) if m != j]) for j in range(4)]
    )
    slopes = np.zeros((4, 4))
    for i in range(4):
        for j in range(4):
            if i != j:
                slopes[i, j] = factor[i] / (factor[j] * (points[i] - points[j]))
        slopes[i, i] = sum((1.0 / (points[i] - points[m]) for m in range(4) if m != i))
    return (slopes, weights)


SLOPES, WEIGHTS = gll_tables()
PAIRS = [(a, k) for a in range(4) for k in range(a + 1, 4)]


def plane(group, a, b):
    return (group * 4 + a) * 4 + b


def stack_copies(f_hbm, metric_hbm, jacobian_hbm, out, at, sems):
    halves, stack, size, _ = out.shape
    span = pl.ds(at, size)
    copies = []
    for half in range(halves):
        columns = pl.ds(half * LANES, LANES)
        pairs = (
            (f_hbm.at[:, span, columns], out.at[half, pl.ds(0, stack - 2)]),
            (metric_hbm.at[span, columns], out.at[half, stack - 2]),
            (jacobian_hbm.at[span, columns], out.at[half, stack - 1]),
        )
        copies.append(
            [pltpu.make_async_copy(x, y, sems.at[half, i]) for i, (x, y) in enumerate(pairs)]
        )
    for per_half in copies:
        for copy in per_half:
            copy.start()
    return copies


def load_kernel(f_hbm, metric_hbm, jacobian_hbm, scale_hbm, top, bottom, scale_ref, scales, sems, scale_sem):
    modes, rows, _ = f_hbm.shape
    halo = top.shape[2]
    scale_copy = pltpu.make_async_copy(scale_hbm, scales, scale_sem)
    scale_copy.start()
    copies = stack_copies(f_hbm, metric_hbm, jacobian_hbm, top, 0, sems.at[0])
    copies += stack_copies(f_hbm, metric_hbm, jacobian_hbm, bottom, rows - halo, sems.at[1])
    scale_copy.wait()
    member = lax.broadcasted_iota(jnp.int32, (1, LANES), 1) % PACK
    for group in range(modes // PACK):
        row = jnp.zeros((1, LANES), jnp.float32)
        for m in range(PACK):
            row = jnp.where(member == m, scales[group * PACK + m], row)
        scale_ref[group : group + 1, :] = row
    for per_half in copies:
        for copy in per_half:
            copy.wait()


def spread_kernel(f_hbm, metric_hbm, jacobian_hbm, t_ref, fields_ref, xs, xt, sems):
    halves, stack, rows, _ = fields_ref.shape
    own = rows // 4
    groups = (stack - 2) // PACK
    per_half = LANES // 4
    copies = stack_copies(f_hbm, metric_hbm, jacobian_hbm, fields_ref, 0, sems)
    for half in range(halves):
        for copy in copies[half]:
            copy.wait()
        for group in range(groups + 1):
            for a in range(4):
                at = (half * (groups + 1) + group) * 4 + a
                for m in range(PACK):
                    index = group * PACK + (m if group < groups else m % 2)
                    xs[at, pl.ds(RIM + m, own, stride=PACK), :] = fields_ref[
                        half, index, pl.ds(a, own, stride=4), :
                    ]
                xs[at, :RIM, :] = jnp.zeros((RIM, LANES), jnp.float32)
                xt[at] = xs[at].T
                for b in range(4):
                    t_ref[plane(group, a, b), half * per_half : (half + 1) * per_half, :] = xt[
                        at, pl.ds(b, per_half, stride=4), :
                    ]


def ghost_kernel(up_ref, down_ref, own_ref, rim_ref, low_ref, high_ref, xs, ends):
    halves, stack, _, _ = up_ref.shape
    groups = (stack - 2) // PACK
    per_half = rim_ref.shape[0] // halves
    height = rim_ref.shape[2]
    rim = lax.broadcasted_iota(jnp.int32, (GHOST, LANES), 1) < RIM
    for half in range(halves):
        for group in range(groups + 1):
            at = half * (groups + 1) + group
            for a in range(4):
                for m in range(PACK):
                    index = group * PACK + (m if group < groups else m % 2)
                    for side, ref in enumerate((down_ref, up_ref)):
                        start = a * RIM + side * GHOST * PACK + m
                        xs[at, pl.ds(start, GHOST, stride=PACK), :] = ref[
                            half, index, pl.ds(a, GHOST, stride=4), :
                        ]
            turned = xs[at].T
            for i in range(per_half):
                rim_ref[half * per_half + i, group] = turned[i * height : (i + 1) * height]
    last = rim_ref.shape[0] - 1
    total = own_ref.shape[1]
    size = 4 * GHOST
    for group in range(groups + 1):
        for a in range(4):
            at = group * 4 + a
            for side, x in enumerate((rim_ref[0, group, :size], rim_ref[last, group, height - size :])):
                ends[side, at] = pltpu.roll(x, LANES - a * RIM, 1) if a else x
            for b in range(4):
                p = at * 4 + b
                picked = pl.ds(b, GHOST, stride=4)
                low_ref[p] = jnp.where(rim, ends[0, at, picked, :], own_ref[p, :GHOST, :])
                high_ref[p] = jnp.where(rim, ends[1, at, picked, :], own_ref[p, total - GHOST :, :])


def line_operator(coefs, values):
    f01, f02, f03, f12, f13, f23 = [
        coef * (values[k] - values[a]) for (a, k), coef in zip(PAIRS, coefs)
    ]
    return f01 + f02 + f03, f12 + f13 - f01, f23 - f02 - f12, f03 + f13 + f23


def over_rows(table):
    i = lax.broadcasted_iota(jnp.int32, (LANES, LANES), 0)
    j = lax.broadcasted_iota(jnp.int32, (LANES, LANES), 1)
    same = jnp.where(i % PACK == j % PACK, 1.0, 0.0).astype(jnp.float32)
    return jnp.dot(
        table, same, precision=lax.Precision.HIGHEST, preferred_element_type=jnp.float32
    )


def tile(t):
    return pl.ds(pl.multiple_of(t * 8, 8), 8)


def spare(t):
    return pl.ds(pl.multiple_of(t * 8 + 8, 8), 8)


def join_rows(first, last):
    return first + pltpu.roll(last, PACK, 1), last + pltpu.roll(first, LANES - PACK, 1)


def join_rows_in_turn(first, last):
    shared = last + pltpu.roll(first, LANES - PACK, 1)
    return pltpu.roll(shared, PACK, 1), shared


def wrap_cols(edge, i, total):
    edge[2 * i, total + 8 : total + 16, :] = edge[2 * i, 8:16, :]
    edge[2 * i + 1, 0:8, :] = edge[2 * i + 1, total : total + 8, :]


def join_cols(edge, i, low, high):
    first = edge[2 * i, low + 8 : high + 8, :] + edge[2 * i + 1, low + 7 : high + 7, :]
    last = edge[2 * i + 1, low + 8 : high + 8, :] + edge[2 * i, low + 9 : high + 9, :]
    return first, last


def prepare(t, fetch, scale_ref, mass_ref, krow, kcol, diag_ref, minv, u0_ref, source_ref, cedge, redge):
    groups = u0_ref.shape[0] // 16
    lane = lax.broadcasted_iota(jnp.int32, (8, LANES), 1)
    even = lane % 2 == 0
    grid = [(a, b) for a in range(4) for b in range(4)]
    scales = [scale_ref[group : group + 1, :] for group in range(groups)]
    flux, mass, lap = {}, {}, {}
    for a, b in grid:
        x = fetch(plane(groups, a, b))
        w = np.float32(WEIGHTS[a] * WEIGHTS[b])
        flux[a, b] = jnp.where(even, x, pltpu.roll(x, 1, 1)) * w
        mass[a, b] = jnp.where(even, pltpu.roll(x, LANES - 1, 1), x) * w
    for group in range(groups):
        inverse = 1.0 / scales[group]
        for a, b in grid:
            mass_ref[plane(group, a, b), tile(t), :] = mass[a, b] * inverse
            source_ref[plane(group, a, b), tile(t), :] = fetch(plane(group, a, b)) * mass[a, b]

    def less(a, b, value):
        lap[a, b] = lap[a, b] + value if (a, b) in lap else value

    for line in range(4):
        for i, (p, q) in enumerate(PAIRS):
            c = [np.float32(SLOPES[j, p] * SLOPES[j, q]) for j in range(4)]
            kr = sum(flux[j, line] * c[j] for j in range(4))
            kc = sum(flux[line, j] * c[j] for j in range(4))
            krow[line * 6 + i, tile(t), :] = kr
            kcol[line * 6 + i, tile(t), :] = kc
            less(p, line, kr)
            less(q, line, kr)
            less(line, p, kc)
            less(line, q, kc)
    for a, b in grid:
        lap[a, b] = -lap[a, b]
    for values, base in ((mass, 0), (lap, 4)):
        for b in range(4):
            values[0, b], values[3, b] = join_rows(values[0, b], values[3, b])
            for a in range(4):
                if b in (0, 3):
                    cedge[2 * (base + a) + b // 3, spare(t), :] = values[a, b]
    for group in range(groups):
        for b in range(4):
            column = [source_ref[plane(group, a, b), tile(t), :] for a in range(4)]
            column[0], column[3] = join_rows(column[0], column[3])
            for a in range(4):
                p = plane(group, a, b)
                if b in (1, 2):
                    diag = mass[a, b] + scales[group] * lap[a, b]
                    inverse = 1.0 / diag
                    diag_ref[p, tile(t), :] = diag
                    u0_ref[p, tile(t), :] = column[a] * inverse
                    minv[p, tile(t), :] = inverse * scales[group]
                else:
                    redge[2 * (group * 4 + a) + b // 3, spare(t), :] = column[a]


def finish(a, low, high, scale_ref, diag_ref, minv, u0_ref, cedge, redge):
    groups = u0_ref.shape[0] // 16
    span = slice(low, high)
    mass_sums = join_cols(cedge, a, low, high)
    lap_sums = join_cols(cedge, 4 + a, low, high)
    for group in range(groups):
        scale = scale_ref[group : group + 1, :]
        source = join_cols(redge, group * 4 + a, low, high)
        for side, b in enumerate((0, 3)):
            diag = mass_sums[side] + scale * lap_sums[side]
            inverse = 1.0 / diag
            diag_ref[plane(group, a, b), span, :] = diag
            u0_ref[plane(group, a, b), span, :] = source[side] * inverse
            minv[plane(group, a, b), span, :] = inverse * scale


def operator_tile(t, own, sums, now_ref, old_ref, new_ref, mass_ref, krow, kcol, minv, w_ref, edge):
    groups = now_ref.shape[0] // 16
    zero = jnp.zeros((8, LANES), jnp.float32)
    sums = list(sums)
    for group in range(groups):
        u = [[now_ref[plane(group, a, b), tile(t), :] for b in range(4)] for a in range(4)]
        along_rows = [
            line_operator(
                [krow[line * 6 + i, tile(t), :] for i in range(6)], [u[a][line] for a in range(4)]
            )
            for line in range(4)
        ]
        along_cols = [
            line_operator([kcol[line * 6 + i, tile(t), :] for i in range(6)], u[line])
            for line in range(4)
        ]
        with_now, with_old = zero, zero
        y = [[None] * 4 for _ in range(4)]
        for a in range(4):
            for b in range(4):
                p = plane(group, a, b)
                value = mass_ref[p, tile(t), :] * u[a][b]
                row, col = along_rows[b][a], along_cols[a][b]
                value = value - row if a == 3 else value + row
                value = value - col if b == 3 else value + col
                y[a][b] = value
                with_now += u[a][b] * value
                if old_ref is None:
                    with_old += w_ref[p, tile(t), :] * u[a][b]
                else:
                    with_old += old_ref[p, tile(t), :] * value
        sums[group] += with_now if own is None else own * with_now
        sums[groups + group] += with_old if own is None else own * with_old
        for b in range(4):
            column = [y[a][b] for a in range(4)]
            column[0], column[3] = join_rows_in_turn(column[0], column[3])
            for a in range(4):
                p = plane(group, a, b)
                if b in (1, 2):
                    if new_ref is None:
                        w_ref[p, tile(t), :] = column[a]
                    else:
                        new_ref[p, tile(t), :] = column[a] * minv[p, tile(t), :] - u[a][b]
                else:
                    edge[2 * (group * 4 + a) + b // 3, spare(t), :] = column[a]
    return tuple(sums)


def several(low, high, count, body, sums):
    def step(i, sums):
        for j in range(count):
            sums = body(low + i * count + j, sums)
        return sums

    steps = (high - low) // count
    sums = lax.fori_loop(0, steps, step, sums)
    for t in range(low + steps * count, high):
        sums = body(jnp.int32(t), sums)
    return sums


def prep_kernel(t_ref, rim_ref, scale_ref, *refs):
    state, (u1_ref, edge, sums_ref) = refs[:9], refs[9:]
    mass_ref, krow, kcol, diag_ref, minv, u0_ref, w_ref, cedge, redge = state
    cols = t_ref.shape[1]
    rim = lax.broadcasted_iota(jnp.int32, (8, LANES), 1) < RIM

    @pl.loop(0, cols // 8)
    def _(t):
        def fetch(p):
            group, a, b = p // 16, p // 4 % 4, p % 4
            outer = rim_ref[t, group, pl.ds(b, 8, stride=4), :]
            if a:
                outer = pltpu.roll(outer, LANES - a * RIM, 1)
            return jnp.where(rim, outer, t_ref[p, tile(t), :])

        prepare(t, fetch, scale_ref, *state)

    for a in range(4):
        finish(a, 8, cols - 8, scale_ref, diag_ref, minv, u0_ref, cedge, redge)

    zero = jnp.zeros((8, LANES), jnp.float32)
    sums = several(
        1,
        cols // 8 - 1,
        3,
        lambda t, sums: operator_tile(
            t, None, sums, u0_ref, None, u1_ref, mass_ref, krow, kcol, minv, w_ref, edge
        ),
        (zero,) * sums_ref.shape[0],
    )
    for i, value in enumerate(sums):
        sums_ref[i] = value


def krylov_kernel(cols, count, right_ref, left_ref, scale_ref, *refs):
    state = refs[count : count + 9]
    u1_ref, edge, sums_ref, u2_ref, part_ref = refs[count + 9 :]
    mass_ref, krow, kcol, diag_ref, minv, u0_ref, w_ref, cedge, redge = state
    groups = u0_ref.shape[0] // 16
    total = u0_ref.shape[1]
    tiles = total // 8
    own_tiles = cols // 8
    scales = [scale_ref[group : group + 1, :] for group in range(groups)]
    prepare(
        own_tiles, lambda p: jnp.concatenate([right_ref[p], left_ref[p]], axis=0), scale_ref, *state
    )

    for a in range(4):
        wrap_cols(cedge, a, total)
        wrap_cols(cedge, 4 + a, total)
        for group in range(groups):
            wrap_cols(redge, group * 4 + a, total)
        for low, high in ((0, 8), (cols - 8, total)):
            finish(a, low, high, scale_ref, diag_ref, minv, u0_ref, cedge, redge)

    zero = jnp.zeros((8, LANES), jnp.float32)
    shared = (mass_ref, krow, kcol, minv, w_ref, edge)

    def apply(now_ref, old_ref, new_ref):
        def body(i, sums):
            if old_ref is None:
                t = jnp.where(i == 0, 0, i + own_tiles - 2)
            else:
                t = i
            own = (t < own_tiles).astype(jnp.float32)
            return operator_tile(t, own, sums, now_ref, old_ref, new_ref, *shared)

        if old_ref is None:
            sums = several(0, 3, 3, body, tuple(sums_ref[i] for i in range(2 * groups)))
        else:
            sums = several(0, tiles, 3, body, (zero,) * (2 * groups))

        for i in range(groups * 4):
            wrap_cols(edge, i, total)
            for b, value in zip((0, 3), join_cols(edge, i, 0, total)):
                p = i * 4 + b
                if new_ref is None:
                    w_ref[p] = value
                else:
                    new_ref[p] = value * minv[p] - now_ref[p]

        return sums[:groups], sums[groups:]

    g00, b0 = apply(u0_ref, None, u1_ref)
    g11, g01 = apply(u1_ref, u0_ref, u2_ref)
    g22, g12 = apply(u2_ref, u1_ref, None)
    rows = [jnp.sum(x, axis=0, keepdims=True) for x in b0]
    for q in (g00, g01, g11, g12, g22):
        rows += [scale * jnp.sum(x, axis=0, keepdims=True) for scale, x in zip(scales, q)]
    rows += [jnp.zeros((1, LANES), jnp.float32)] * (-len(rows) % 8)
    table = jnp.concatenate(rows, axis=0)
    lanes = lax.broadcasted_iota(jnp.int32, table.shape, 1)
    lines = lax.broadcasted_iota(jnp.int32, table.shape, 0)
    table = jnp.where(lanes >= RIM, table, 0.0)
    table = over_rows(table)
    table = jnp.where(lanes // PACK == lines, table, 0.0)
    part_ref[...] = jnp.broadcast_to(jnp.sum(table, axis=0, keepdims=True), part_ref.shape)


def combine_kernel(
    parts_ref, scale_ref, u0_ref, u1_ref, u2_ref, w_ref, diag_ref, sol_hbm, res_hbm, sol, res, xs, xt, sems
):
    halves, modes, rows, _ = sol.shape
    groups = modes // PACK
    own = rows // 4
    per_half = LANES // 4
    total = jnp.sum(parts_ref[...], axis=0, keepdims=True)
    table = jnp.broadcast_to(total, (24, LANES))
    lanes = lax.broadcasted_iota(jnp.int32, table.shape, 1)
    lines = lax.broadcasted_iota(jnp.int32, table.shape, 0)
    table = jnp.where(lanes // PACK == lines, table, 0.0)
    table = over_rows(table)
    b0, g00, g01, g11, g12, g22 = [table[q * groups : (q + 1) * groups] for q in range(6)]
    g02 = g11
    b1 = g00 - b0
    b2 = g01 - b1
    l10 = g01 / g00
    l20 = g02 / g00
    d1 = g11 - l10 * g01
    t12 = g12 - l20 * g01
    l21 = t12 / d1
    d2 = g22 - l20 * g02 - l21 * t12
    y1 = b1 - l10 * b0
    y2 = b2 - l20 * b0 - l21 * y1
    c2 = y2 / d2
    c1 = y1 / d1 - l21 * c2
    c0 = b0 / g00 - l10 * c1 - l20 * c2
    copies = []
    for half in range(halves):
        span = slice(half * per_half, (half + 1) * per_half)
        for group in range(groups):
            k0, k1, k2 = [c[group : group + 1, :] for c in (c0, c1, c2)]
            r0, r1, r2 = 1.0 - k0, k0 + k1, k2 * scale_ref[group : group + 1, :]
            for a in range(4):
                slot = group * 4 + a
                for b in range(4):
                    p = plane(group, a, b)
                    u0, u1, u2 = u0_ref[p, span, :], u1_ref[p, span, :], u2_ref[p, span, :]
                    xs[0, slot, pl.ds(b, per_half, stride=4), :] = k0 * u0 + k1 * u1 + k2 * u2
                    xs[1, slot, pl.ds(b, per_half, stride=4), :] = (
                        diag_ref[p, span, :] * (r0 * u0 - r1 * u1 - k1 * u2) - r2 * w_ref[p, span, :]
                    )
                for i, out in enumerate((sol, res)):
                    xt[i, slot] = xs[i, slot].T
                    for m in range(PACK):
                        out[half, group * PACK + m, pl.ds(a, own, stride=4), :] = xt[
                            i, slot, pl.ds(RIM + m, own, stride=PACK), :
                        ]
            span_modes = pl.ds(group * PACK, PACK)
            for i, (out, hbm) in enumerate(((sol, sol_hbm), (res, res_hbm))):
                copy = pltpu.make_async_copy(
                    out.at[half, span_modes],
                    hbm.at[span_modes, :, pl.ds(half * LANES, LANES)],
                    sems.at[half, group, i],
                )
                copy.start()
                copies.append(copy)
    for copy in copies:
        copy.wait()


def shards(forcing, metric, jacobian, mode_scale):
    modes, rows, cols = forcing.shape
    groups = modes // PACK
    halo = 4 * GHOST
    f32 = jnp.float32

    def shift(x, axis, step):
        count = lax.axis_size(axis)
        return lax.ppermute(x, axis, [(i, (i + step) % count) for i in range(count)])

    vmem = pl.BlockSpec(memory_space=pltpu.VMEM)
    anywhere = pl.BlockSpec(memory_space=pl.ANY)
    array = lambda *shape: jax.ShapeDtypeStruct(shape, f32)
    planes = 16 * (groups + 1)
    ecols = cols // 4
    halves = cols // LANES
    inputs = [
        pltpu.with_memory_space_constraint(x, pltpu.HBM)
        for x in (forcing, metric, jacobian, mode_scale)
    ]
    top, bottom, scale = pl.pallas_call(
        load_kernel,
        in_specs=[anywhere] * 4,
        out_specs=[vmem] * 3,
        out_shape=[array(halves, modes + 2, halo, LANES)] * 2 + [array(groups, LANES)],
        scratch_shapes=[
            pltpu.SMEM((modes,), f32),
            pltpu.SemaphoreType.DMA((2, halves, 3)),
            pltpu.SemaphoreType.DMA,
        ],
        compiler_params=pltpu.CompilerParams(vmem_limit_bytes=4 << 20),
        name="load",
    )(*inputs)
    up = shift(bottom, "curve", 1)
    down = shift(top, "curve", -1)

    spread = pl.pallas_call(
        spread_kernel,
        in_specs=[anywhere] * 3,
        out_specs=vmem,
        out_shape=array(planes, ecols, LANES),
        scratch_shapes=[
            pltpu.VMEM((halves, modes + 2, rows, LANES), f32),
            pltpu.VMEM((halves * planes // 4, LANES, LANES), f32),
            pltpu.VMEM((halves * planes // 4, LANES, LANES), f32),
            pltpu.SemaphoreType.DMA((halves, 3)),
        ],
        compiler_params=pltpu.CompilerParams(vmem_limit_bytes=12 << 20),
        cost_estimate=pl.CostEstimate(flops=10_000_000, bytes_accessed=0, transcendentals=0),
        name="spread",
    )(*inputs[:3])
    rim, low, high = pl.pallas_call(
        ghost_kernel,
        in_specs=[vmem] * 3,
        out_specs=[vmem] * 3,
        out_shape=[array(ecols // 8, groups + 1, 32, LANES)] + [array(planes, GHOST, LANES)] * 2,
        scratch_shapes=[
            pltpu.VMEM((halves * (groups + 1), LANES, LANES), f32),
            pltpu.VMEM((2, planes // 4, 4 * GHOST, LANES), f32),
        ],
        compiler_params=pltpu.CompilerParams(vmem_limit_bytes=12 << 20),
        name="ghost",
    )(up, down, spread)

    left = shift(high, "sub", 1)
    right = shift(low, "sub", -1)

    total = ecols + 2 * GHOST
    field = array(16 * groups, total, LANES)
    lines = array(24, total, LANES)
    state = pl.pallas_call(
        prep_kernel,
        in_specs=[vmem] * 3,
        out_specs=[vmem] * 12,
        out_shape=[field, lines, lines, field, field, field, field]
        + [array(16, total + 16, LANES), array(8 * groups, total + 16, LANES)]
        + [field, array(8 * groups, total + 16, LANES), array(2 * groups, 8, LANES)],
        compiler_params=pltpu.CompilerParams(vmem_limit_bytes=24 << 20),
        cost_estimate=pl.CostEstimate(flops=20_000_000, bytes_accessed=0, transcendentals=0),
        name="prep",
    )(spread, rim, scale)
    devices = lax.axis_size(AXES[0]) * lax.axis_size(AXES[1])
    count = len(state)
    out = pl.pallas_call(
        functools.partial(krylov_kernel, ecols, count),
        in_specs=[vmem] * (3 + count),
        out_specs=[vmem] * (count + 2),
        out_shape=[array(*x.shape) for x in state] + [field, array(devices, LANES)],
        input_output_aliases={3 + i: i for i in range(count)},
        compiler_params=pltpu.CompilerParams(vmem_limit_bytes=24 << 20),
        name="krylov",
    )(right, left, scale, *state)
    diag, u0, w3, u1 = out[3], out[5], out[6], out[9]
    u2, part = out[count:]

    parts = lax.all_to_all(part, AXES, 0, 0, tiled=True)

    out = jax.ShapeDtypeStruct((modes, rows, cols), f32)
    return tuple(
        pl.pallas_call(
            combine_kernel,
            in_specs=[vmem] * 7,
            out_specs=[anywhere] * 2,
            out_shape=[out] * 2,
            scratch_shapes=[
                pltpu.VMEM((halves, modes, rows, LANES), f32),
                pltpu.VMEM((halves, modes, rows, LANES), f32),
                pltpu.VMEM((2, 4 * groups, LANES, LANES), f32),
                pltpu.VMEM((2, 4 * groups, LANES, LANES), f32),
                pltpu.SemaphoreType.DMA((halves, groups, 2)),
            ],
            compiler_params=pltpu.CompilerParams(vmem_limit_bytes=20 << 20),
            name="combine",
        )(parts, scale, u0, u1, u2, w3, diag)
    )


def solution(mesh):
    in_specs = (P(None, "curve", "sub"), P("curve", "sub"), P("curve", "sub"), P())
    out_specs = (P(None, "curve", "sub"), P(None, "curve", "sub"))
    return jax.shard_map(
        shards, mesh=mesh, in_specs=in_specs, out_specs=out_specs, check_vma=False
    )
```

```python
import functools
import math

import jax
import jax.numpy as jnp
import numpy as np
from jax import lax
from jax.experimental import pallas as pl
from jax.experimental.pallas import tpu as pltpu
from jax.sharding import PartitionSpec as P

GHOST = 4
PACK = 4
LANES = 128
AXES = ("curve", "sub")
RIM = 2 * GHOST * PACK


def gll_tables():
    points = np.array([-1.0, -1.0 / math.sqrt(5.0), 1.0 / math.sqrt(5.0), 1.0])
    weights = np.array([1.0 / 6.0, 5.0 / 6.0, 5.0 / 6.0, 1.0 / 6.0])
    factor = np.array(
        [np.prod([points[j] - points[m] for m in range(4) if m != j]) for j in range(4)]
    )
    slopes = np.zeros((4, 4))
    for i in range(4):
        for j in range(4):
            if i != j:
                slopes[i, j] = factor[i] / (factor[j] * (points[i] - points[j]))
        slopes[i, i] = sum((1.0 / (points[i] - points[m]) for m in range(4) if m != i))
    return (slopes, weights)


SLOPES, WEIGHTS = gll_tables()
PAIRS = [(a, k) for a in range(4) for k in range(a + 1, 4)]


def plane(group, a, b):
    return (group * 4 + a) * 4 + b


def stack_copies(f_hbm, metric_hbm, jacobian_hbm, out, at, sems):
    halves, stack, size, _ = out.shape
    span = pl.ds(at, size)
    copies = []
    for half in range(halves):
        columns = pl.ds(half * LANES, LANES)
        pairs = (
            (f_hbm.at[:, span, columns], out.at[half, pl.ds(0, stack - 2)]),
            (metric_hbm.at[span, columns], out.at[half, stack - 2]),
            (jacobian_hbm.at[span, columns], out.at[half, stack - 1]),
        )
        copies.append(
            [pltpu.make_async_copy(x, y, sems.at[half, i]) for i, (x, y) in enumerate(pairs)]
        )
    for per_half in copies:
        for copy in per_half:
            copy.start()
    return copies


def load_kernel(f_hbm, metric_hbm, jacobian_hbm, scale_hbm, top, bottom, scale_ref, scales, sems, scale_sem):
    modes, rows, _ = f_hbm.shape
    halo = top.shape[2]
    scale_copy = pltpu.make_async_copy(scale_hbm, scales, scale_sem)
    scale_copy.start()
    copies = stack_copies(f_hbm, metric_hbm, jacobian_hbm, top, 0, sems.at[0])
    copies += stack_copies(f_hbm, metric_hbm, jacobian_hbm, bottom, rows - halo, sems.at[1])
    scale_copy.wait()
    member = lax.broadcasted_iota(jnp.int32, (1, LANES), 1) % PACK
    for group in range(modes // PACK):
        row = jnp.zeros((1, LANES), jnp.float32)
        for m in range(PACK):
            row = jnp.where(member == m, scales[group * PACK + m], row)
        scale_ref[group : group + 1, :] = row
    for per_half in copies:
        for copy in per_half:
            copy.wait()


def spread_kernel(f_hbm, metric_hbm, jacobian_hbm, t_ref, fields_ref, xs, xt, sems):
    halves, stack, rows, _ = fields_ref.shape
    own = rows // 4
    groups = (stack - 2) // PACK
    per_half = LANES // 4
    copies = stack_copies(f_hbm, metric_hbm, jacobian_hbm, fields_ref, 0, sems)
    for half in range(halves):
        for copy in copies[half]:
            copy.wait()
        for group in range(groups + 1):
            for a in range(4):
                at = (half * (groups + 1) + group) * 4 + a
                for m in range(PACK):
                    index = group * PACK + (m if group < groups else m % 2)
                    xs[at, pl.ds(RIM + m, own, stride=PACK), :] = fields_ref[
                        half, index, pl.ds(a, own, stride=4), :
                    ]
                xs[at, :RIM, :] = jnp.zeros((RIM, LANES), jnp.float32)
                xt[at] = xs[at].T
                for b in range(4):
                    t_ref[plane(group, a, b), half * per_half : (half + 1) * per_half, :] = xt[
                        at, pl.ds(b, per_half, stride=4), :
                    ]


def ghost_kernel(up_ref, down_ref, own_ref, rim_ref, low_ref, high_ref, xs, ends):
    halves, stack, _, _ = up_ref.shape
    groups = (stack - 2) // PACK
    per_half = rim_ref.shape[0] // halves
    height = rim_ref.shape[2]
    rim = lax.broadcasted_iota(jnp.int32, (GHOST, LANES), 1) < RIM
    for half in range(halves):
        for group in range(groups + 1):
            at = half * (groups + 1) + group
            for a in range(4):
                for m in range(PACK):
                    index = group * PACK + (m if group < groups else m % 2)
                    for side, ref in enumerate((down_ref, up_ref)):
                        start = a * RIM + side * GHOST * PACK + m
                        xs[at, pl.ds(start, GHOST, stride=PACK), :] = ref[
                            half, index, pl.ds(a, GHOST, stride=4), :
                        ]
            turned = xs[at].T
            for i in range(per_half):
                rim_ref[half * per_half + i, group] = turned[i * height : (i + 1) * height]
    last = rim_ref.shape[0] - 1
    total = own_ref.shape[1]
    size = 4 * GHOST
    for group in range(groups + 1):
        for a in range(4):
            at = group * 4 + a
            for side, x in enumerate((rim_ref[0, group, :size], rim_ref[last, group, height - size :])):
                ends[side, at] = pltpu.roll(x, LANES - a * RIM, 1) if a else x
            for b in range(4):
                p = at * 4 + b
                picked = pl.ds(b, GHOST, stride=4)
                low_ref[p] = jnp.where(rim, ends[0, at, picked, :], own_ref[p, :GHOST, :])
                high_ref[p] = jnp.where(rim, ends[1, at, picked, :], own_ref[p, total - GHOST :, :])


def line_operator(coefs, values):
    f01, f02, f03, f12, f13, f23 = [
        coef * (values[k] - values[a]) for (a, k), coef in zip(PAIRS, coefs)
    ]
    return f01 + f02 + f03, f12 + f13 - f01, f23 - f02 - f12, f03 + f13 + f23


def over_rows(table):
    i = lax.broadcasted_iota(jnp.int32, (LANES, LANES), 0)
    j = lax.broadcasted_iota(jnp.int32, (LANES, LANES), 1)
    same = jnp.where(i % PACK == j % PACK, 1.0, 0.0).astype(jnp.float32)
    return jnp.dot(
        table, same, precision=lax.Precision.HIGHEST, preferred_element_type=jnp.float32
    )


def tile(t):
    return pl.ds(pl.multiple_of(t * 8, 8), 8)


def spare(t):
    return pl.ds(pl.multiple_of(t * 8 + 8, 8), 8)


def join_rows(first, last):
    return first + pltpu.roll(last, PACK, 1), last + pltpu.roll(first, LANES - PACK, 1)


def join_rows_in_turn(first, last):
    shared = last + pltpu.roll(first, LANES - PACK, 1)
    return pltpu.roll(shared, PACK, 1), shared


def wrap_cols(edge, i, total):
    edge[2 * i, total + 8 : total + 16, :] = edge[2 * i, 8:16, :]
    edge[2 * i + 1, 0:8, :] = edge[2 * i + 1, total : total + 8, :]


def join_cols(edge, i, low, high):
    first = edge[2 * i, low + 8 : high + 8, :] + edge[2 * i + 1, low + 7 : high + 7, :]
    last = edge[2 * i + 1, low + 8 : high + 8, :] + edge[2 * i, low + 9 : high + 9, :]
    return first, last


def prepare(t, fetch, scale_ref, mass_ref, krow, kcol, diag_ref, minv, u0_ref, source_ref, cedge, redge):
    groups = u0_ref.shape[0] // 16
    lane = lax.broadcasted_iota(jnp.int32, (8, LANES), 1)
    even = lane % 2 == 0
    grid = [(a, b) for a in range(4) for b in range(4)]
    scales = [scale_ref[group : group + 1, :] for group in range(groups)]
    flux, mass, lap = {}, {}, {}
    for a, b in grid:
        x = fetch(plane(groups, a, b))
        w = np.float32(WEIGHTS[a] * WEIGHTS[b])
        flux[a, b] = jnp.where(even, x, pltpu.roll(x, 1, 1)) * w
        mass[a, b] = jnp.where(even, pltpu.roll(x, LANES - 1, 1), x) * w
    for group in range(groups):
        inverse = 1.0 / scales[group]
        for a, b in grid:
            mass_ref[plane(group, a, b), tile(t), :] = mass[a, b] * inverse
            source_ref[plane(group, a, b), tile(t), :] = fetch(plane(group, a, b)) * mass[a, b]

    def less(a, b, value):
        lap[a, b] = lap[a, b] + value if (a, b) in lap else value

    for line in range(4):
        for i, (p, q) in enumerate(PAIRS):
            c = [np.float32(SLOPES[j, p] * SLOPES[j, q]) for j in range(4)]
            kr = sum(flux[j, line] * c[j] for j in range(4))
            kc = sum(flux[line, j] * c[j] for j in range(4))
            krow[line * 6 + i, tile(t), :] = kr
            kcol[line * 6 + i, tile(t), :] = kc
            less(p, line, kr)
            less(q, line, kr)
            less(line, p, kc)
            less(line, q, kc)
    for a, b in grid:
        lap[a, b] = -lap[a, b]
    for values, base in ((mass, 0), (lap, 4)):
        for b in range(4):
            values[0, b], values[3, b] = join_rows(values[0, b], values[3, b])
            for a in range(4):
                if b in (0, 3):
                    cedge[2 * (base + a) + b // 3, spare(t), :] = values[a, b]
    for group in range(groups):
        for b in range(4):
            column = [source_ref[plane(group, a, b), tile(t), :] for a in range(4)]
            column[0], column[3] = join_rows(column[0], column[3])
            for a in range(4):
                p = plane(group, a, b)
                if b in (1, 2):
                    diag = mass[a, b] + scales[group] * lap[a, b]
                    inverse = 1.0 / diag
                    diag_ref[p, tile(t), :] = diag
                    u0_ref[p, tile(t), :] = column[a] * inverse
                    minv[p, tile(t), :] = inverse * scales[group]
                else:
                    redge[2 * (group * 4 + a) + b // 3, spare(t), :] = column[a]


def finish(a, low, high, scale_ref, diag_ref, minv, u0_ref, cedge, redge):
    groups = u0_ref.shape[0] // 16
    span = slice(low, high)
    mass_sums = join_cols(cedge, a, low, high)
    lap_sums = join_cols(cedge, 4 + a, low, high)
    for group in range(groups):
        scale = scale_ref[group : group + 1, :]
        source = join_cols(redge, group * 4 + a, low, high)
        for side, b in enumerate((0, 3)):
            diag = mass_sums[side] + scale * lap_sums[side]
            inverse = 1.0 / diag
            diag_ref[plane(group, a, b), span, :] = diag
            u0_ref[plane(group, a, b), span, :] = source[side] * inverse
            minv[plane(group, a, b), span, :] = inverse * scale


def operator_tile(t, own, sums, now_ref, old_ref, new_ref, mass_ref, krow, kcol, minv, w_ref, edge):
    groups = now_ref.shape[0] // 16
    zero = jnp.zeros((8, LANES), jnp.float32)
    sums = list(sums)
    for group in range(groups):
        u = [[now_ref[plane(group, a, b), tile(t), :] for b in range(4)] for a in range(4)]
        along_rows = [
            line_operator(
                [krow[line * 6 + i, tile(t), :] for i in range(6)], [u[a][line] for a in range(4)]
            )
            for line in range(4)
        ]
        along_cols = [
            line_operator([kcol[line * 6 + i, tile(t), :] for i in range(6)], u[line])
            for line in range(4)
        ]
        with_now, with_old = zero, zero
        y = [[None] * 4 for _ in range(4)]
        for a in range(4):
            for b in range(4):
                p = plane(group, a, b)
                value = mass_ref[p, tile(t), :] * u[a][b]
                row, col = along_rows[b][a], along_cols[a][b]
                value = value - row if a == 3 else value + row
                value = value - col if b == 3 else value + col
                y[a][b] = value
                with_now += u[a][b] * value
                if old_ref is None:
                    with_old += w_ref[p, tile(t), :] * u[a][b]
                else:
                    with_old += old_ref[p, tile(t), :] * value
        sums[group] += with_now if own is None else own * with_now
        sums[groups + group] += with_old if own is None else own * with_old
        for b in range(4):
            column = [y[a][b] for a in range(4)]
            column[0], column[3] = join_rows_in_turn(column[0], column[3])
            for a in range(4):
                p = plane(group, a, b)
                if b in (1, 2):
                    if new_ref is None:
                        w_ref[p, tile(t), :] = column[a]
                    else:
                        new_ref[p, tile(t), :] = column[a] * minv[p, tile(t), :] - u[a][b]
                else:
                    edge[2 * (group * 4 + a) + b // 3, spare(t), :] = column[a]
    return tuple(sums)


def several(low, high, count, body, sums):
    def step(i, sums):
        for j in range(count):
            sums = body(low + i * count + j, sums)
        return sums

    steps = (high - low) // count
    sums = lax.fori_loop(0, steps, step, sums)
    for t in range(low + steps * count, high):
        sums = body(jnp.int32(t), sums)
    return sums


def prep_kernel(t_ref, rim_ref, scale_ref, *refs):
    state, (u1_ref, edge, sums_ref) = refs[:9], refs[9:]
    mass_ref, krow, kcol, diag_ref, minv, u0_ref, w_ref, cedge, redge = state
    cols = t_ref.shape[1]
    rim = lax.broadcasted_iota(jnp.int32, (8, LANES), 1) < RIM

    def one(t):
        def fetch(p):
            group, a, b = p // 16, p // 4 % 4, p % 4
            outer = rim_ref[t, group, pl.ds(b, 8, stride=4), :]
            if a:
                outer = pltpu.roll(outer, LANES - a * RIM, 1)
            return jnp.where(rim, outer, t_ref[p, tile(t), :])

        prepare(t, fetch, scale_ref, *state)

    @pl.loop(0, cols // 16)
    def _(i):
        one(2 * i)
        one(2 * i + 1)

    @pl.loop(0, 4)
    def _(a):
        finish(a, 8, cols - 8, scale_ref, diag_ref, minv, u0_ref, cedge, redge)

    zero = jnp.zeros((8, LANES), jnp.float32)
    sums = several(
        1,
        cols // 8 - 1,
        3,
        lambda t, sums: operator_tile(
            t, None, sums, u0_ref, None, u1_ref, mass_ref, krow, kcol, minv, w_ref, edge
        ),
        (zero,) * sums_ref.shape[0],
    )
    for i, value in enumerate(sums):
        sums_ref[i] = value


def krylov_kernel(cols, count, right_ref, left_ref, scale_ref, *refs):
    state = refs[count : count + 9]
    u1_ref, edge, sums_ref, u2_ref, part_ref = refs[count + 9 :]
    mass_ref, krow, kcol, diag_ref, minv, u0_ref, w_ref, cedge, redge = state
    groups = u0_ref.shape[0] // 16
    total = u0_ref.shape[1]
    tiles = total // 8
    own_tiles = cols // 8
    scales = [scale_ref[group : group + 1, :] for group in range(groups)]
    prepare(
        own_tiles, lambda p: jnp.concatenate([right_ref[p], left_ref[p]], axis=0), scale_ref, *state
    )

    @pl.loop(0, 4)
    def _(a):
        wrap_cols(cedge, a, total)
        wrap_cols(cedge, 4 + a, total)
        for group in range(groups):
            wrap_cols(redge, group * 4 + a, total)
        for low, high in ((0, 8), (cols - 8, total)):
            finish(a, low, high, scale_ref, diag_ref, minv, u0_ref, cedge, redge)

    zero = jnp.zeros((8, LANES), jnp.float32)
    shared = (mass_ref, krow, kcol, minv, w_ref, edge)

    def apply(now_ref, old_ref, new_ref):
        def body(i, sums):
            if old_ref is None:
                t = jnp.where(i == 0, 0, i + own_tiles - 2)
            else:
                t = i
            own = (t < own_tiles).astype(jnp.float32)
            return operator_tile(t, own, sums, now_ref, old_ref, new_ref, *shared)

        if old_ref is None:
            sums = several(0, 3, 3, body, tuple(sums_ref[i] for i in range(2 * groups)))
        else:
            sums = several(0, tiles, 3, body, (zero,) * (2 * groups))

        @pl.loop(0, groups * 4)
        def _(i):
            wrap_cols(edge, i, total)
            for b, value in zip((0, 3), join_cols(edge, i, 0, total)):
                p = i * 4 + b
                if new_ref is None:
                    w_ref[p] = value
                else:
                    new_ref[p] = value * minv[p] - now_ref[p]

        return sums[:groups], sums[groups:]

    g00, b0 = apply(u0_ref, None, u1_ref)
    g11, g01 = apply(u1_ref, u0_ref, u2_ref)
    g22, g12 = apply(u2_ref, u1_ref, None)
    rows = [jnp.sum(x, axis=0, keepdims=True) for x in b0]
    for q in (g00, g01, g11, g12, g22):
        rows += [scale * jnp.sum(x, axis=0, keepdims=True) for scale, x in zip(scales, q)]
    rows += [jnp.zeros((1, LANES), jnp.float32)] * (-len(rows) % 8)
    table = jnp.concatenate(rows, axis=0)
    lanes = lax.broadcasted_iota(jnp.int32, table.shape, 1)
    lines = lax.broadcasted_iota(jnp.int32, table.shape, 0)
    table = jnp.where(lanes >= RIM, table, 0.0)
    table = over_rows(table)
    table = jnp.where(lanes // PACK == lines, table, 0.0)
    part_ref[...] = jnp.broadcast_to(jnp.sum(table, axis=0, keepdims=True), part_ref.shape)


def combine_kernel(
    parts_ref, scale_ref, u0_ref, u1_ref, u2_ref, w_ref, diag_ref, sol_hbm, res_hbm, sol, res, xs, xt, sems
):
    halves, modes, rows, _ = sol.shape
    groups = modes // PACK
    own = rows // 4
    per_half = LANES // 4
    total = jnp.sum(parts_ref[...], axis=0, keepdims=True)
    table = jnp.broadcast_to(total, (24, LANES))
    lanes = lax.broadcasted_iota(jnp.int32, table.shape, 1)
    lines = lax.broadcasted_iota(jnp.int32, table.shape, 0)
    table = jnp.where(lanes // PACK == lines, table, 0.0)
    table = over_rows(table)
    b0, g00, g01, g11, g12, g22 = [table[q * groups : (q + 1) * groups] for q in range(6)]
    g02 = g11
    b1 = g00 - b0
    b2 = g01 - b1
    l10 = g01 / g00
    l20 = g02 / g00
    d1 = g11 - l10 * g01
    t12 = g12 - l20 * g01
    l21 = t12 / d1
    d2 = g22 - l20 * g02 - l21 * t12
    y1 = b1 - l10 * b0
    y2 = b2 - l20 * b0 - l21 * y1
    c2 = y2 / d2
    c1 = y1 / d1 - l21 * c2
    c0 = b0 / g00 - l10 * c1 - l20 * c2
    copies = []
    for half in range(halves):
        span = slice(half * per_half, (half + 1) * per_half)
        for group in range(groups):
            k0, k1, k2 = [c[group : group + 1, :] for c in (c0, c1, c2)]
            r0, r1, r2 = 1.0 - k0, k0 + k1, k2 * scale_ref[group : group + 1, :]
            for a in range(4):
                slot = group * 4 + a
                for b in range(4):
                    p = plane(group, a, b)
                    u0, u1, u2 = u0_ref[p, span, :], u1_ref[p, span, :], u2_ref[p, span, :]
                    xs[0, slot, pl.ds(b, per_half, stride=4), :] = k0 * u0 + k1 * u1 + k2 * u2
                    xs[1, slot, pl.ds(b, per_half, stride=4), :] = (
                        diag_ref[p, span, :] * (r0 * u0 - r1 * u1 - k1 * u2) - r2 * w_ref[p, span, :]
                    )
                for i, out in enumerate((sol, res)):
                    xt[i, slot] = xs[i, slot].T
                    for m in range(PACK):
                        out[half, group * PACK + m, pl.ds(a, own, stride=4), :] = xt[
                            i, slot, pl.ds(RIM + m, own, stride=PACK), :
                        ]
            span_modes = pl.ds(group * PACK, PACK)
            for i, (out, hbm) in enumerate(((sol, sol_hbm), (res, res_hbm))):
                copy = pltpu.make_async_copy(
                    out.at[half, span_modes],
                    hbm.at[span_modes, :, pl.ds(half * LANES, LANES)],
                    sems.at[half, group, i],
                )
                copy.start()
                copies.append(copy)
    for copy in copies:
        copy.wait()


def shards(forcing, metric, jacobian, mode_scale):
    modes, rows, cols = forcing.shape
    groups = modes // PACK
    halo = 4 * GHOST
    f32 = jnp.float32

    def shift(x, axis, step):
        count = lax.axis_size(axis)
        return lax.ppermute(x, axis, [(i, (i + step) % count) for i in range(count)])

    vmem = pl.BlockSpec(memory_space=pltpu.VMEM)
    anywhere = pl.BlockSpec(memory_space=pl.ANY)
    array = lambda *shape: jax.ShapeDtypeStruct(shape, f32)
    planes = 16 * (groups + 1)
    ecols = cols // 4
    halves = cols // LANES
    inputs = [
        pltpu.with_memory_space_constraint(x, pltpu.HBM)
        for x in (forcing, metric, jacobian, mode_scale)
    ]
    top, bottom, scale = pl.pallas_call(
        load_kernel,
        in_specs=[anywhere] * 4,
        out_specs=[vmem] * 3,
        out_shape=[array(halves, modes + 2, halo, LANES)] * 2 + [array(groups, LANES)],
        scratch_shapes=[
            pltpu.SMEM((modes,), f32),
            pltpu.SemaphoreType.DMA((2, halves, 3)),
            pltpu.SemaphoreType.DMA,
        ],
        compiler_params=pltpu.CompilerParams(vmem_limit_bytes=4 << 20),
        name="load",
    )(*inputs)
    up = shift(bottom, "curve", 1)
    down = shift(top, "curve", -1)

    spread = pl.pallas_call(
        spread_kernel,
        in_specs=[anywhere] * 3,
        out_specs=vmem,
        out_shape=array(planes, ecols, LANES),
        scratch_shapes=[
            pltpu.VMEM((halves, modes + 2, rows, LANES), f32),
            pltpu.VMEM((halves * planes // 4, LANES, LANES), f32),
            pltpu.VMEM((halves * planes // 4, LANES, LANES), f32),
            pltpu.SemaphoreType.DMA((halves, 3)),
        ],
        compiler_params=pltpu.CompilerParams(vmem_limit_bytes=12 << 20),
        cost_estimate=pl.CostEstimate(flops=10_000_000, bytes_accessed=0, transcendentals=0),
        name="spread",
    )(*inputs[:3])
    rim, low, high = pl.pallas_call(
        ghost_kernel,
        in_specs=[vmem] * 3,
        out_specs=[vmem] * 3,
        out_shape=[array(ecols // 8, groups + 1, 32, LANES)] + [array(planes, GHOST, LANES)] * 2,
        scratch_shapes=[
            pltpu.VMEM((halves * (groups + 1), LANES, LANES), f32),
            pltpu.VMEM((2, planes // 4, 4 * GHOST, LANES), f32),
        ],
        compiler_params=pltpu.CompilerParams(vmem_limit_bytes=12 << 20),
        name="ghost",
    )(up, down, spread)

    left = shift(high, "sub", 1)
    right = shift(low, "sub", -1)

    total = ecols + 2 * GHOST
    field = array(16 * groups, total, LANES)
    lines = array(24, total, LANES)
    state = pl.pallas_call(
        prep_kernel,
        in_specs=[vmem] * 3,
        out_specs=[vmem] * 12,
        out_shape=[field, lines, lines, field, field, field, field]
        + [array(16, total + 16, LANES), array(8 * groups, total + 16, LANES)]
        + [field, array(8 * groups, total + 16, LANES), array(2 * groups, 8, LANES)],
        compiler_params=pltpu.CompilerParams(vmem_limit_bytes=24 << 20),
        cost_estimate=pl.CostEstimate(flops=20_000_000, bytes_accessed=0, transcendentals=0),
        name="prep",
    )(spread, rim, scale)
    devices = lax.axis_size(AXES[0]) * lax.axis_size(AXES[1])
    count = len(state)
    out = pl.pallas_call(
        functools.partial(krylov_kernel, ecols, count),
        in_specs=[vmem] * (3 + count),
        out_specs=[vmem] * (count + 2),
        out_shape=[array(*x.shape) for x in state] + [field, array(devices, LANES)],
        input_output_aliases={3 + i: i for i in range(count)},
        compiler_params=pltpu.CompilerParams(vmem_limit_bytes=24 << 20),
        name="krylov",
    )(right, left, scale, *state)
    diag, u0, w3, u1 = out[3], out[5], out[6], out[9]
    u2, part = out[count:]

    parts = lax.all_to_all(part, AXES, 0, 0, tiled=True)

    out = jax.ShapeDtypeStruct((modes, rows, cols), f32)
    return tuple(
        pl.pallas_call(
            combine_kernel,
            in_specs=[vmem] * 7,
            out_specs=[anywhere] * 2,
            out_shape=[out] * 2,
            scratch_shapes=[
                pltpu.VMEM((halves, modes, rows, LANES), f32),
                pltpu.VMEM((halves, modes, rows, LANES), f32),
                pltpu.VMEM((2, 4 * groups, LANES, LANES), f32),
                pltpu.VMEM((2, 4 * groups, LANES, LANES), f32),
                pltpu.SemaphoreType.DMA((halves, groups, 2)),
            ],
            compiler_params=pltpu.CompilerParams(vmem_limit_bytes=20 << 20),
            name="combine",
        )(parts, scale, u0, u1, u2, w3, diag)
    )


def solution(mesh):
    in_specs = (P(None, "curve", "sub"), P("curve", "sub"), P("curve", "sub"), P())
    out_specs = (P(None, "curve", "sub"), P(None, "curve", "sub"))
    return jax.shard_map(
        shards, mesh=mesh, in_specs=in_specs, out_specs=out_specs, check_vma=False
    )
```
